32 devices in a mesh: replica: 8 (over z, y), model: 4 (over x, core).
Axes of the slice: x: 2, y: 2, z: 4, core: 2. Of those that a mesh axis runs over, the one named last changes fastest.
Arguments:
- slope_up: float32 [8, 1024, 4096], P('replica', None, 'model'), may hold values from -4 to 4
- slope_down: float32 [8, 4096, 1024], P('replica', 'model'), may hold values from -4 to 4
- slope_query: float32 [8, 1024, 1024], P('replica', None, 'model'), may hold values from -4 to 4
- slope_key: float32 [8, 1024, 1024], P('replica', None, 'model'), may hold values from -4 to 4
- slope_value: float32 [8, 1024, 1024], P('replica', None, 'model'), may hold values from -4 to 4
- slope_mixed: float32 [8, 1024, 1024], P('replica', 'model'), may hold values from -4 to 4
- slope_norm: float32 [8, 1024], P('replica'), may hold values from -8 to 8
- slope_bias: float32 [8, 1024], P('replica'), may hold values from -8 to 8
- param_up: float32 [1024, 4096], P('replica', 'model'), may hold values from -0.25 to 0.25
- param_down: float32 [4096, 1024], P('model', 'replica'), may hold values from -0.125 to 0.125
- param_query: float32 [1024, 1024], P('replica', 'model'), may hold values from -0.25 to 0.25
- param_key: float32 [1024, 1024], P('replica', 'model'), may hold values from -0.25 to 0.25
- param_value: float32 [1024, 1024], P('replica', 'model'), may hold values from -0.25 to 0.25
- param_mixed: float32 [1024, 1024], P('model', 'replica'), may hold values from -0.25 to 0.25
- param_norm: float32 [1024], P('replica'), may hold values from 0.25 to 1.75
- param_bias: float32 [1024], P('replica'), may hold values from -3 to 3
- state_up: float32 [1024, 4096], P('replica', 'model'), may hold values from 0.0001953125 to 0.001953125
- state_down: float32 [4096, 1024], P('model', 'replica'), may hold values from 4.8828126e-05 to 0.00048828125
- state_query: float32 [1024, 1024], P('replica', 'model'), may hold values from 0.0001953125 to 0.001953125
- state_key: float32 [1024, 1024], P('replica', 'model'), may hold values from 0.0001953125 to 0.001953125
- state_value: float32 [1024, 1024], P('replica', 'model'), may hold values from 0.0001953125 to 0.001953125
- state_mixed: float32 [1024, 1024], P('model', 'replica'), may hold values from 0.0001953125 to 0.001953125
- state_norm: float32 [1024], P('replica'), may hold values from 0.05 to 0.8
- state_bias: float32 [1024], P('replica'), may hold values from 0.05 to 0.8
Outputs:
- half_up: bfloat16 [1024, 4096], P(None, 'model')
- half_down: bfloat16 [4096, 1024], P('model')
- half_query: bfloat16 [1024, 1024], P(None, 'model')
- half_key: bfloat16 [1024, 1024], P(None, 'model')
- half_value: bfloat16 [1024, 1024], P(None, 'model')
- half_mixed: bfloat16 [1024, 1024], P('model')
- half_norm: bfloat16 [1024], replicated
- half_bias: bfloat16 [1024], replicated
- next_up: float32 [1024, 4096], P('replica', 'model')
- next_down: float32 [4096, 1024], P('model', 'replica')
- next_query: float32 [1024, 1024], P('replica', 'model')
- next_key: float32 [1024, 1024], P('replica', 'model')
- next_value: float32 [1024, 1024], P('replica', 'model')
- next_mixed: float32 [1024, 1024], P('model', 'replica')
- next_norm: float32 [1024], P('replica')
- next_bias: float32 [1024], P('replica')
- state_new_up: float32 [1024, 4096], P('replica', 'model')
- state_new_down: float32 [4096, 1024], P('model', 'replica')
- state_new_query: float32 [1024, 1024], P('replica', 'model')
- state_new_key: float32 [1024, 1024], P('replica', 'model')
- state_new_value: float32 [1024, 1024], P('replica', 'model')
- state_new_mixed: float32 [1024, 1024], P('model', 'replica')
- state_new_norm: float32 [1024], P('replica')
- state_new_bias: float32 [1024], P('replica')
The draws below stay inside these ranges and needn't reach their ends.
All inputs are finite; a program needn't handle non-finite values.
Results may differ from the reference program's by a relative error of at most 0.001.
Values may be sent and summed in bfloat16 or wider, within the bound.
A program may use at most 64 MiB of HBM per device.

```python
import jax
import jax.numpy as jnp
from jax import lax

WIDTH = 1024
INNER = 4096
ATTN = 1024
REPLICAS = 8


def strengthened(drawn, own_key, source, target, parts, factor):
    owner, partner = [(jnp.arange(drawn.shape[axis_at]) // (drawn.shape[axis_at] // parts)).reshape([-1 if axis == axis_at else 1 for axis in range(drawn.ndim)]) for axis_at in (source, target)]
    chosen = jax.random.permutation(own_key, parts)[partner]
    strong = (owner == chosen) | (owner == (partner + parts // 2) % parts)
    return jnp.where(strong, factor * drawn, drawn)


def shard_levels(rng, dims, split, least, top_value):
    level, own = 1.0, jax.random.fold_in(rng, 6)
    for axis_at, blocks in split:
        heights = jnp.exp(jax.random.uniform(jax.random.fold_in(own, axis_at), (blocks,), jnp.float32, least / len(split), top_value / len(split)))
        level = level * jnp.repeat(heights, dims[axis_at] // blocks).reshape([-1 if axis == axis_at else 1 for axis in range(len(dims))])
    return level


def noise(own_key, shape, scale, reach, shards=(), kind=jnp.bfloat16):
    loudness = shard_levels(own_key, shape, shards, -0.22, 0.18) if shards else 1.0
    drawn = jax.random.normal(own_key, shape, jnp.float32) * scale * loudness
    return jnp.minimum(jnp.maximum(drawn, -reach), reach).astype(kind)


def heavy_noise(stream_key, dims, deviation, most, cuts, heavy, kind=jnp.bfloat16):
    array = deviation * jax.random.normal(stream_key, dims, jnp.float32)
    if cuts:
        array = array * shard_levels(stream_key, dims, cuts, -0.22, 0.18)
    return jnp.clip(strengthened(array, jax.random.fold_in(stream_key, 3), *heavy), -most, most).astype(kind)


def setup_inputs(seed: int = 0) -> dict:
    key_of = jax.random.split(jax.random.key(seed), 25)
    return {
        "slope_up": heavy_noise(key_of[0], (REPLICAS, WIDTH, INNER), 0.5, 4.0, ((0, 8), (2, 4)), (0, 1, 8, 2.0), jnp.float32),
        "slope_down": heavy_noise(key_of[1], (REPLICAS, INNER, WIDTH), 0.5, 4.0, ((0, 8), (1, 4)), (0, 2, 8, 2.0), jnp.float32),
        "slope_query": heavy_noise(key_of[2], (REPLICAS, WIDTH, ATTN), 0.5, 4.0, ((0, 8), (2, 4)), (0, 1, 8, 2.0), jnp.float32),
        "slope_key": heavy_noise(key_of[3], (REPLICAS, WIDTH, ATTN), 0.5, 4.0, ((0, 8), (2, 4)), (0, 1, 8, 2.0), jnp.float32),
        "slope_value": heavy_noise(key_of[4], (REPLICAS, WIDTH, ATTN), 0.5, 4.0, ((0, 8), (2, 4)), (0, 1, 8, 2.0), jnp.float32),
        "slope_mixed": heavy_noise(key_of[5], (REPLICAS, ATTN, WIDTH), 0.5, 4.0, ((0, 8), (1, 4)), (0, 2, 8, 2.0), jnp.float32),
        "slope_norm": heavy_noise(key_of[6], (REPLICAS, WIDTH), 1.0, 8.0, ((0, 8),), (0, 1, 8, 2.0), jnp.float32),
        "slope_bias": heavy_noise(key_of[7], (REPLICAS, WIDTH), 1.0, 8.0, ((0, 8),), (0, 1, 8, 2.0), jnp.float32),
        "param_up": heavy_noise(key_of[8], (WIDTH, INNER), WIDTH ** -0.5, 0.25, ((0, 8), (1, 4)), (1, 0, 8, 2.0), jnp.float32),
        "param_down": heavy_noise(key_of[9], (INNER, WIDTH), INNER ** -0.5, 0.125, ((0, 4), (1, 8)), (0, 1, 8, 2.0), jnp.float32),
        "param_query": heavy_noise(key_of[10], (WIDTH, ATTN), WIDTH ** -0.5, 0.25, ((0, 8), (1, 4)), (1, 0, 8, 2.0), jnp.float32),
        "param_key": heavy_noise(key_of[11], (WIDTH, ATTN), WIDTH ** -0.5, 0.25, ((0, 8), (1, 4)), (1, 0, 8, 2.0), jnp.float32),
        "param_value": heavy_noise(key_of[12], (WIDTH, ATTN), WIDTH ** -0.5, 0.25, ((0, 8), (1, 4)), (1, 0, 8, 2.0), jnp.float32),
        "param_mixed": heavy_noise(key_of[13], (ATTN, WIDTH), ATTN ** -0.5, 0.25, ((0, 4), (1, 8)), (0, 1, 8, 2.0), jnp.float32),
        "param_norm": jnp.clip(1.0 + 0.15 * jax.random.normal(key_of[14], (WIDTH,), jnp.float32), 0.25, 1.75),
        "param_bias": noise(key_of[15], (WIDTH,), 0.5, 3.0, ((0, 8),), jnp.float32),
        "state_up": jnp.clip(0.0001953125 + 0.0017578125 * jax.random.uniform(key_of[16], (WIDTH, INNER), jnp.float32) ** shard_levels(key_of[16], (WIDTH, INNER), ((0, 8), (1, 4)), -0.2, 0.2), 0.0001953125, 0.001953125),
        "state_down": jnp.clip(4.882812572759576e-05 + 0.0004394531 * jax.random.uniform(key_of[17], (INNER, WIDTH), jnp.float32) ** shard_levels(key_of[17], (INNER, WIDTH), ((0, 4), (1, 8)), -0.2, 0.2), 4.882812572759576e-05, 0.00048828125),
        "state_query": jnp.clip(0.0001953125 + 0.0017578125 * jax.random.uniform(key_of[18], (WIDTH, ATTN), jnp.float32) ** shard_levels(key_of[18], (WIDTH, ATTN), ((0, 8), (1, 4)), -0.2, 0.2), 0.0001953125, 0.001953125),
        "state_key": jnp.clip(0.0001953125 + 0.0017578125 * jax.random.uniform(key_of[19], (WIDTH, ATTN), jnp.float32) ** shard_levels(key_of[19], (WIDTH, ATTN), ((0, 8), (1, 4)), -0.2, 0.2), 0.0001953125, 0.001953125),
        "state_value": jnp.clip(0.0001953125 + 0.0017578125 * jax.random.uniform(key_of[20], (WIDTH, ATTN), jnp.float32) ** shard_levels(key_of[20], (WIDTH, ATTN), ((0, 8), (1, 4)), -0.2, 0.2), 0.0001953125, 0.001953125),
        "state_mixed": jnp.clip(0.0001953125 + 0.0017578125 * jax.random.uniform(key_of[21], (ATTN, WIDTH), jnp.float32) ** shard_levels(key_of[21], (ATTN, WIDTH), ((0, 4), (1, 8)), -0.2, 0.2), 0.0001953125, 0.001953125),
        "state_norm": jnp.clip(0.05 + 0.75 * jax.random.uniform(key_of[22], (WIDTH,), jnp.float32) ** shard_levels(key_of[22], (WIDTH,), ((0, 8),), -0.2, 0.2), 0.05, 0.8),
        "state_bias": jnp.clip(0.05 + 0.75 * jax.random.uniform(key_of[23], (WIDTH,), jnp.float32) ** shard_levels(key_of[23], (WIDTH,), ((0, 8),), -0.2, 0.2), 0.05, 0.8),
    }


learn_rate = 0.025
hold_rate = 0.7

def reference(slope_up, slope_down, slope_query, slope_key, slope_value, slope_mixed, slope_norm, slope_bias, param_up, param_down, param_query, param_key, param_value, param_mixed, param_norm, param_bias, state_up, state_down, state_query, state_key, state_value, state_mixed, state_norm, state_bias):
    mean_up = lax.optimization_barrier(jnp.sum(slope_up.astype(jnp.float32), axis=0)) * REPLICAS ** (-0.5)
    mean_down = lax.optimization_barrier(jnp.sum(slope_down.astype(jnp.float32), axis=0)) * REPLICAS ** (-0.5)
    mean_query = lax.optimization_barrier(jnp.sum(slope_query.astype(jnp.float32), axis=0)) * REPLICAS ** (-0.5)
    mean_key = lax.optimization_barrier(jnp.sum(slope_key.astype(jnp.float32), axis=0)) * REPLICAS ** (-0.5)
    mean_value = lax.optimization_barrier(jnp.sum(slope_value.astype(jnp.float32), axis=0)) * REPLICAS ** (-0.5)
    mean_mixed = lax.optimization_barrier(jnp.sum(slope_mixed.astype(jnp.float32), axis=0)) * REPLICAS ** (-0.5)
    mean_norm = lax.optimization_barrier(jnp.sum(slope_norm.astype(jnp.float32), axis=0)) * REPLICAS ** (-0.5)
    mean_bias = lax.optimization_barrier(jnp.sum(slope_bias.astype(jnp.float32), axis=0)) * REPLICAS ** (-0.5)
    ratio_up = jnp.sqrt(lax.optimization_barrier(jnp.sum(param_up * param_up, axis=1, keepdims=True))) * lax.rsqrt(lax.optimization_barrier(jnp.sum(mean_up * mean_up, axis=1, keepdims=True)) + 1e-06)
    mean_up = mean_up * ratio_up
    ratio_down = jnp.sqrt(lax.optimization_barrier(jnp.sum(param_down * param_down, axis=0, keepdims=True))) * lax.rsqrt(lax.optimization_barrier(jnp.sum(mean_down * mean_down, axis=0, keepdims=True)) + 1e-06)
    mean_down = mean_down * ratio_down
    ratio_query = jnp.sqrt(lax.optimization_barrier(jnp.sum(param_query * param_query, axis=1, keepdims=True))) * lax.rsqrt(lax.optimization_barrier(jnp.sum(mean_query * mean_query, axis=1, keepdims=True)) + 1e-06)
    mean_query = mean_query * ratio_query
    ratio_key = jnp.sqrt(lax.optimization_barrier(jnp.sum(param_key * param_key, axis=1, keepdims=True))) * lax.rsqrt(lax.optimization_barrier(jnp.sum(mean_key * mean_key, axis=1, keepdims=True)) + 1e-06)
    mean_key = mean_key * ratio_key
    ratio_value = jnp.sqrt(lax.optimization_barrier(jnp.sum(param_value * param_value, axis=1, keepdims=True))) * lax.rsqrt(lax.optimization_barrier(jnp.sum(mean_value * mean_value, axis=1, keepdims=True)) + 1e-06)
    mean_value = mean_value * ratio_value
    ratio_mixed = jnp.sqrt(lax.optimization_barrier(jnp.sum(param_mixed * param_mixed, axis=0, keepdims=True))) * lax.rsqrt(lax.optimization_barrier(jnp.sum(mean_mixed * mean_mixed, axis=0, keepdims=True)) + 1e-06)
    mean_mixed = mean_mixed * ratio_mixed
    state_new_up = hold_rate * state_up + (1.0 - hold_rate) * mean_up * mean_up
    next_up = param_up - learn_rate * mean_up * lax.rsqrt(state_new_up + 1e-06)
    state_new_down = hold_rate * state_down + (1.0 - hold_rate) * mean_down * mean_down
    next_down = param_down - learn_rate * mean_down * lax.rsqrt(state_new_down + 1e-06)
    state_new_query = hold_rate * state_query + (1.0 - hold_rate) * mean_query * mean_query
    next_query = param_query - learn_rate * mean_query * lax.rsqrt(state_new_query + 1e-06)
    state_new_key = hold_rate * state_key + (1.0 - hold_rate) * mean_key * mean_key
    next_key = param_key - learn_rate * mean_key * lax.rsqrt(state_new_key + 1e-06)
    state_new_value = hold_rate * state_value + (1.0 - hold_rate) * mean_value * mean_value
    next_value = param_value - learn_rate * mean_value * lax.rsqrt(state_new_value + 1e-06)
    state_new_mixed = hold_rate * state_mixed + (1.0 - hold_rate) * mean_mixed * mean_mixed
    next_mixed = param_mixed - learn_rate * mean_mixed * lax.rsqrt(state_new_mixed + 1e-06)
    state_new_norm = hold_rate * state_norm + (1.0 - hold_rate) * mean_norm * mean_norm
    next_norm = param_norm - learn_rate * mean_norm * lax.rsqrt(state_new_norm + 1e-06)
    state_new_bias = hold_rate * state_bias + (1.0 - hold_rate) * mean_bias * mean_bias
    next_bias = param_bias - learn_rate * mean_bias * lax.rsqrt(state_new_bias + 1e-06)
    half_up = next_up.astype(jnp.bfloat16)
    half_down = next_down.astype(jnp.bfloat16)
    half_query = next_query.astype(jnp.bfloat16)
    half_key = next_key.astype(jnp.bfloat16)
    half_value = next_value.astype(jnp.bfloat16)
    half_mixed = next_mixed.astype(jnp.bfloat16)
    half_norm = next_norm.astype(jnp.bfloat16)
    half_bias = next_bias.astype(jnp.bfloat16)
    return (half_up, half_down, half_query, half_key, half_value, half_mixed, half_norm, half_bias, next_up, next_down, next_query, next_key, next_value, next_mixed, next_norm, next_bias, state_new_up, state_new_down, state_new_query, state_new_key, state_new_value, state_new_mixed, state_new_norm, state_new_bias)
```

```python
import functools

import jax
import jax.numpy as jnp
from jax import lax
from jax.experimental import pallas as pl
from jax.experimental.pallas import tpu as pltpu
from jax.sharding import PartitionSpec as P

learn_rate = 0.025
hold_rate = 0.7
root = 9
MESH = pl.DeviceIdType.MESH


class Group:
    def __init__(self, members, rows):
        self.members = members
        self.rows = rows


GROUPS = (Group((0,), True), Group((1,), False), Group((5,), False), Group((2, 3, 4), True))
KINDS = (("A", "A", "B", "B"), ("A", "A", "A", "A"), ("A",), ("A", "B", "A", "B"))
CHUNKS = ((0, 0), (0, 2), (0, 3), (3, 1), (1, 2), (3, 0), (1, 0), (1, 3), (1, 1), (3, 2), (0, 1), (3, 3), (2, 0))
OWN = (0, 3, 1, 2)
SENT = ({"A": (4, 1, 0), "B": (1, 2, 0)}, {"A": (4, 2, 3), "B": (1, 4, 6)})
STEP = 16384
END = (
    ("E", 0, 0, 7), ("sY", 0, 0, 6), ("E", 0, 0, 5), ("sY", 0, 0, 4), ("E", 0, 0, 3), ("E", 0, 2, 6),
    ("sI", 0, 2, 6), ("E", 0, 2, 7), ("sI", 0, 2, 7), ("E", 0, 2, 4), ("E", 0, 2, 5), ("E", 0, 2, 2),
    ("E", 0, 2, 3), ("E", 0, 0, 1), ("E", 0, 3, 6), ("E", 0, 3, 7), ("E", 0, 3, 4), ("sY", 0, 0, 2),
    ("E", 0, 3, 5), ("E", 0, 3, 2), ("E", 0, 3, 3), ("sI", 0, 2, 4), ("E", 3, 1, 6), ("E", 3, 1, 7),
    ("E", 3, 1, 4), ("E", 3, 1, 5), ("E", 3, 1, 2), ("E", 3, 1, 3), ("E", 1, 2, 7), ("E", 1, 2, 5),
    ("E", 1, 2, 3), ("sY", 0, 0, 0), ("E", 1, 2, 1), ("V", 0, 0, 0), ("E", 3, 0, 7), ("E", 3, 0, 5),
    ("sI", 0, 2, 5), ("E", 3, 0, 3), ("E", 3, 0, 1), ("G", 0, 0, 6), ("E", 1, 0, 7), ("E", 1, 0, 5),
    ("E", 1, 0, 3), ("E", 1, 0, 1), ("E", 1, 3, 7), ("sY", 1, 2, 6), ("E", 1, 3, 5), ("E", 1, 3, 3),
    ("E", 1, 3, 1), ("sI", 0, 0, 6), ("E", 1, 1, 7), ("E", 1, 1, 5), ("G", 0, 0, 4), ("E", 1, 1, 3),
    ("E", 1, 1, 1), ("E", 3, 2, 7), ("E", 3, 2, 5), ("E", 3, 2, 3), ("sY", 1, 2, 4), ("E", 3, 2, 1),
    ("E", 0, 1, 7), ("E", 0, 1, 5), ("E", 0, 1, 3), ("sI", 0, 0, 4), ("E", 0, 1, 1), ("G", 0, 0, 2),
    ("E", 3, 3, 6), ("E", 3, 3, 7), ("E", 3, 3, 4), ("E", 3, 3, 5), ("E", 3, 3, 2), ("E", 3, 3, 3),
    ("sY", 1, 2, 2), ("E", 2, 0, 7), ("E", 2, 0, 5), ("E", 2, 0, 3), ("sI", 0, 0, 2), ("E", 2, 0, 1),
    ("sY", 1, 2, 0), ("sI", 0, 2, 2), ("G", 1, 2, 6), ("sY", 3, 0, 6), ("sI", 0, 2, 3), ("G", 1, 2, 4),
    ("sY", 3, 0, 4), ("sI", 0, 3, 6), ("G", 1, 2, 2), ("sY", 3, 0, 2), ("G", 0, 2, 1), ("sI", 0, 3, 7),
    ("sY", 0, 2, 0), ("G", 3, 0, 6), ("sY", 3, 0, 0), ("sI", 0, 3, 4), ("G", 3, 0, 4), ("sY", 1, 0, 6),
    ("sI", 0, 3, 5), ("G", 3, 0, 2), ("N", 0, 0, 0), ("n", 0, 0, 0), ("sY", 1, 0, 4), ("sI", 0, 3, 2),
    ("N", 0, 2, 0), ("n", 0, 2, 0), ("sY", 1, 0, 2), ("sI", 0, 3, 3), ("sY", 1, 0, 0), ("sI", 3, 1, 6),
    ("G", 1, 0, 6), ("U", 0, 0, 0), ("aY", 0, 0, 0), ("U", 0, 2, 0), ("sI", 3, 1, 7), ("G", 1, 0, 4),
    ("aY", 0, 0, 2), ("sI", 3, 1, 4), ("G", 1, 0, 2), ("sI", 3, 1, 5), ("aY", 0, 2, 0), ("sI", 3, 1, 2),
    ("G", 0, 3, 1), ("sY", 0, 3, 0), ("sI", 3, 1, 3), ("aY", 0, 0, 4), ("aI", 0, 0, 0), ("V", 0, 0, 1),
    ("aI", 0, 2, 0), ("sY", 1, 3, 6), ("aI", 0, 2, 1), ("sY", 1, 3, 4), ("N", 0, 3, 0), ("n", 0, 3, 0),
    ("sI", 1, 2, 6), ("sY", 1, 3, 2), ("sI", 1, 2, 4), ("sY", 1, 3, 0), ("G", 1, 3, 6), ("G", 3, 1, 1),
    ("sI", 1, 2, 2), ("U", 0, 3, 0), ("sY", 3, 1, 0), ("G", 1, 3, 4), ("aI", 0, 3, 0), ("aY", 0, 3, 0),
    ("G", 1, 3, 2), ("sY", 1, 1, 6), ("sI", 3, 0, 6), ("sY", 1, 1, 4), ("sI", 3, 0, 4), ("N", 3, 1, 0),
    ("n", 3, 1, 0), ("sI", 3, 0, 2), ("aY", 0, 0, 6), ("aI", 0, 3, 1), ("sY", 1, 1, 2), ("sI", 1, 0, 6),
    ("G", 1, 1, 6), ("U", 3, 1, 0), ("sY", 1, 1, 0), ("sI", 1, 0, 4), ("G", 1, 1, 4), ("sY", 3, 2, 6),
    ("sI", 1, 0, 2), ("sY", 3, 2, 4), ("sI", 1, 3, 6), ("G", 1, 1, 2), ("N", 1, 2, 0), ("sY", 3, 2, 2),
    ("sI", 1, 3, 4), ("sY", 3, 2, 0), ("G", 3, 2, 6), ("sY", 0, 1, 6), ("sI", 1, 3, 2), ("G", 3, 2, 4),
    ("sY", 0, 1, 4), ("sI", 1, 1, 6), ("G", 3, 2, 2), ("sY", 0, 1, 2), ("N", 3, 0, 0), ("n", 3, 0, 0),
    ("sI", 1, 1, 4), ("sY", 0, 1, 0), ("sI", 1, 1, 2), ("G", 0, 1, 6), ("aY", 3, 1, 0), ("aI", 3, 1, 0),
    ("G", 0, 1, 4), ("U", 3, 0, 0), ("aY", 3, 0, 0), ("sI", 3, 2, 6), ("G", 0, 1, 2), ("sY", 2, 0, 6),
    ("N", 1, 0, 0), ("sI", 3, 2, 4), ("sY", 2, 0, 4), ("sI", 3, 2, 2), ("aY", 3, 0, 2), ("aI", 3, 1, 1),
    ("N", 1, 3, 0), ("sI", 0, 1, 6), ("aY", 3, 0, 4), ("G", 2, 0, 6), ("sI", 0, 1, 4), ("sY", 2, 0, 2),
    ("G", 2, 0, 4), ("sY", 2, 0, 0), ("sI", 0, 1, 2), ("N", 1, 1, 0), ("V", 0, 0, 2), ("n", 1, 0, 0),
    ("aI", 3, 0, 0), ("sI", 3, 3, 6), ("U", 1, 2, 0), ("aY", 1, 2, 0), ("U", 1, 0, 0), ("aY", 1, 0, 0),
    ("U", 1, 3, 0), ("U", 1, 1, 0), ("aI", 1, 2, 0), ("G", 2, 0, 2), ("aY", 1, 2, 2), ("sI", 3, 3, 7),
    ("aY", 1, 0, 2), ("sI", 3, 3, 4), ("N", 3, 2, 0), ("n", 3, 2, 0), ("sI", 3, 3, 5), ("aY", 1, 3, 0),
    ("sI", 3, 3, 2), ("aY", 1, 1, 0), ("sI", 3, 3, 3), ("aY", 1, 3, 2), ("U", 3, 2, 0), ("aI", 1, 0, 0),
    ("sI", 2, 0, 6), ("aY", 1, 2, 4), ("sI", 2, 0, 4), ("aY", 1, 0, 4), ("N", 0, 1, 0), ("n", 0, 1, 0),
    ("sI", 2, 0, 2), ("aY", 3, 2, 0), ("aI", 1, 3, 0), ("aY", 1, 1, 2), ("U", 0, 1, 0), ("aY", 0, 1, 0),
    ("aI", 1, 1, 0), ("aY", 1, 2, 6), ("aI", 3, 2, 0), ("G", 3, 3, 1), ("sY", 3, 3, 0), ("aI", 0, 1, 0),
    ("aY", 3, 0, 6), ("aY", 1, 3, 4), ("aY", 3, 2, 2), ("N", 3, 3, 0), ("n", 3, 3, 0), ("aY", 1, 1, 4),
    ("aY", 0, 1, 2), ("aY", 1, 0, 6), ("N", 2, 0, 0), ("n", 2, 0, 0), ("U", 3, 3, 0), ("aI", 3, 3, 0),
    ("aY", 3, 3, 0), ("aY", 3, 2, 4), ("U", 2, 0, 0), ("aI", 2, 0, 0), ("aY", 1, 3, 6), ("aY", 2, 0, 0),
    ("aI", 3, 3, 1), ("aY", 1, 1, 6), ("aY", 3, 2, 6), ("aY", 0, 1, 4), ("aY", 0, 1, 6), ("aY", 2, 0, 4),
    ("aY", 2, 0, 2), ("aY", 2, 0, 6),
)
MID = (
    ("E", 0, 0, 7), ("sY", 0, 0, 6), ("E", 0, 0, 5), ("sY", 0, 0, 4), ("E", 0, 0, 3), ("E", 0, 0, 1),
    ("E", 1, 2, 7), ("E", 1, 2, 5), ("E", 1, 2, 3), ("sY", 0, 0, 2), ("E", 1, 2, 1), ("E", 3, 0, 7),
    ("E", 3, 0, 5), ("E", 3, 0, 3), ("E", 3, 0, 1), ("E", 1, 0, 7), ("E", 1, 0, 5), ("E", 1, 0, 3),
    ("E", 1, 0, 1), ("E", 1, 3, 7), ("E", 1, 3, 5), ("E", 1, 3, 3), ("sY", 0, 0, 0), ("E", 1, 3, 1),
    ("E", 1, 1, 7), ("E", 1, 1, 5), ("E", 1, 1, 3), ("E", 1, 1, 1), ("E", 3, 2, 7), ("E", 3, 2, 5),
    ("E", 3, 2, 3), ("E", 3, 2, 1), ("G", 0, 2, 6), ("sI", 0, 2, 6), ("E", 0, 1, 7), ("E", 0, 1, 5),
    ("sY", 1, 2, 6), ("E", 0, 1, 3), ("E", 0, 1, 1), ("E", 2, 0, 7), ("E", 2, 0, 5), ("V", 0, 0, 0),
    ("E", 2, 0, 3), ("E", 2, 0, 1), ("G", 0, 2, 7), ("sI", 0, 2, 7), ("sY", 1, 2, 4), ("G", 0, 2, 4),
    ("sI", 0, 2, 4), ("sY", 1, 2, 2), ("G", 0, 2, 0), ("sO", 0, 2, 0), ("G", 0, 2, 5), ("sI", 0, 2, 5),
    ("sY", 1, 2, 0), ("G", 0, 2, 1), ("sO", 0, 2, 1), ("G", 0, 0, 6), ("sI", 0, 0, 6), ("sY", 3, 0, 6),
    ("G", 0, 0, 4), ("sI", 0, 0, 4), ("sY", 3, 0, 4), ("sY", 3, 0, 2), ("G", 0, 0, 0), ("sO", 0, 0, 0),
    ("sY", 3, 0, 0), ("sY", 1, 0, 6), ("N", 0, 0, 0), ("n", 0, 0, 0), ("G", 0, 2, 3), ("sY", 0, 2, 2),
    ("G", 0, 3, 6), ("sI", 0, 3, 6), ("sY", 1, 0, 4), ("G", 0, 3, 7), ("sI", 0, 3, 7), ("U", 0, 0, 0),
    ("aY", 0, 0, 2), ("aO", 0, 0, 2), ("aI", 0, 0, 2), ("G", 0, 3, 4), ("sI", 0, 3, 4), ("sY", 1, 0, 2),
    ("G", 0, 3, 0), ("sO", 0, 3, 0), ("N", 0, 2, 0), ("n", 0, 2, 0), ("G", 0, 3, 5), ("sI", 0, 3, 5),
    ("sY", 1, 0, 0), ("G", 0, 3, 1), ("sO", 0, 3, 1), ("sY", 1, 3, 6), ("aO", 0, 0, 4), ("aY", 0, 0, 4),
    ("U", 0, 2, 0), ("aO", 0, 2, 2), ("aI", 0, 2, 2), ("G", 3, 1, 6), ("sI", 3, 1, 6), ("aY", 0, 2, 2),
    ("G", 3, 1, 7), ("sI", 3, 1, 7), ("G", 0, 3, 3), ("G", 3, 1, 4), ("sY", 0, 3, 2), ("sI", 3, 1, 4),
    ("aO", 0, 2, 4), ("G", 3, 1, 5), ("sI", 3, 1, 5), ("sY", 1, 3, 4), ("G", 3, 1, 0), ("sO", 3, 1, 0),
    ("sY", 1, 3, 2), ("G", 3, 1, 1), ("sO", 3, 1, 1), ("aO", 0, 2, 3), ("aI", 0, 2, 3), ("sY", 1, 3, 0),
    ("aI", 0, 0, 0), ("N", 0, 3, 0), ("n", 0, 3, 0), ("G", 3, 1, 3), ("sY", 3, 1, 2), ("aI", 0, 2, 0),
    ("aO", 0, 2, 5), ("aY", 0, 0, 0), ("aI", 0, 2, 1), ("sY", 1, 1, 6), ("aO", 0, 0, 6), ("U", 0, 3, 0),
    ("aO", 0, 3, 2), ("aI", 0, 3, 2), ("G", 1, 2, 6), ("sI", 1, 2, 6), ("aY", 0, 0, 6), ("aO", 0, 2, 6),
    ("N", 3, 1, 0), ("n", 3, 1, 0), ("G", 1, 2, 4), ("sI", 1, 2, 4), ("aY", 0, 3, 2), ("aO", 0, 2, 7),
    ("sY", 1, 1, 4), ("aO", 0, 3, 4), ("aI", 0, 3, 0), ("U", 3, 1, 0), ("sY", 1, 1, 2), ("aI", 3, 1, 2),
    ("G", 1, 2, 0), ("sO", 1, 2, 0), ("G", 3, 0, 6), ("sI", 3, 0, 6), ("G", 3, 0, 4), ("V", 0, 0, 1),
    ("sY", 1, 1, 0), ("N", 1, 2, 0), ("aO", 3, 1, 2), ("aI", 0, 3, 3), ("sY", 3, 2, 6), ("aO", 0, 3, 6),
    ("sI", 3, 0, 4), ("aO", 0, 3, 3), ("sY", 3, 2, 4), ("aI", 0, 3, 1), ("G", 3, 0, 0), ("sY", 3, 2, 2),
    ("G", 1, 0, 6), ("sO", 3, 0, 0), ("sI", 1, 0, 6), ("sY", 3, 2, 0), ("G", 1, 0, 4), ("aO", 0, 3, 5),
    ("sI", 1, 0, 4), ("sY", 0, 1, 6), ("N", 3, 0, 0), ("n", 3, 0, 0), ("aO", 3, 1, 4), ("sY", 0, 1, 4),
    ("aO", 0, 3, 7), ("G", 1, 3, 6), ("sI", 1, 3, 6), ("sY", 0, 1, 2), ("G", 1, 0, 0), ("sO", 1, 0, 0),
    ("G", 1, 3, 4), ("sI", 1, 3, 4), ("U", 3, 0, 0), ("aY", 3, 1, 2), ("aI", 3, 0, 2), ("N", 1, 0, 0),
    ("aO", 3, 0, 2), ("sY", 0, 1, 0), ("G", 1, 3, 0), ("sO", 1, 3, 0), ("G", 1, 1, 6), ("aY", 3, 0, 2),
    ("sI", 1, 1, 6), ("N", 1, 3, 0), ("G", 1, 1, 4), ("sY", 2, 0, 6), ("sI", 1, 1, 4), ("aO", 3, 0, 4),
    ("aO", 3, 1, 3), ("aI", 3, 1, 3), ("aY", 3, 0, 4), ("G", 1, 1, 0), ("sO", 1, 1, 0), ("sY", 2, 0, 4),
    ("aI", 3, 1, 0), ("G", 3, 2, 6), ("sY", 2, 0, 2), ("sI", 3, 2, 6), ("N", 1, 1, 0), ("n", 1, 0, 0),
    ("G", 3, 2, 4), ("aO", 3, 1, 5), ("sI", 3, 2, 4), ("sY", 2, 0, 0), ("aO", 3, 1, 6), ("aI", 3, 1, 1),
    ("U", 1, 2, 0), ("aY", 1, 2, 2), ("aO", 1, 2, 2), ("aI", 1, 2, 2), ("U", 1, 0, 0), ("aO", 1, 0, 2),
    ("U", 1, 3, 0), ("U", 1, 1, 0), ("G", 3, 2, 0), ("aY", 1, 0, 2), ("aI", 1, 0, 2), ("N", 3, 2, 0),
    ("n", 3, 2, 0), ("G", 0, 1, 6), ("sO", 3, 2, 0), ("sI", 0, 1, 6), ("aY", 1, 3, 2), ("G", 0, 1, 4),
    ("aO", 3, 1, 7), ("sI", 0, 1, 4), ("aY", 1, 1, 2), ("aO", 1, 3, 2), ("U", 3, 2, 0), ("aO", 1, 2, 4),
    ("aY", 1, 2, 4), ("aI", 3, 0, 0), ("G", 3, 3, 6), ("aO", 1, 0, 4), ("aY", 3, 0, 0), ("sI", 3, 3, 6),
    ("G", 0, 1, 0), ("aI", 1, 2, 0), ("sO", 0, 1, 0), ("aY", 1, 2, 0), ("N", 0, 1, 0), ("n", 0, 1, 0),
    ("aI", 1, 3, 2), ("V", 0, 0, 2), ("G", 3, 3, 7), ("aY", 1, 0, 4), ("aO", 1, 1, 2), ("G", 3, 3, 4),
    ("sI", 3, 3, 7), ("aY", 3, 0, 6), ("G", 3, 3, 0), ("sO", 3, 3, 0), ("G", 3, 3, 5), ("sI", 3, 3, 4),
    ("aY", 3, 2, 2), ("aO", 1, 2, 6), ("U", 0, 1, 0), ("sI", 3, 3, 5), ("aY", 1, 2, 6), ("aO", 3, 0, 6),
    ("aI", 1, 1, 2), ("aY", 1, 3, 4), ("G", 3, 3, 1), ("sO", 3, 3, 1), ("aI", 1, 0, 0), ("aY", 1, 0, 0),
    ("G", 2, 0, 6), ("aO", 1, 3, 4), ("sI", 2, 0, 6), ("G", 3, 3, 3), ("sY", 3, 3, 2), ("aO", 3, 2, 2),
    ("G", 2, 0, 4), ("sI", 2, 0, 4), ("aO", 1, 1, 4), ("aY", 1, 1, 4), ("aI", 3, 2, 2), ("aO", 0, 1, 2),
    ("aY", 0, 1, 2), ("aI", 1, 3, 0), ("aO", 1, 0, 6), ("aY", 1, 0, 6), ("G", 2, 0, 0), ("N", 3, 3, 0),
    ("n", 3, 3, 0), ("aI", 1, 1, 0), ("sO", 2, 0, 0), ("aY", 1, 3, 0), ("N", 2, 0, 0), ("n", 2, 0, 0),
    ("aI", 3, 2, 0), ("aO", 3, 2, 4), ("aY", 1, 1, 0), ("aI", 0, 1, 2), ("U", 3, 3, 0), ("aY", 1, 3, 6),
    ("aO", 1, 3, 6), ("aI", 0, 1, 0), ("U", 2, 0, 0), ("aO", 3, 3, 2), ("aY", 1, 1, 6), ("aI", 3, 3, 2),
    ("aO", 1, 1, 6), ("aY", 3, 2, 6), ("aI", 2, 0, 2), ("aO", 3, 2, 6), ("aY", 3, 2, 4), ("aO", 0, 1, 4),
    ("aY", 3, 2, 0), ("aI", 3, 3, 0), ("aO", 0, 1, 6), ("aY", 0, 1, 6), ("aO", 3, 3, 4), ("aY", 0, 1, 4),
    ("aI", 2, 0, 0), ("aO", 3, 3, 6), ("aY", 0, 1, 0), ("aO", 2, 0, 4), ("aY", 3, 3, 2), ("aI", 3, 3, 1),
    ("aO", 2, 0, 2), ("aY", 2, 0, 4), ("aO", 2, 0, 6), ("aY", 2, 0, 6), ("aO", 3, 3, 7), ("aY", 2, 0, 2),
    ("aI", 3, 3, 3), ("aO", 3, 3, 3), ("aY", 2, 0, 0), ("aO", 3, 3, 5),
)


def lanes_of(shapes, g, ref, i):
    n = len(GROUPS[g].members)
    w = shapes[g][1] // n
    return ref if n == 1 else ref.at[..., i * w : (i + 1) * w]


def finish(shapes, *refs):
    n = len(GROUPS)
    full, own, st = refs[0:n], refs[n : 2 * n], refs[2 * n : 3 * n]
    vectors = refs[3 * n : 3 * n + 6]
    halves, nexts, news = (refs[3 * n + 6 + 8 * k : 3 * n + 14 + 8 * k] for k in range(3))
    sem, vec_sem = refs[3 * n + 30 :]
    for g, group in enumerate(GROUPS):
        w = shapes[g][1]
        for i, a in enumerate(group.members):
            if group.rows:
                pltpu.make_async_copy(lanes_of(shapes, g, full[g], i), halves[a], sem.at[0, g]).start()
            else:
                for b in range(8):
                    dst = halves[a].at[:, b * w : (b + 1) * w]
                    pltpu.make_async_copy(full[g].at[b], dst, sem.at[0, g]).start()
            pltpu.make_async_copy(lanes_of(shapes, g, own[g], i), nexts[a], sem.at[1, g]).start()
            pltpu.make_async_copy(lanes_of(shapes, g, st[g], i), news[a], sem.at[2, g]).start()
    copies = []
    for i, dst in enumerate((*halves[6:], *nexts[6:], *news[6:])):
        copies.append(pltpu.make_async_copy(vectors[i], dst, vec_sem.at[i]))
        copies[-1].start()
    for g in range(n):
        for k, ref in enumerate((full[g], own[g], st[g])):
            pltpu.make_async_copy(ref, ref, sem.at[k, g]).wait()
    for c in copies:
        c.wait()


def kernel(replicas, models, limit, shapes, *refs):
    slopes, slope_norm, slope_bias = refs[0:6], refs[6], refs[7]
    params, param_norm, param_bias = refs[8:14], refs[14], refs[15]
    states, state_norm, state_bias = refs[16:22], refs[22], refs[23]
    groups = range(len(GROUPS))
    n = len(GROUPS)
    full, own, st = refs[24 : 24 + n], refs[24 + n : 24 + 2 * n], refs[24 + 2 * n : 24 + 3 * n]
    half_norm, half_bias, next_norm, next_bias, new_norm, new_bias = refs[24 + 3 * n : 30 + 3 * n]
    scratch = list(refs[30 + 3 * n :])
    take = lambda: [scratch.pop(0) for _ in groups]
    xin, enc, rec, sq, sqr = (take() for _ in range(5))
    vs, vown, vrec, vnext, vag, vh_norm, vh_bias = (scratch.pop(0) for _ in range(7))
    rs_s, rs_r, ag_s, ag_r, n_s, n_r, v_s, v_r, w_s, w_r = (scratch.pop(0) for _ in range(10))
    load_sem, own_sem, st_sem, vown_sem = scratch

    r = lax.axis_index("replica")
    m = lax.axis_index("model")
    y, z = lax.rem(r, 2), r // 2
    side = z // 2
    slab = [(p + side * (3 - 2 * p)) * 2 + (y if d == 0 else 1 - y) for p in range(4) for d in (0, 1)]

    scale = 2.0**13 / (limit * replicas)
    rate = replicas ** (-0.5)

    def encode(x):
        t = x * scale
        t2 = t * t
        t4 = t2 * t2
        return (t4 * t4 * t).astype(jnp.bfloat16)

    def decode(c):
        f = c.astype(jnp.float32)
        a = jnp.exp(jnp.log(jnp.abs(f)) * (1.0 / root)) * (1.0 / scale)
        return jnp.where(f < 0, -a, a)

    lanes = functools.partial(lanes_of, shapes)
    at = {k: i for i, k in enumerate(CHUNKS)}
    height = lambda g: shapes[g][0] // len(KINDS[g])
    rows = lambda g, c: pl.ds(c * height(g), height(g))

    def source(g, c, s):
        w = shapes[g][1]
        if GROUPS[g].rows:
            return xin[g].at[slab[s], rows(g, c)]
        return xin[g].at[rows(g, c), pl.ds(pl.multiple_of(slab[s] * w, w), w)]

    def loop(g, body):
        h, w = height(g), shapes[g][1]
        step = min(h, max(16, STEP // w // 16 * 16))
        while h % step:
            step -= 16
        lax.fori_loop(0, h // step, lambda i, c: (body(pl.ds(pl.multiple_of(i * step, step), step)), c)[1], 0)

    def remote(src, dst, s, d, peer, axis="replica"):
        return pltpu.make_async_remote_copy(
            src_ref=src, dst_ref=dst, send_sem=s, recv_sem=d, device_id={axis: peer}, device_id_type=MESH
        )

    def whole(ref, sem):
        pltpu.make_async_copy(ref, ref, sem).wait()

    barrier = pltpu.get_barrier_semaphore()
    for j in range(1, replicas):
        pl.semaphore_signal(barrier, inc=1, device_id={"replica": lax.rem(r + j, replicas)}, device_id_type=MESH)
    for j in range(1, models):
        pl.semaphore_signal(barrier, inc=1, device_id={"model": lax.rem(m + j, models)}, device_id_type=MESH)

    def chunk_of(g, c):
        return xin[g].at[:, rows(g, c)] if GROUPS[g].rows else xin[g].at[rows(g, c)]

    for g, c in CHUNKS:
        for i, a in enumerate(GROUPS[g].members):
            src = slopes[a].at[:, rows(g, c)] if GROUPS[g].rows else slopes[a].at[rows(g, c)]
            pltpu.make_async_copy(src, lanes(g, chunk_of(g, c), i), load_sem.at[at[g, c]]).start()
    for g in OWN:
        for i, a in enumerate(GROUPS[g].members):
            pltpu.make_async_copy(params[a], lanes(g, own[g], i), own_sem.at[g]).start()
            pltpu.make_async_copy(states[a], lanes(g, st[g], i), st_sem.at[g]).start()

    vs[0:1, :] = slope_norm[...]
    vs[1:2, :] = slope_bias[...]
    for g in groups:
        if not GROUPS[g].rows:
            sq[g][...] = jnp.zeros_like(sq[g])

    def rule(p, s, v):
        s = hold_rate * s + (1.0 - hold_rate) * v * v
        return p - learn_rate * v * lax.rsqrt(s + 1e-06), s

    def fold(x):
        total = x[:, 0:128]
        for k in range(128, x.shape[1], 128):
            total = total + x[:, k : k + 128]
        return jnp.sum(total, axis=1, keepdims=True)

    width = vs.shape[1] // replicas

    def vec_out(j):
        to = lax.rem(r + j, replicas)
        return remote(
            vs.at[:, pl.ds(pl.multiple_of(to * width, width), width)],
            vrec.at[j - 1], v_s.at[j - 1], v_r.at[j - 1], to,
        )

    def vec_back(j):
        return remote(vnext, vag.at[j - 1], w_s.at[j - 1], w_r.at[j - 1], lax.rem(r + j, replicas))

    def vec_start():
        pltpu.make_async_copy(vs.at[:, pl.ds(pl.multiple_of(r * width, width), width)], vown, vown_sem).start()
        for j in range(1, replicas):
            vec_out(j).start()

    def vec_update():
        pltpu.make_async_copy(vown, vown, vown_sem).wait()
        total = vown[...]
        for j in range(1, replicas):
            vec_out(j).wait_recv()
            total = total + vrec[j - 1]
        v = total * rate
        p, s = rule(param_norm[...], state_norm[...], v[0:1, :])
        next_norm[...] = p
        new_norm[...] = s
        vnext[0:1, :] = p
        p, s = rule(param_bias[...], state_bias[...], v[1:2, :])
        next_bias[...] = p
        new_bias[...] = s
        vnext[1:2, :] = p
        for j in range(1, replicas):
            vec_back(j).start()

    def vec_finish():
        vh_norm[pl.ds(r, 1), :] = vnext[0:1, :]
        vh_bias[pl.ds(r, 1), :] = vnext[1:2, :]
        for j in range(1, replicas):
            vec_back(j).wait_recv()
            at = lax.rem(r + replicas - j, replicas)
            vh_norm[pl.ds(at, 1), :] = vag[j - 1, 0:1, :]
            vh_bias[pl.ds(at, 1), :] = vag[j - 1, 1:2, :]
        half_norm[...] = vh_norm[...].astype(jnp.bfloat16)
        half_bias[...] = vh_bias[...].astype(jnp.bfloat16)

    def run(mid, order):
        mine = 1 if mid else 0
        peers = {"Y": z * 2 + (1 - y), "n": None}
        if mid:
            peers["sO"] = peers["aO"] = side * 6 + y
            peers["sI"] = peers["aI"] = (3 - z) * 2 + y
        else:
            peers["sI"] = peers["aI"] = (1 + side) * 2 + y
        peers["sY"] = peers["aY"] = z * 2 + (1 - y)
        done = set()

        def kind(g, c):
            return KINDS[g][c]

        def landing(g, c, by, s):
            if kind(g, c) == "A":
                return {"Y": 0, "O": 3, "I": 7}[by] + s // 2
            return {"Y": 10, "O": s - 2, "I": 6 + s}[by]

        def outgoing(g, c, op, s):
            p = s // 2
            if kind(g, c) == "A":
                if op == "sY":
                    return p
                return 3 + p if p else 4
            if op == "sY":
                return 6
            if not mid:
                return s - 2
            return s - 4 if p >= 2 else 4 + s

        def across(op, s):
            return (3 - s // 2) * 2 + s % 2 if mid and op[1] == "I" else s

        def send(op, g, c, s):
            by = {"sY": "Y", "sO": "I", "sI": "I" if mid else "O"}[op]
            slot = landing(g, c, by, across(op, s))
            return remote(
                enc[g].at[outgoing(g, c, op, s), rows(g, c)],
                rec[g].at[slot, rows(g, c)],
                rs_s.at[g],
                rs_r.at[at[g, c], slot],
                peers[op],
            )

        def gather(op, g, c, s):
            to = s + 1 if op == "aY" else across(op, s)
            ref = full[g].at[slab[s], rows(g, c)]
            link = {"aY": 0, "aI": 1, "aO": 2}[op]
            return remote(ref, ref, ag_s.at[at[g, c], link], ag_r.at[at[g, c], to], peers[op])

        def got(g, c, s):
            if s != mine * 2 and (g, c, s) not in done:
                done.add((g, c, s))
                ref = full[g].at[slab[s], rows(g, c)]
                whole(ref, ag_r.at[at[g, c], s])

        def arrived(g, c, by, s):
            slot = landing(g, c, by, s)
            ref = rec[g].at[slot, rows(g, c)]
            whole(ref, rs_r.at[at[g, c], slot])
            return ref

        def once(key, ref, sem):
            if key not in done:
                done.add(key)
                whole(ref, sem)

        def loaded(g, c):
            once(("load", g, c), chunk_of(g, c), load_sem.at[at[g, c]])

        def parts(g, c, s):
            loaded(g, c)
            by = []
            a, p = kind(g, c) == "A", s // 2
            if a or s == mine * 2:
                by.append("Y")
            if mid and p >= 1:
                by.append("O")
            if p == mine or (mid and p == 0):
                by.append("I")
            return [arrived(g, c, b, s) for b in by]

        def encode_op(g, c, s, op):
            loaded(g, c)
            src, dst = source(g, c, s), enc[g].at[outgoing(g, c, op, s), rows(g, c)]

            def body(d):
                dst[d, :] = encode(src[d, :])

            loop(g, body)

        def add_op(g, c, s):
            src = source(g, c, s)
            op = "sY" if s // 2 == mine else "sO" if mid and s < 2 else "sI"
            dst = enc[g].at[outgoing(g, c, op, s), rows(g, c)]
            got = parts(g, c, s)

            def body(d):
                total = src[d, :]
                for ref in got:
                    total = total + decode(ref[d, :])
                dst[d, :] = encode(total)

            loop(g, body)

        def mean_op(g, c):
            acc = source(g, c, mine * 2)
            got = parts(g, c, mine * 2)
            once(("own", g), own[g], own_sem.at[g])
            held = own[g].at[rows(g, c)]
            k = len(GROUPS[g].members)
            w = shapes[g][1] // k

            def mean(d):
                total = acc[d, :]
                for ref in got:
                    total = total + decode(ref[d, :])
                v = total * rate
                acc[d, :] = v
                return v

            if GROUPS[g].rows:
                sums = sq[g].at[rows(g, c)]

                def body(d):
                    v, p = mean(d), held[d, :]
                    v, p = v * v, p * p
                    lane = lax.broadcasted_iota(jnp.int32, (v.shape[0], 128), 1)
                    out = jnp.zeros((v.shape[0], 128), jnp.float32)
                    for i in range(k):
                        cols = slice(i * w, (i + 1) * w)
                        out = jnp.where(lane == 2 * i, fold(p[:, cols]), out)
                        out = jnp.where(lane == 2 * i + 1, fold(v[:, cols]), out)
                    sums[d, :] = out

            else:

                def body(d):
                    v, p = mean(d), held[d, :]
                    sq[g][0] += jnp.sum((p * p).reshape(-1, 8, w), axis=0)
                    sq[g][1] += jnp.sum((v * v).reshape(-1, 8, w), axis=0)

            loop(g, body)

        def norms(g, c, j):
            if GROUPS[g].rows:
                src, dst = sq[g].at[rows(g, c)], sqr[g].at[j - 1, rows(g, c)]
            else:
                src, dst = sq[g], sqr[g].at[j - 1]
            return remote(src, dst, n_s.at[at[g, c], j - 1], n_r.at[at[g, c], j - 1], lax.rem(m + j, models), "model")

        def update_op(g, c):
            first = c if GROUPS[g].rows else 0
            for j in range(1, models):
                if ("norm", g, first, j) not in done:
                    done.add(("norm", g, first, j))
                    norms(g, first, j).wait_recv()
            once(("st", g), st[g], st_sem.at[g])
            acc, half = source(g, c, mine * 2), full[g].at[slab[mine * 2], rows(g, c)]
            held, hold = own[g].at[rows(g, c)], st[g].at[rows(g, c)]
            k = len(GROUPS[g].members)
            w = shapes[g][1] // k

            def put(d, cols, t):
                p, s = rule(held[d, cols], hold[d, cols], acc[d, cols] * t)
                held[d, cols] = p
                hold[d, cols] = s
                half[d, cols] = p.astype(jnp.bfloat16)

            if GROUPS[g].rows:
                sums = [sq[g].at[rows(g, c)]] + [sqr[g].at[j, rows(g, c)] for j in range(models - 1)]

                def body(d):
                    total = sums[0][d, :]
                    for ref in sums[1:]:
                        total = total + ref[d, :]
                    lane = lax.broadcasted_iota(jnp.int32, total.shape, 1)
                    pick = lambda i: jnp.sum(jnp.where(lane == i, total, 0.0), axis=1, keepdims=True)
                    for i in range(k):
                        t = jnp.sqrt(pick(2 * i)) * lax.rsqrt(pick(2 * i + 1) + 1e-06)
                        put(d, slice(i * w, (i + 1) * w), t)

            else:
                total = sq[g][...]
                for j in range(models - 1):
                    total = total + sqr[g][j]
                total = jnp.sum(total, axis=1, keepdims=True)
                t = jnp.sqrt(total[0]) * lax.rsqrt(total[1] + 1e-06)

                def body(d):
                    put(d, slice(None), t)

            loop(g, body)

        met = False
        for op, g, c, s in order:
            if op not in ("E", "G") and not met:
                met = True
                pl.semaphore_wait(barrier, replicas + models - 2)
            if op == "E":
                encode_op(g, c, s, "sY" if kind(g, c) == "A" else "sI")
            elif op == "G":
                add_op(g, c, s)
            elif op in ("sY", "sI", "sO"):
                send(op, g, c, s).start()
            elif op == "N":
                mean_op(g, c)
            elif op == "n":
                for j in range(1, models):
                    norms(g, c, j).start()
            elif op == "U":
                update_op(g, c)
            elif op == "V":
                (vec_start, vec_update, vec_finish)[s]()
            else:
                got(g, c, s)
                gather(op, g, c, s).start()

        for g, c in CHUNKS:
            for s in range(8):
                got(g, c, s)
        for g in groups:
            whole(enc[g], rs_s.at[g])
        for g, c in CHUNKS:
            for link, count in enumerate(SENT[mid][kind(g, c)]):
                if count:
                    whole(full[g].at[pl.ds(0, count), rows(g, c)], ag_s.at[at[g, c], link])
            if GROUPS[g].rows or c == 0:
                for j in range(1, models):
                    norms(g, c, j).wait_send()
        for j in range(1, replicas):
            vec_out(j).wait_send()
            vec_back(j).wait_send()

    end = jnp.logical_or(z == 0, z == 3)

    @pl.when(end)
    def _():
        run(False, END)

    @pl.when(jnp.logical_not(end))
    def _():
        run(True, MID)


def fused(replicas, models, shapes, *args):
    slopes, params = args[0:6], args[8:14]
    f32, bf16 = jnp.float32, jnp.bfloat16
    vec = args[6].shape[1]
    width = vec // replicas
    row = lambda a: a.reshape(1, -1)
    by_rows = [a in g.members and g.rows for a in range(6) for g in GROUPS if a in g.members]
    cut = lambda a, rows: a.reshape(replicas, -1, a.shape[-1]) if rows else a[0]
    args = (
        *(cut(a, rows) for a, rows in zip(slopes, by_rows)), *args[6:14],
        row(args[14]), row(args[15]), *args[16:22], row(args[22]), row(args[23]),
    )
    S = jax.ShapeDtypeStruct
    n, chunks = len(GROUPS), len(CHUNKS)
    held = [((replicas, *s), bf16) for s in shapes] + [(s, f32) for s in shapes] * 2
    held += [((replicas, width), bf16)] * 2 + [((1, width), f32)] * 4
    ANY, VM = pl.BlockSpec(memory_space=pl.ANY), pl.BlockSpec(memory_space=pltpu.VMEM)
    part = [ANY] * 6 + [VM] * 2
    scratch = [
        pltpu.VMEM((replicas, *s) if g.rows else (s[0], s[1] * replicas), f32) for g, s in zip(GROUPS, shapes)
    ]
    scratch += [pltpu.VMEM((7, *s), bf16) for s in shapes]
    scratch += [pltpu.VMEM((11 if "B" in k else 9, *s), bf16) for k, s in zip(KINDS, shapes)]
    sq = [(s[0], 128) if g.rows else (2, 8, s[1]) for g, s in zip(GROUPS, shapes)]
    scratch += [pltpu.VMEM(s, f32) for s in sq]
    scratch += [pltpu.VMEM((models - 1, *s), f32) for s in sq]
    scratch += [
        pltpu.VMEM((2, vec), f32),
        pltpu.VMEM((2, width), f32),
        pltpu.VMEM((replicas - 1, 2, width), f32),
        pltpu.VMEM((2, width), f32),
        pltpu.VMEM((replicas - 1, 2, width), f32),
        pltpu.VMEM((replicas, width), f32),
        pltpu.VMEM((replicas, width), f32),
    ]
    dma = pltpu.SemaphoreType.DMA
    scratch += [dma((n,)), dma((chunks, 11)), dma((chunks, 3)), dma((chunks, 8))]
    scratch += [dma((chunks, models - 1))] * 2 + [dma((replicas - 1,))] * 4
    scratch += [dma((chunks,))] + [dma((n,))] * 2 + [dma(())]
    out = pl.pallas_call(
        functools.partial(kernel, replicas, models, 4.0, shapes),
        out_shape=[pltpu.VMEM(*h) for h in held],
        in_specs=part * 3,
        out_specs=[VM] * len(held),
        scratch_shapes=scratch,
        compiler_params=pltpu.CompilerParams(
            collective_id=0, has_side_effects=True, vmem_limit_bytes=54 * 1024 * 1024
        ),
    )(*args)
    outs = [
        S((replicas, a.shape[1] // replicas, a.shape[2]) if rows else a.shape[1:], bf16)
        for a, rows in zip(slopes, by_rows)
    ]
    outs += [S((replicas, width), bf16)] * 2
    for _ in range(2):
        outs += [S(a.shape, f32) for a in params] + [S((1, width), f32)] * 2
    out = pl.pallas_call(
        functools.partial(finish, shapes),
        out_shape=outs,
        in_specs=[VM] * len(held),
        out_specs=[ANY] * len(outs),
        scratch_shapes=[dma((3, n)), dma((6,))],
        compiler_params=pltpu.CompilerParams(vmem_limit_bytes=1024 * 1024),
    )(*out)
    flat = lambda a: a.reshape(-1)
    return (
        *(a.reshape(-1, a.shape[-1]) for a in out[0:6]), flat(out[6]), flat(out[7]),
        *out[8:14], flat(out[14]), flat(out[15]),
        *out[16:22], flat(out[22]), flat(out[23]),
    )


def plain(
    slope_up,
    slope_down,
    slope_query,
    slope_key,
    slope_value,
    slope_mixed,
    slope_norm,
    slope_bias,
    param_up,
    param_down,
    param_query,
    param_key,
    param_value,
    param_mixed,
    param_norm,
    param_bias,
    state_up,
    state_down,
    state_query,
    state_key,
    state_value,
    state_mixed,
    state_norm,
    state_bias,
):
    mean_up, mean_down, mean_query, mean_key, mean_value, mean_mixed = (
        lax.psum_scatter(slope_up[0], "replica", scatter_dimension=0, tiled=True),
        lax.psum_scatter(slope_down[0], "replica", scatter_dimension=1, tiled=True),
        lax.psum_scatter(slope_query[0], "replica", scatter_dimension=0, tiled=True),
        lax.psum_scatter(slope_key[0], "replica", scatter_dimension=0, tiled=True),
        lax.psum_scatter(slope_value[0], "replica", scatter_dimension=0, tiled=True),
        lax.psum_scatter(slope_mixed[0], "replica", scatter_dimension=1, tiled=True),
    )
    whole_norm, whole_bias = lax.psum((slope_norm[0], slope_bias[0]), "replica")
    place = lax.axis_index("replica")
    mean_norm = lax.dynamic_slice_in_dim(
        whole_norm, place * param_norm.shape[0], param_norm.shape[0]
    )
    mean_bias = lax.dynamic_slice_in_dim(
        whole_bias, place * param_bias.shape[0], param_bias.shape[0]
    )
    mean_rate = lax.axis_size("replica") ** (-0.5)
    mean_up = mean_up * mean_rate
    mean_down = mean_down * mean_rate
    mean_query = mean_query * mean_rate
    mean_key = mean_key * mean_rate
    mean_value = mean_value * mean_rate
    mean_mixed = mean_mixed * mean_rate
    mean_norm = mean_norm * mean_rate
    mean_bias = mean_bias * mean_rate
    (
        own_up,
        own_down,
        own_query,
        own_key,
        own_value,
        own_mixed,
        slope_up_norm,
        slope_down_norm,
        slope_query_norm,
        slope_key_norm,
        slope_value_norm,
        slope_mixed_norm,
    ) = lax.psum(
        (
            jnp.sum(param_up * param_up, axis=1, keepdims=True),
            jnp.sum(param_down * param_down, axis=0, keepdims=True),
            jnp.sum(param_query * param_query, axis=1, keepdims=True),
            jnp.sum(param_key * param_key, axis=1, keepdims=True),
            jnp.sum(param_value * param_value, axis=1, keepdims=True),
            jnp.sum(param_mixed * param_mixed, axis=0, keepdims=True),
            jnp.sum(mean_up * mean_up, axis=1, keepdims=True),
            jnp.sum(mean_down * mean_down, axis=0, keepdims=True),
            jnp.sum(mean_query * mean_query, axis=1, keepdims=True),
            jnp.sum(mean_key * mean_key, axis=1, keepdims=True),
            jnp.sum(mean_value * mean_value, axis=1, keepdims=True),
            jnp.sum(mean_mixed * mean_mixed, axis=0, keepdims=True),
        ),
        "model",
    )
    mean_up = mean_up * (jnp.sqrt(own_up) * lax.rsqrt(slope_up_norm + 1e-06))
    mean_down = mean_down * (jnp.sqrt(own_down) * lax.rsqrt(slope_down_norm + 1e-06))
    mean_query = mean_query * (jnp.sqrt(own_query) * lax.rsqrt(slope_query_norm + 1e-06))
    mean_key = mean_key * (jnp.sqrt(own_key) * lax.rsqrt(slope_key_norm + 1e-06))
    mean_value = mean_value * (jnp.sqrt(own_value) * lax.rsqrt(slope_value_norm + 1e-06))
    mean_mixed = mean_mixed * (jnp.sqrt(own_mixed) * lax.rsqrt(slope_mixed_norm + 1e-06))
    state_new_up = hold_rate * state_up + (1.0 - hold_rate) * mean_up * mean_up
    next_up = param_up - learn_rate * mean_up * lax.rsqrt(state_new_up + 1e-06)
    state_new_down = hold_rate * state_down + (1.0 - hold_rate) * mean_down * mean_down
    next_down = param_down - learn_rate * mean_down * lax.rsqrt(state_new_down + 1e-06)
    state_new_query = hold_rate * state_query + (1.0 - hold_rate) * mean_query * mean_query
    next_query = param_query - learn_rate * mean_query * lax.rsqrt(state_new_query + 1e-06)
    state_new_key = hold_rate * state_key + (1.0 - hold_rate) * mean_key * mean_key
    next_key = param_key - learn_rate * mean_key * lax.rsqrt(state_new_key + 1e-06)
    state_new_value = hold_rate * state_value + (1.0 - hold_rate) * mean_value * mean_value
    next_value = param_value - learn_rate * mean_value * lax.rsqrt(state_new_value + 1e-06)
    state_new_mixed = hold_rate * state_mixed + (1.0 - hold_rate) * mean_mixed * mean_mixed
    next_mixed = param_mixed - learn_rate * mean_mixed * lax.rsqrt(state_new_mixed + 1e-06)
    state_new_norm = hold_rate * state_norm + (1.0 - hold_rate) * mean_norm * mean_norm
    next_norm = param_norm - learn_rate * mean_norm * lax.rsqrt(state_new_norm + 1e-06)
    state_new_bias = hold_rate * state_bias + (1.0 - hold_rate) * mean_bias * mean_bias
    next_bias = param_bias - learn_rate * mean_bias * lax.rsqrt(state_new_bias + 1e-06)
    half_up, half_down, half_query, half_key, half_value, half_mixed, half_norm, half_bias = (
        lax.all_gather(next_up.astype(jnp.bfloat16), "replica", axis=0, tiled=True),
        lax.all_gather(next_down.astype(jnp.bfloat16), "replica", axis=1, tiled=True),
        lax.all_gather(next_query.astype(jnp.bfloat16), "replica", axis=0, tiled=True),
        lax.all_gather(next_key.astype(jnp.bfloat16), "replica", axis=0, tiled=True),
        lax.all_gather(next_value.astype(jnp.bfloat16), "replica", axis=0, tiled=True),
        lax.all_gather(next_mixed.astype(jnp.bfloat16), "replica", axis=1, tiled=True),
        lax.all_gather(next_norm.astype(jnp.bfloat16), "replica", axis=0, tiled=True),
        lax.all_gather(next_bias.astype(jnp.bfloat16), "replica", axis=0, tiled=True),
    )
    return (
        half_up,
        half_down,
        half_query,
        half_key,
        half_value,
        half_mixed,
        half_norm,
        half_bias,
        next_up,
        next_down,
        next_query,
        next_key,
        next_value,
        next_mixed,
        next_norm,
        next_bias,
        state_new_up,
        state_new_down,
        state_new_query,
        state_new_key,
        state_new_value,
        state_new_mixed,
        state_new_norm,
        state_new_bias,
    )


def solution(mesh):
    replicas, models = mesh.shape["replica"], mesh.shape["model"]

    def local(*args):
        if replicas != 2**3 or any(a.shape[k] % 128 for a in args[8:14] for k in (0, 1)):
            return plain(*args)
        shapes = []
        for g, kinds in zip(GROUPS, KINDS):
            h, w = args[8 + g.members[0]].shape
            shapes.append((h, w * len(g.members)))
            if h % (16 * len(kinds)) or (w != 128 and not g.rows):
                return plain(*args)
        if args[14].shape[0] % 128:
            return plain(*args)
        return fused(replicas, models, shapes, *args)

    placed = (
        P("replica", None, "model"),
        P("replica", "model", None),
        P("replica", None, "model"),
        P("replica", None, "model"),
        P("replica", None, "model"),
        P("replica", "model", None),
        P("replica", None),
        P("replica", None),
        P("replica", "model"),
        P("model", "replica"),
        P("replica", "model"),
        P("replica", "model"),
        P("replica", "model"),
        P("model", "replica"),
        P("replica"),
        P("replica"),
        P("replica", "model"),
        P("model", "replica"),
        P("replica", "model"),
        P("replica", "model"),
        P("replica", "model"),
        P("model", "replica"),
        P("replica"),
        P("replica"),
    )
    return jax.shard_map(
        local,
        mesh=mesh,
        in_specs=placed,
        out_specs=(
            P(None, "model"),
            P("model", None),
            P(None, "model"),
            P(None, "model"),
            P(None, "model"),
            P("model", None),
            P(),
            P(),
            P("replica", "model"),
            P("model", "replica"),
            P("replica", "model"),
            P("replica", "model"),
            P("replica", "model"),
            P("model", "replica"),
            P("replica"),
            P("replica"),
            P("replica", "model"),
            P("model", "replica"),
            P("replica", "model"),
            P("replica", "model"),
            P("replica", "model"),
            P("model", "replica"),
            P("replica"),
            P("replica"),
        ),
        check_vma=False,
    )
```

```python
import functools

import jax
import jax.numpy as jnp
from jax import lax
from jax.experimental import pallas as pl
from jax.experimental.pallas import tpu as pltpu
from jax.sharding import PartitionSpec as P

learn_rate = 0.025
hold_rate = 0.7
root = 9
MESH = pl.DeviceIdType.MESH


class Group:
    def __init__(self, members, rows):
        self.members = members
        self.rows = rows


GROUPS = (Group((0,), True), Group((1,), False), Group((5,), False), Group((2, 3, 4), True))
A, B = 0, 1
E, G, N, X, U, V, SY, SI, SO, AY, AI, AO = range(12)
SIZES = ((2, 2, 2, 2), (4, 4), (8,), (1, 2, 2, 2, 1))
SUMS = ((B, A, B, A), (A, A), (A,), (A, A, A, B, B))
BACK = ((A, B, A, B), (A, A), (B,), (B, B, A, A, B))
CHUNKS = ((3, 0), (3, 4), (0, 3), (0, 1), (2, 0), (3, 3), (1, 0), (1, 1), (3, 2), (0, 0), (0, 2), (3, 1))
OWN = (3, 0, 2, 1)
SENT = (((4, 1, 0), (1, 2, 0)), ((4, 2, 3), (1, 4, 6)))
STEP = 16384
END = (
    (E, 3, 0, 5), (SY, 3, 0, 4), (E, 3, 4, 7), (SI, 3, 4, 7), (E, 3, 4, 4), (SI, 3, 4, 4),
    (E, 3, 0, 3), (SY, 3, 0, 2), (E, 3, 4, 2), (E, 3, 4, 3), (E, 3, 4, 5), (SI, 3, 4, 5),
    (E, 3, 0, 7), (SY, 3, 0, 6), (E, 3, 4, 6), (E, 3, 0, 1), (SY, 3, 0, 0), (E, 0, 3, 3),
    (SI, 3, 4, 6), (E, 0, 3, 5), (E, 0, 3, 1), (E, 0, 3, 7), (SY, 0, 3, 6), (E, 2, 0, 5),
    (SI, 3, 4, 2), (V, 0, 0, 0), (E, 0, 1, 3), (E, 0, 1, 7), (SY, 0, 1, 6), (E, 2, 0, 3),
    (SI, 3, 4, 3), (E, 0, 1, 5), (E, 3, 3, 4), (E, 3, 3, 5), (E, 3, 3, 7), (SI, 3, 3, 7),
    (G, 3, 0, 4), (E, 1, 0, 3), (E, 3, 3, 6), (E, 1, 0, 5), (SI, 3, 0, 4), (G, 3, 0, 2),
    (SY, 0, 3, 4), (E, 0, 1, 1), (E, 3, 3, 2), (E, 2, 0, 7), (G, 3, 0, 6), (E, 3, 3, 3),
    (E, 1, 1, 5), (SI, 3, 0, 6), (E, 2, 0, 1), (E, 1, 0, 7), (E, 1, 1, 3), (SI, 3, 3, 6),
    (SY, 2, 0, 6), (E, 0, 0, 5), (E, 0, 0, 4), (E, 1, 1, 7), (SI, 3, 0, 2), (E, 3, 2, 5),
    (E, 0, 0, 2), (E, 0, 0, 6), (G, 0, 3, 6), (E, 1, 0, 1), (E, 0, 0, 3), (E, 1, 1, 1),
    (SI, 0, 3, 6), (SY, 1, 0, 6), (E, 0, 2, 4), (E, 3, 2, 3), (E, 0, 2, 5), (E, 3, 2, 7),
    (SI, 0, 0, 6), (E, 3, 2, 1), (E, 0, 2, 7), (G, 0, 1, 6), (E, 0, 0, 7), (E, 0, 2, 3),
    (SY, 0, 3, 2), (E, 0, 2, 6), (E, 0, 2, 2), (E, 3, 1, 5), (E, 3, 1, 7), (E, 3, 1, 3),
    (SI, 0, 1, 6), (E, 3, 1, 1), (G, 0, 3, 4), (G, 3, 4, 1), (SI, 0, 3, 4), (G, 2, 0, 6),
    (SY, 3, 4, 0), (SI, 2, 0, 6), (SY, 0, 3, 0), (SY, 0, 1, 4), (SI, 0, 0, 7), (G, 1, 0, 6),
    (G, 3, 3, 1), (SY, 3, 2, 6), (SI, 1, 0, 6), (G, 0, 3, 2), (N, 3, 0, 0), (X, 3, 0, 0),
    (N, 3, 4, 0), (X, 3, 4, 0), (SY, 1, 1, 6), (SI, 0, 3, 2), (SY, 0, 1, 0), (G, 0, 1, 4),
    (U, 3, 0, 0), (U, 3, 4, 0), (AI, 3, 0, 0), (G, 3, 2, 6), (N, 0, 3, 0), (X, 0, 3, 0),
    (SY, 3, 3, 0), (AI, 3, 4, 0), (SI, 0, 1, 4), (SY, 0, 1, 2), (SI, 0, 2, 6), (G, 1, 1, 6),
    (SY, 2, 0, 0), (SI, 1, 1, 6), (U, 0, 3, 0), (N, 0, 1, 0), (X, 0, 1, 0), (SY, 2, 0, 4),
    (SI, 0, 2, 7), (V, 0, 0, 1), (N, 3, 3, 0), (X, 3, 3, 0), (SY, 2, 0, 2), (G, 0, 1, 2),
    (SY, 1, 0, 4), (SI, 0, 1, 2), (U, 0, 1, 0), (N, 2, 0, 0), (X, 2, 0, 0), (SY, 1, 1, 4),
    (U, 3, 3, 0), (SI, 3, 2, 6), (G, 0, 0, 1), (G, 2, 0, 4), (AI, 0, 3, 0), (G, 2, 0, 2),
    (SY, 1, 0, 2), (SI, 3, 3, 5), (U, 2, 0, 0), (SI, 3, 3, 4), (G, 1, 0, 4), (SI, 2, 0, 4),
    (SY, 1, 0, 0), (SI, 2, 0, 2), (SI, 3, 3, 2), (G, 1, 1, 4), (SY, 1, 1, 2), (SI, 1, 0, 4),
    (AI, 0, 1, 0), (G, 1, 0, 2), (SY, 3, 2, 4), (SI, 3, 3, 3), (N, 1, 0, 0), (SY, 1, 1, 0),
    (AI, 3, 3, 0), (SY, 3, 1, 6), (SI, 1, 1, 4), (G, 1, 1, 2), (SI, 1, 0, 2), (G, 0, 2, 1),
    (G, 3, 2, 4), (SY, 3, 2, 2), (SY, 3, 2, 0), (SI, 1, 1, 2), (SY, 0, 0, 0), (N, 1, 1, 0),
    (X, 1, 0, 0), (SY, 0, 2, 0), (G, 3, 1, 6), (SI, 3, 1, 6), (G, 3, 2, 2), (SY, 3, 1, 4),
    (N, 3, 2, 0), (X, 3, 2, 0), (SY, 3, 1, 0), (U, 1, 0, 0), (U, 1, 1, 0), (N, 0, 0, 0),
    (X, 0, 0, 0), (AI, 2, 0, 0), (SY, 3, 1, 2), (AY, 3, 4, 0), (SI, 3, 2, 4), (N, 0, 2, 0),
    (X, 0, 2, 0), (U, 3, 2, 0), (AY, 3, 0, 0), (G, 3, 1, 4), (SI, 0, 0, 5), (AY, 0, 3, 0),
    (AY, 0, 1, 0), (U, 0, 0, 0), (SI, 0, 0, 4), (G, 3, 1, 2), (V, 0, 0, 2), (AY, 2, 0, 0),
    (U, 0, 2, 0), (AI, 3, 4, 1), (AY, 3, 3, 0), (AI, 3, 0, 1), (AI, 0, 3, 1), (AY, 1, 0, 0),
    (SI, 3, 2, 2), (AY, 1, 1, 0), (AI, 0, 1, 1), (AI, 2, 0, 1), (AY, 3, 2, 0), (AI, 1, 0, 0),
    (N, 3, 1, 0), (X, 3, 1, 0), (SI, 0, 2, 5), (AY, 3, 3, 6), (U, 3, 1, 0), (AY, 3, 3, 2),
    (SI, 0, 0, 3), (AY, 1, 0, 2), (AI, 1, 1, 0), (AY, 0, 0, 0), (SI, 0, 0, 2), (AY, 0, 2, 0),
    (SI, 0, 2, 3), (AY, 1, 1, 2), (SI, 0, 2, 2), (AY, 3, 3, 4), (SI, 0, 2, 4), (SI, 3, 1, 4),
    (AY, 3, 2, 2), (AY, 3, 1, 0), (AI, 0, 0, 0), (AY, 1, 0, 4), (AI, 3, 2, 0), (AY, 1, 1, 4),
    (AI, 0, 2, 0), (SI, 3, 1, 2), (AY, 3, 2, 4), (AI, 3, 1, 1), (AI, 3, 1, 0), (AY, 0, 0, 2),
    (AY, 1, 0, 6), (AY, 1, 1, 6), (AY, 0, 0, 4), (AY, 3, 2, 6), (AY, 0, 0, 6), (AY, 0, 2, 2),
    (AY, 0, 2, 6), (AY, 0, 2, 4),
)
MID = (
    (E, 3, 0, 1), (SY, 3, 0, 0), (E, 3, 0, 3), (SY, 3, 0, 2), (E, 3, 0, 5), (E, 3, 0, 7),
    (E, 0, 3, 5), (E, 0, 3, 1), (SY, 3, 0, 6), (E, 0, 3, 3), (E, 0, 1, 3), (E, 0, 1, 1),
    (E, 2, 0, 3), (SY, 3, 0, 4), (E, 2, 0, 1), (E, 0, 1, 5), (E, 2, 0, 5), (E, 0, 3, 7),
    (SY, 0, 3, 6), (E, 0, 1, 7), (E, 2, 0, 7), (E, 1, 0, 1), (SY, 0, 3, 0), (E, 1, 0, 3),
    (E, 1, 0, 5), (E, 1, 0, 7), (E, 1, 1, 3), (E, 1, 1, 5), (G, 3, 4, 7), (SI, 3, 4, 7),
    (E, 1, 1, 1), (E, 3, 2, 3), (V, 0, 0, 0), (G, 3, 4, 4), (SI, 3, 4, 4), (SY, 0, 1, 0),
    (E, 3, 2, 1), (E, 3, 2, 5), (E, 1, 1, 7), (G, 3, 4, 5), (SI, 3, 4, 5), (E, 3, 1, 3),
    (E, 3, 2, 7), (E, 3, 1, 1), (G, 3, 4, 6), (SI, 3, 4, 6), (E, 3, 1, 5), (E, 3, 1, 7),
    (SY, 0, 1, 6), (G, 3, 4, 1), (SO, 3, 4, 1), (SY, 2, 0, 6), (G, 3, 3, 7), (SI, 3, 3, 7),
    (G, 3, 4, 3), (G, 3, 0, 4), (SI, 3, 0, 4), (G, 3, 4, 0), (SO, 3, 4, 0), (SY, 3, 4, 2),
    (G, 3, 0, 6), (SI, 3, 0, 6), (G, 3, 3, 6), (SI, 3, 3, 6), (SY, 0, 3, 4), (SY, 0, 3, 2),
    (G, 3, 3, 1), (SO, 3, 3, 1), (G, 0, 3, 6), (SI, 0, 3, 6), (N, 3, 0, 0), (X, 3, 0, 0),
    (SY, 2, 0, 0), (G, 3, 0, 0), (SO, 3, 0, 0), (N, 3, 4, 0), (X, 3, 4, 0), (G, 0, 0, 6),
    (SI, 0, 0, 6), (G, 3, 3, 0), (SO, 3, 3, 0), (SY, 1, 0, 6), (G, 0, 1, 6), (SI, 0, 1, 6),
    (SY, 1, 0, 0), (U, 3, 0, 0), (AO, 3, 0, 2), (AI, 3, 0, 2), (G, 0, 3, 0), (SO, 0, 3, 0),
    (G, 0, 3, 4), (SI, 0, 3, 4), (U, 3, 4, 0), (AO, 3, 4, 2), (AI, 3, 4, 2), (G, 0, 0, 0),
    (G, 2, 0, 6), (SO, 0, 0, 0), (AY, 3, 4, 2), (SI, 2, 0, 6), (G, 0, 1, 0), (SO, 0, 1, 0),
    (G, 0, 0, 7), (SI, 0, 0, 7), (AO, 3, 0, 4), (AY, 3, 0, 2), (AO, 3, 4, 4), (SY, 0, 1, 4),
    (G, 1, 0, 6), (SI, 1, 0, 6), (SY, 0, 1, 2), (G, 2, 0, 0), (SO, 2, 0, 0), (N, 0, 3, 0),
    (X, 0, 3, 0), (SY, 1, 1, 6), (AO, 3, 4, 3), (AI, 3, 4, 3), (G, 0, 0, 1), (AO, 3, 0, 3),
    (SY, 1, 1, 0), (SO, 0, 0, 1), (AI, 3, 0, 3), (AI, 3, 4, 0), (G, 0, 1, 4), (SI, 0, 1, 4),
    (AI, 3, 0, 0), (U, 0, 3, 0), (AO, 0, 3, 2), (G, 0, 2, 6), (G, 1, 0, 0), (AY, 0, 3, 2),
    (SO, 1, 0, 0), (SI, 0, 2, 6), (AO, 3, 4, 5), (AI, 0, 3, 2), (G, 1, 1, 6), (SI, 1, 1, 6),
    (SY, 2, 0, 2), (AO, 3, 0, 5), (G, 0, 2, 7), (SI, 0, 2, 7), (SY, 2, 0, 4), (AO, 3, 4, 6),
    (G, 0, 2, 0), (AO, 3, 0, 6), (N, 0, 1, 0), (X, 0, 1, 0), (SO, 0, 2, 0), (SY, 3, 2, 6),
    (AO, 0, 3, 4), (AI, 0, 3, 3), (SY, 3, 2, 0), (AO, 0, 3, 3), (SY, 1, 0, 4), (AI, 0, 3, 0),
    (G, 3, 3, 5), (U, 0, 1, 0), (AO, 0, 1, 2), (AY, 0, 1, 2), (G, 1, 1, 0), (SI, 3, 3, 5),
    (G, 3, 3, 4), (V, 0, 0, 1), (SO, 1, 1, 0), (G, 3, 2, 6), (G, 0, 2, 1), (SI, 3, 3, 4),
    (G, 2, 0, 4), (SO, 0, 2, 1), (SY, 1, 0, 2), (SI, 2, 0, 4), (SI, 3, 2, 6), (SY, 1, 1, 4),
    (AO, 0, 3, 5), (AI, 0, 1, 2), (AI, 0, 1, 3), (AO, 0, 1, 3), (SY, 1, 1, 2), (G, 1, 0, 4),
    (N, 2, 0, 0), (AO, 0, 3, 6), (X, 2, 0, 0), (SI, 1, 0, 4), (G, 3, 2, 0), (AI, 0, 1, 0),
    (SO, 3, 2, 0), (G, 3, 3, 3), (SY, 3, 3, 2), (AO, 0, 1, 4), (U, 2, 0, 0), (AO, 0, 1, 5),
    (AI, 2, 0, 2), (AY, 2, 0, 2), (AO, 2, 0, 2), (AI, 3, 3, 0), (G, 1, 1, 4), (AY, 3, 3, 0),
    (SI, 1, 1, 4), (SY, 3, 2, 4), (AO, 0, 1, 6), (N, 3, 3, 0), (X, 3, 3, 0), (SY, 3, 1, 6),
    (N, 1, 0, 0), (AO, 2, 0, 4), (SY, 3, 1, 0), (AI, 2, 0, 3), (AO, 2, 0, 3), (AY, 3, 3, 6),
    (AO, 3, 3, 6), (SY, 3, 2, 2), (U, 3, 3, 0), (AI, 3, 3, 2), (AO, 3, 3, 2), (AY, 3, 3, 2),
    (G, 3, 1, 6), (SI, 3, 1, 6), (N, 1, 1, 0), (X, 1, 0, 0), (SY, 3, 1, 2), (AI, 2, 0, 0),
    (AO, 2, 0, 5), (SY, 3, 1, 4), (G, 3, 2, 4), (SI, 3, 2, 4), (AO, 3, 3, 4), (AY, 3, 3, 4),
    (G, 0, 0, 5), (SI, 0, 0, 5), (G, 3, 1, 0), (SO, 3, 1, 0), (U, 1, 0, 0), (AO, 1, 0, 2),
    (AY, 1, 0, 2), (AI, 1, 0, 2), (U, 1, 1, 0), (AY, 1, 1, 2), (G, 0, 0, 4), (AO, 1, 1, 2),
    (SI, 0, 0, 4), (AO, 2, 0, 6), (AI, 3, 0, 1), (N, 3, 2, 0), (X, 3, 2, 0), (AI, 3, 4, 1),
    (AI, 0, 3, 1), (AY, 1, 0, 4), (AI, 0, 1, 1), (AO, 1, 0, 4), (U, 3, 2, 0), (AY, 3, 2, 2),
    (AI, 1, 1, 2), (AO, 3, 2, 2), (AI, 2, 0, 1), (AY, 1, 0, 0), (AO, 3, 4, 7), (G, 0, 2, 5),
    (AO, 3, 0, 7), (SI, 0, 2, 5), (V, 0, 0, 2), (AO, 0, 3, 7), (G, 0, 0, 3), (SY, 0, 0, 2),
    (AO, 0, 1, 7), (AI, 3, 2, 2), (AY, 1, 1, 4), (AO, 1, 1, 4), (AI, 1, 0, 0), (AY, 1, 1, 0),
    (AO, 2, 0, 7), (AI, 1, 1, 0), (N, 0, 0, 0), (X, 0, 0, 0), (AY, 3, 2, 4), (G, 0, 2, 3),
    (AO, 3, 2, 4), (SY, 0, 2, 2), (U, 0, 0, 0), (AO, 0, 0, 2), (AI, 0, 0, 2), (AO, 1, 0, 6),
    (G, 0, 2, 4), (AY, 1, 0, 6), (SI, 0, 2, 4), (G, 3, 1, 4), (AY, 0, 0, 2), (SI, 3, 1, 4),
    (AO, 1, 1, 6), (AI, 0, 0, 0), (AO, 0, 0, 4), (AY, 0, 0, 4), (AI, 3, 2, 0), (N, 0, 2, 0),
    (AY, 1, 1, 6), (X, 0, 2, 0), (AI, 0, 2, 0), (N, 3, 1, 0), (X, 3, 1, 0), (AI, 3, 1, 1),
    (AY, 3, 2, 0), (AO, 0, 0, 6), (AI, 3, 1, 0), (AO, 3, 2, 6), (U, 0, 2, 0), (AI, 0, 2, 2),
    (AO, 0, 2, 2), (AY, 0, 2, 2), (U, 3, 1, 0), (AI, 3, 1, 2), (AO, 3, 1, 2), (AY, 3, 1, 2),
    (AO, 0, 2, 6), (AY, 3, 2, 6), (AO, 3, 1, 7), (AY, 0, 0, 6), (AY, 0, 2, 4), (AO, 0, 2, 4),
    (AI, 3, 1, 3), (AO, 3, 1, 3), (AY, 0, 2, 6), (AO, 3, 1, 4), (AY, 0, 0, 0), (AO, 3, 1, 6),
    (AY, 0, 2, 0), (AO, 3, 1, 5),
)


def lanes_of(shapes, g, ref, i):
    n = len(GROUPS[g].members)
    w = shapes[g][1] // n
    return ref if n == 1 else ref.at[..., i * w : (i + 1) * w]


def finish(shapes, *refs):
    n = len(GROUPS)
    full, own, st = refs[0:n], refs[n : 2 * n], refs[2 * n : 3 * n]
    vectors = refs[3 * n : 3 * n + 6]
    halves, nexts, news = (refs[3 * n + 6 + 8 * k : 3 * n + 14 + 8 * k] for k in range(3))
    sem, vec_sem = refs[3 * n + 30 :]
    for g, group in enumerate(GROUPS):
        w = shapes[g][1]
        for i, a in enumerate(group.members):
            if group.rows:
                pltpu.make_async_copy(lanes_of(shapes, g, full[g], i), halves[a], sem.at[0, g]).start()
            else:
                for b in range(8):
                    dst = halves[a].at[:, b * w : (b + 1) * w]
                    pltpu.make_async_copy(full[g].at[b], dst, sem.at[0, g]).start()
            pltpu.make_async_copy(lanes_of(shapes, g, own[g], i), nexts[a], sem.at[1, g]).start()
            pltpu.make_async_copy(lanes_of(shapes, g, st[g], i), news[a], sem.at[2, g]).start()
    copies = []
    for i, dst in enumerate((*halves[6:], *nexts[6:], *news[6:])):
        copies.append(pltpu.make_async_copy(vectors[i], dst, vec_sem.at[i]))
        copies[-1].start()
    for g in range(n):
        for k, ref in enumerate((full[g], own[g], st[g])):
            pltpu.make_async_copy(ref, ref, sem.at[k, g]).wait()
    for c in copies:
        c.wait()


def kernel(replicas, models, limit, shapes, *refs):
    slopes, slope_norm, slope_bias = refs[0:6], refs[6], refs[7]
    params, param_norm, param_bias = refs[8:14], refs[14], refs[15]
    states, state_norm, state_bias = refs[16:22], refs[22], refs[23]
    groups = range(len(GROUPS))
    n = len(GROUPS)
    full, own, st = refs[24 : 24 + n], refs[24 + n : 24 + 2 * n], refs[24 + 2 * n : 24 + 3 * n]
    half_norm, half_bias, next_norm, next_bias, new_norm, new_bias = refs[24 + 3 * n : 30 + 3 * n]
    scratch = list(refs[30 + 3 * n :])
    take = lambda: [scratch.pop(0) for _ in groups]
    xin, enc, rec, sq, sqr = (take() for _ in range(5))
    vs, vown, vrec, vnext, vag, vh_norm, vh_bias = (scratch.pop(0) for _ in range(7))
    rs_s, rs_r, ag_s, ag_r, n_s, n_r, v_s, v_r, w_s, w_r = (scratch.pop(0) for _ in range(10))
    load_sem, own_sem, st_sem, vown_sem = scratch

    r = lax.axis_index("replica")
    m = lax.axis_index("model")
    y, z = lax.rem(r, 2), r // 2
    side = z // 2
    slab = [(p + side * (3 - 2 * p)) * 2 + (y if d == 0 else 1 - y) for p in range(4) for d in (0, 1)]

    scale = 2.0**13 / (limit * replicas)
    rate = replicas ** (-0.5)

    def encode(x):
        t = x * scale
        t2 = t * t
        t4 = t2 * t2
        return (t4 * t4 * t).astype(jnp.bfloat16)

    def decode(c):
        f = c.astype(jnp.float32)
        a = jnp.exp(jnp.log(jnp.abs(f)) * (1.0 / root)) * (1.0 / scale)
        return jnp.where(f < 0, -a, a)

    lanes = functools.partial(lanes_of, shapes)
    at = {k: i for i, k in enumerate(CHUNKS)}
    unit = lambda g: shapes[g][0] // sum(SIZES[g])
    height = lambda g, c: unit(g) * SIZES[g][c]
    rows = lambda g, c: pl.ds(unit(g) * sum(SIZES[g][:c]), height(g, c))

    def source(g, c, s):
        w = shapes[g][1]
        if GROUPS[g].rows:
            return xin[g].at[slab[s], rows(g, c)]
        return xin[g].at[rows(g, c), pl.ds(pl.multiple_of(slab[s] * w, w), w)]

    def loop(g, c, body):
        h, w = height(g, c), shapes[g][1]
        step = min(h, max(16, STEP // w // 16 * 16))
        while h % step:
            step -= 16
        lax.fori_loop(0, h // step, lambda i, c: (body(pl.ds(pl.multiple_of(i * step, step), step)), c)[1], 0)

    def remote(src, dst, s, d, peer, axis="replica"):
        return pltpu.make_async_remote_copy(
            src_ref=src, dst_ref=dst, send_sem=s, recv_sem=d, device_id={axis: peer}, device_id_type=MESH
        )

    def whole(ref, sem):
        pltpu.make_async_copy(ref, ref, sem).wait()

    barrier = pltpu.get_barrier_semaphore()
    for j in range(1, replicas):
        pl.semaphore_signal(barrier, inc=1, device_id={"replica": lax.rem(r + j, replicas)}, device_id_type=MESH)
    for j in range(1, models):
        pl.semaphore_signal(barrier, inc=1, device_id={"model": lax.rem(m + j, models)}, device_id_type=MESH)

    def chunk_of(g, c):
        return xin[g].at[:, rows(g, c)] if GROUPS[g].rows else xin[g].at[rows(g, c)]

    for g, c in CHUNKS:
        for i, a in enumerate(GROUPS[g].members):
            src = slopes[a].at[:, rows(g, c)] if GROUPS[g].rows else slopes[a].at[rows(g, c)]
            pltpu.make_async_copy(src, lanes(g, chunk_of(g, c), i), load_sem.at[at[g, c]]).start()
    for g in OWN:
        for i, a in enumerate(GROUPS[g].members):
            pltpu.make_async_copy(params[a], lanes(g, own[g], i), own_sem.at[g]).start()
            pltpu.make_async_copy(states[a], lanes(g, st[g], i), st_sem.at[g]).start()

    vs[0:1, :] = slope_norm[...]
    vs[1:2, :] = slope_bias[...]
    for g in groups:
        if not GROUPS[g].rows:
            sq[g][...] = jnp.zeros_like(sq[g])

    def rule(p, s, v):
        s = hold_rate * s + (1.0 - hold_rate) * v * v
        return p - learn_rate * v * lax.rsqrt(s + 1e-06), s

    def fold(x):
        total = x[:, 0:128]
        for k in range(128, x.shape[1], 128):
            total = total + x[:, k : k + 128]
        return jnp.sum(total, axis=1, keepdims=True)

    width = vs.shape[1] // replicas

    def vec_out(j):
        to = lax.rem(r + j, replicas)
        return remote(
            vs.at[:, pl.ds(pl.multiple_of(to * width, width), width)],
            vrec.at[j - 1], v_s.at[j - 1], v_r.at[j - 1], to,
        )

    def vec_back(j):
        return remote(vnext, vag.at[j - 1], w_s.at[j - 1], w_r.at[j - 1], lax.rem(r + j, replicas))

    def vec_start():
        pltpu.make_async_copy(vs.at[:, pl.ds(pl.multiple_of(r * width, width), width)], vown, vown_sem).start()
        for j in range(1, replicas):
            vec_out(j).start()

    def vec_update():
        pltpu.make_async_copy(vown, vown, vown_sem).wait()
        total = vown[...]
        for j in range(1, replicas):
            vec_out(j).wait_recv()
            total = total + vrec[j - 1]
        v = total * rate
        p, s = rule(param_norm[...], state_norm[...], v[0:1, :])
        next_norm[...] = p
        new_norm[...] = s
        vnext[0:1, :] = p
        p, s = rule(param_bias[...], state_bias[...], v[1:2, :])
        next_bias[...] = p
        new_bias[...] = s
        vnext[1:2, :] = p
        for j in range(1, replicas):
            vec_back(j).start()

    def vec_finish():
        vh_norm[pl.ds(r, 1), :] = vnext[0:1, :]
        vh_bias[pl.ds(r, 1), :] = vnext[1:2, :]
        for j in range(1, replicas):
            vec_back(j).wait_recv()
            at = lax.rem(r + replicas - j, replicas)
            vh_norm[pl.ds(at, 1), :] = vag[j - 1, 0:1, :]
            vh_bias[pl.ds(at, 1), :] = vag[j - 1, 1:2, :]
        half_norm[...] = vh_norm[...].astype(jnp.bfloat16)
        half_bias[...] = vh_bias[...].astype(jnp.bfloat16)

    def run(mid, order):
        mine = 1 if mid else 0
        peers = {}
        if mid:
            peers[SO] = peers[AO] = side * 6 + y
            peers[SI] = peers[AI] = (3 - z) * 2 + y
        else:
            peers[SI] = peers[AI] = (1 + side) * 2 + y
        peers[SY] = peers[AY] = z * 2 + (1 - y)
        done = set()

        def kind(g, c):
            return SUMS[g][c]

        def landing(g, c, by, s):
            if kind(g, c) == A:
                return (0, 7, 3)[by] + s // 2
            return (10, 6 + s, s - 2)[by]

        def outgoing(g, c, op, s):
            p = s // 2
            if kind(g, c) == A:
                if op == SY:
                    return p
                return 3 + p if p else 4
            if op == SY:
                return 6
            if not mid:
                return s - 2
            return s - 4 if p >= 2 else 4 + s

        def across(op, s):
            return (3 - s // 2) * 2 + s % 2 if mid and op in (SI, AI) else s

        def send(op, g, c, s):
            by = {SY: 0, SO: 1, SI: 1 if mid else 2}[op]
            slot = landing(g, c, by, across(op, s))
            return remote(
                enc[g].at[outgoing(g, c, op, s), rows(g, c)],
                rec[g].at[slot, rows(g, c)],
                rs_s.at[g],
                rs_r.at[at[g, c], slot],
                peers[op],
            )

        def gather(op, g, c, s):
            to = s + 1 if op == AY else across(op, s)
            ref = full[g].at[slab[s], rows(g, c)]
            link = {AY: 0, AI: 1, AO: 2}[op]
            return remote(ref, ref, ag_s.at[at[g, c], link], ag_r.at[at[g, c], to], peers[op])

        def got(g, c, s):
            if s != mine * 2 and (g, c, s) not in done:
                done.add((g, c, s))
                ref = full[g].at[slab[s], rows(g, c)]
                whole(ref, ag_r.at[at[g, c], s])

        def arrived(g, c, by, s):
            slot = landing(g, c, by, s)
            ref = rec[g].at[slot, rows(g, c)]
            whole(ref, rs_r.at[at[g, c], slot])
            return ref

        def once(key, ref, sem):
            if key not in done:
                done.add(key)
                whole(ref, sem)

        def loaded(g, c):
            once((-1, g, c), chunk_of(g, c), load_sem.at[at[g, c]])

        def parts(g, c, s):
            loaded(g, c)
            by = []
            a, p = kind(g, c) == A, s // 2
            if a or s == mine * 2:
                by.append(0)
            if mid and p >= 1:
                by.append(2)
            if p == mine or (mid and p == 0):
                by.append(1)
            return [arrived(g, c, b, s) for b in by]

        def encode_op(g, c, s, op):
            loaded(g, c)
            src, dst = source(g, c, s), enc[g].at[outgoing(g, c, op, s), rows(g, c)]

            def body(d):
                dst[d, :] = encode(src[d, :])

            loop(g, c, body)

        def add_op(g, c, s):
            src = source(g, c, s)
            op = SY if s // 2 == mine else SO if mid and s < 2 else SI
            dst = enc[g].at[outgoing(g, c, op, s), rows(g, c)]
            got = parts(g, c, s)

            def body(d):
                total = src[d, :]
                for ref in got:
                    total = total + decode(ref[d, :])
                dst[d, :] = encode(total)

            loop(g, c, body)

        def mean_op(g, c):
            acc = source(g, c, mine * 2)
            got = parts(g, c, mine * 2)
            once((-2, g), own[g], own_sem.at[g])
            held = own[g].at[rows(g, c)]
            k = len(GROUPS[g].members)
            w = shapes[g][1] // k

            def mean(d):
                total = acc[d, :]
                for ref in got:
                    total = total + decode(ref[d, :])
                v = total * rate
                acc[d, :] = v
                return v

            if GROUPS[g].rows:
                sums = sq[g].at[rows(g, c)]

                def body(d):
                    v, p = mean(d), held[d, :]
                    v, p = v * v, p * p
                    lane = lax.broadcasted_iota(jnp.int32, (v.shape[0], 128), 1)
                    out = jnp.zeros((v.shape[0], 128), jnp.float32)
                    for i in range(k):
                        cols = slice(i * w, (i + 1) * w)
                        out = jnp.where(lane == 2 * i, fold(p[:, cols]), out)
                        out = jnp.where(lane == 2 * i + 1, fold(v[:, cols]), out)
                    sums[d, :] = out

            else:

                def body(d):
                    v, p = mean(d), held[d, :]
                    sq[g][0] += jnp.sum((p * p).reshape(-1, 8, w), axis=0)
                    sq[g][1] += jnp.sum((v * v).reshape(-1, 8, w), axis=0)

            loop(g, c, body)

        def norms(g, c, j):
            if GROUPS[g].rows:
                src, dst = sq[g].at[rows(g, c)], sqr[g].at[j - 1, rows(g, c)]
            else:
                src, dst = sq[g], sqr[g].at[j - 1]
            return remote(src, dst, n_s.at[at[g, c], j - 1], n_r.at[at[g, c], j - 1], lax.rem(m + j, models), "model")

        def update_op(g, c):
            first = c if GROUPS[g].rows else 0
            for j in range(1, models):
                if (-4, g, first, j) not in done:
                    done.add((-4, g, first, j))
                    norms(g, first, j).wait_recv()
            once((-3, g), st[g], st_sem.at[g])
            acc, half = source(g, c, mine * 2), full[g].at[slab[mine * 2], rows(g, c)]
            held, hold = own[g].at[rows(g, c)], st[g].at[rows(g, c)]
            k = len(GROUPS[g].members)
            w = shapes[g][1] // k

            def put(d, cols, t):
                p, s = rule(held[d, cols], hold[d, cols], acc[d, cols] * t)
                held[d, cols] = p
                hold[d, cols] = s
                half[d, cols] = p.astype(jnp.bfloat16)

            if GROUPS[g].rows:
                sums = [sq[g].at[rows(g, c)]] + [sqr[g].at[j, rows(g, c)] for j in range(models - 1)]

                def body(d):
                    total = sums[0][d, :]
                    for ref in sums[1:]:
                        total = total + ref[d, :]
                    lane = lax.broadcasted_iota(jnp.int32, total.shape, 1)
                    pick = lambda i: jnp.sum(jnp.where(lane == i, total, 0.0), axis=1, keepdims=True)
                    for i in range(k):
                        t = jnp.sqrt(pick(2 * i)) * lax.rsqrt(pick(2 * i + 1) + 1e-06)
                        put(d, slice(i * w, (i + 1) * w), t)

            else:
                total = sq[g][...]
                for j in range(models - 1):
                    total = total + sqr[g][j]
                total = jnp.sum(total, axis=1, keepdims=True)
                t = jnp.sqrt(total[0]) * lax.rsqrt(total[1] + 1e-06)

                def body(d):
                    put(d, slice(None), t)

            loop(g, c, body)

        met = False
        for op, g, c, s in order:
            if op not in (E, G) and not met:
                met = True
                pl.semaphore_wait(barrier, replicas + models - 2)
            if op == E:
                encode_op(g, c, s, SY if kind(g, c) == A else SI)
            elif op == G:
                add_op(g, c, s)
            elif op in (SY, SI, SO):
                send(op, g, c, s).start()
            elif op == N:
                mean_op(g, c)
            elif op == X:
                for j in range(1, models):
                    norms(g, c, j).start()
            elif op == U:
                update_op(g, c)
            elif op == V:
                (vec_start, vec_update, vec_finish)[s]()
            else:
                got(g, c, s)
                gather(op, g, c, s).start()

        for g, c in CHUNKS:
            for s in range(8):
                got(g, c, s)
        for g in groups:
            whole(enc[g], rs_s.at[g])
        for g, c in CHUNKS:
            for link, count in enumerate(SENT[mid][BACK[g][c]]):
                if count:
                    whole(full[g].at[pl.ds(0, count), rows(g, c)], ag_s.at[at[g, c], link])
            if GROUPS[g].rows or c == 0:
                for j in range(1, models):
                    norms(g, c, j).wait_send()
        for j in range(1, replicas):
            vec_out(j).wait_send()
            vec_back(j).wait_send()

    end = jnp.logical_or(z == 0, z == 3)

    @pl.when(end)
    def _():
        run(False, END)

    @pl.when(jnp.logical_not(end))
    def _():
        run(True, MID)


def fused(replicas, models, shapes, *args):
    slopes, params = args[0:6], args[8:14]
    f32, bf16 = jnp.float32, jnp.bfloat16
    vec = args[6].shape[1]
    width = vec // replicas
    row = lambda a: a.reshape(1, -1)
    by_rows = [a in g.members and g.rows for a in range(6) for g in GROUPS if a in g.members]
    cut = lambda a, rows: a.reshape(replicas, -1, a.shape[-1]) if rows else a[0]
    args = (
        *(cut(a, rows) for a, rows in zip(slopes, by_rows)), *args[6:14],
        row(args[14]), row(args[15]), *args[16:22], row(args[22]), row(args[23]),
    )
    S = jax.ShapeDtypeStruct
    n, chunks = len(GROUPS), len(CHUNKS)
    held = [((replicas, *s), bf16) for s in shapes] + [(s, f32) for s in shapes] * 2
    held += [((replicas, width), bf16)] * 2 + [((1, width), f32)] * 4
    ANY, VM = pl.BlockSpec(memory_space=pl.ANY), pl.BlockSpec(memory_space=pltpu.VMEM)
    part = [ANY] * 6 + [VM] * 2
    scratch = [
        pltpu.VMEM((replicas, *s) if g.rows else (s[0], s[1] * replicas), f32) for g, s in zip(GROUPS, shapes)
    ]
    scratch += [pltpu.VMEM((7, *s), bf16) for s in shapes]
    scratch += [pltpu.VMEM((11 if B in k else 9, *s), bf16) for k, s in zip(SUMS, shapes)]
    sq = [(s[0], 128) if g.rows else (2, 8, s[1]) for g, s in zip(GROUPS, shapes)]
    scratch += [pltpu.VMEM(s, f32) for s in sq]
    scratch += [pltpu.VMEM((models - 1, *s), f32) for s in sq]
    scratch += [
        pltpu.VMEM((2, vec), f32),
        pltpu.VMEM((2, width), f32),
        pltpu.VMEM((replicas - 1, 2, width), f32),
        pltpu.VMEM((2, width), f32),
        pltpu.VMEM((replicas - 1, 2, width), f32),
        pltpu.VMEM((replicas, width), f32),
        pltpu.VMEM((replicas, width), f32),
    ]
    dma = pltpu.SemaphoreType.DMA
    scratch += [dma((n,)), dma((chunks, 11)), dma((chunks, 3)), dma((chunks, 8))]
    scratch += [dma((chunks, models - 1))] * 2 + [dma((replicas - 1,))] * 4
    scratch += [dma((chunks,))] + [dma((n,))] * 2 + [dma(())]
    out = pl.pallas_call(
        functools.partial(kernel, replicas, models, 4.0, shapes),
        out_shape=[pltpu.VMEM(*h) for h in held],
        in_specs=part * 3,
        out_specs=[VM] * len(held),
        scratch_shapes=scratch,
        compiler_params=pltpu.CompilerParams(
            collective_id=0, has_side_effects=True, vmem_limit_bytes=54 * 1024 * 1024
        ),
    )(*args)
    outs = [
        S((replicas, a.shape[1] // replicas, a.shape[2]) if rows else a.shape[1:], bf16)
        for a, rows in zip(slopes, by_rows)
    ]
    outs += [S((replicas, width), bf16)] * 2
    for _ in range(2):
        outs += [S(a.shape, f32) for a in params] + [S((1, width), f32)] * 2
    out = pl.pallas_call(
        functools.partial(finish, shapes),
        out_shape=outs,
        in_specs=[VM] * len(held),
        out_specs=[ANY] * len(outs),
        scratch_shapes=[dma((3, n)), dma((6,))],
        compiler_params=pltpu.CompilerParams(vmem_limit_bytes=1024 * 1024),
    )(*out)
    flat = lambda a: a.reshape(-1)
    return (
        *(a.reshape(-1, a.shape[-1]) for a in out[0:6]), flat(out[6]), flat(out[7]),
        *out[8:14], flat(out[14]), flat(out[15]),
        *out[16:22], flat(out[22]), flat(out[23]),
    )


def plain(
    slope_up,
    slope_down,
    slope_query,
    slope_key,
    slope_value,
    slope_mixed,
    slope_norm,
    slope_bias,
    param_up,
    param_down,
    param_query,
    param_key,
    param_value,
    param_mixed,
    param_norm,
    param_bias,
    state_up,
    state_down,
    state_query,
    state_key,
    state_value,
    state_mixed,
    state_norm,
    state_bias,
):
    mean_up, mean_down, mean_query, mean_key, mean_value, mean_mixed = (
        lax.psum_scatter(slope_up[0], "replica", scatter_dimension=0, tiled=True),
        lax.psum_scatter(slope_down[0], "replica", scatter_dimension=1, tiled=True),
        lax.psum_scatter(slope_query[0], "replica", scatter_dimension=0, tiled=True),
        lax.psum_scatter(slope_key[0], "replica", scatter_dimension=0, tiled=True),
        lax.psum_scatter(slope_value[0], "replica", scatter_dimension=0, tiled=True),
        lax.psum_scatter(slope_mixed[0], "replica", scatter_dimension=1, tiled=True),
    )
    whole_norm, whole_bias = lax.psum((slope_norm[0], slope_bias[0]), "replica")
    place = lax.axis_index("replica")
    mean_norm = lax.dynamic_slice_in_dim(
        whole_norm, place * param_norm.shape[0], param_norm.shape[0]
    )
    mean_bias = lax.dynamic_slice_in_dim(
        whole_bias, place * param_bias.shape[0], param_bias.shape[0]
    )
    mean_rate = lax.axis_size("replica") ** (-0.5)
    mean_up = mean_up * mean_rate
    mean_down = mean_down * mean_rate
    mean_query = mean_query * mean_rate
    mean_key = mean_key * mean_rate
    mean_value = mean_value * mean_rate
    mean_mixed = mean_mixed * mean_rate
    mean_norm = mean_norm * mean_rate
    mean_bias = mean_bias * mean_rate
    (
        own_up,
        own_down,
        own_query,
        own_key,
        own_value,
        own_mixed,
        slope_up_norm,
        slope_down_norm,
        slope_query_norm,
        slope_key_norm,
        slope_value_norm,
        slope_mixed_norm,
    ) = lax.psum(
        (
            jnp.sum(param_up * param_up, axis=1, keepdims=True),
            jnp.sum(param_down * param_down, axis=0, keepdims=True),
            jnp.sum(param_query * param_query, axis=1, keepdims=True),
            jnp.sum(param_key * param_key, axis=1, keepdims=True),
            jnp.sum(param_value * param_value, axis=1, keepdims=True),
            jnp.sum(param_mixed * param_mixed, axis=0, keepdims=True),
            jnp.sum(mean_up * mean_up, axis=1, keepdims=True),
            jnp.sum(mean_down * mean_down, axis=0, keepdims=True),
            jnp.sum(mean_query * mean_query, axis=1, keepdims=True),
            jnp.sum(mean_key * mean_key, axis=1, keepdims=True),
            jnp.sum(mean_value * mean_value, axis=1, keepdims=True),
            jnp.sum(mean_mixed * mean_mixed, axis=0, keepdims=True),
        ),
        "model",
    )
    mean_up = mean_up * (jnp.sqrt(own_up) * lax.rsqrt(slope_up_norm + 1e-06))
    mean_down = mean_down * (jnp.sqrt(own_down) * lax.rsqrt(slope_down_norm + 1e-06))
    mean_query = mean_query * (jnp.sqrt(own_query) * lax.rsqrt(slope_query_norm + 1e-06))
    mean_key = mean_key * (jnp.sqrt(own_key) * lax.rsqrt(slope_key_norm + 1e-06))
    mean_value = mean_value * (jnp.sqrt(own_value) * lax.rsqrt(slope_value_norm + 1e-06))
    mean_mixed = mean_mixed * (jnp.sqrt(own_mixed) * lax.rsqrt(slope_mixed_norm + 1e-06))
    state_new_up = hold_rate * state_up + (1.0 - hold_rate) * mean_up * mean_up
    next_up = param_up - learn_rate * mean_up * lax.rsqrt(state_new_up + 1e-06)
    state_new_down = hold_rate * state_down + (1.0 - hold_rate) * mean_down * mean_down
    next_down = param_down - learn_rate * mean_down * lax.rsqrt(state_new_down + 1e-06)
    state_new_query = hold_rate * state_query + (1.0 - hold_rate) * mean_query * mean_query
    next_query = param_query - learn_rate * mean_query * lax.rsqrt(state_new_query + 1e-06)
    state_new_key = hold_rate * state_key + (1.0 - hold_rate) * mean_key * mean_key
    next_key = param_key - learn_rate * mean_key * lax.rsqrt(state_new_key + 1e-06)
    state_new_value = hold_rate * state_value + (1.0 - hold_rate) * mean_value * mean_value
    next_value = param_value - learn_rate * mean_value * lax.rsqrt(state_new_value + 1e-06)
    state_new_mixed = hold_rate * state_mixed + (1.0 - hold_rate) * mean_mixed * mean_mixed
    next_mixed = param_mixed - learn_rate * mean_mixed * lax.rsqrt(state_new_mixed + 1e-06)
    state_new_norm = hold_rate * state_norm + (1.0 - hold_rate) * mean_norm * mean_norm
    next_norm = param_norm - learn_rate * mean_norm * lax.rsqrt(state_new_norm + 1e-06)
    state_new_bias = hold_rate * state_bias + (1.0 - hold_rate) * mean_bias * mean_bias
    next_bias = param_bias - learn_rate * mean_bias * lax.rsqrt(state_new_bias + 1e-06)
    half_up, half_down, half_query, half_key, half_value, half_mixed, half_norm, half_bias = (
        lax.all_gather(next_up.astype(jnp.bfloat16), "replica", axis=0, tiled=True),
        lax.all_gather(next_down.astype(jnp.bfloat16), "replica", axis=1, tiled=True),
        lax.all_gather(next_query.astype(jnp.bfloat16), "replica", axis=0, tiled=True),
        lax.all_gather(next_key.astype(jnp.bfloat16), "replica", axis=0, tiled=True),
        lax.all_gather(next_value.astype(jnp.bfloat16), "replica", axis=0, tiled=True),
        lax.all_gather(next_mixed.astype(jnp.bfloat16), "replica", axis=1, tiled=True),
        lax.all_gather(next_norm.astype(jnp.bfloat16), "replica", axis=0, tiled=True),
        lax.all_gather(next_bias.astype(jnp.bfloat16), "replica", axis=0, tiled=True),
    )
    return (
        half_up,
        half_down,
        half_query,
        half_key,
        half_value,
        half_mixed,
        half_norm,
        half_bias,
        next_up,
        next_down,
        next_query,
        next_key,
        next_value,
        next_mixed,
        next_norm,
        next_bias,
        state_new_up,
        state_new_down,
        state_new_query,
        state_new_key,
        state_new_value,
        state_new_mixed,
        state_new_norm,
        state_new_bias,
    )


def solution(mesh):
    replicas, models = mesh.shape["replica"], mesh.shape["model"]

    def local(*args):
        if replicas != 2**3 or any(a.shape[k] % 128 for a in args[8:14] for k in (0, 1)):
            return plain(*args)
        shapes = []
        for g, sizes in zip(GROUPS, SIZES):
            h, w = args[8 + g.members[0]].shape
            shapes.append((h, w * len(g.members)))
            if h % (16 * sum(sizes)) or (w != 128 and not g.rows):
                return plain(*args)
        if args[14].shape[0] % 128:
            return plain(*args)
        return fused(replicas, models, shapes, *args)

    placed = (
        P("replica", None, "model"),
        P("replica", "model", None),
        P("replica", None, "model"),
        P("replica", None, "model"),
        P("replica", None, "model"),
        P("replica", "model", None),
        P("replica", None),
        P("replica", None),
        P("replica", "model"),
        P("model", "replica"),
        P("replica", "model"),
        P("replica", "model"),
        P("replica", "model"),
        P("model", "replica"),
        P("replica"),
        P("replica"),
        P("replica", "model"),
        P("model", "replica"),
        P("replica", "model"),
        P("replica", "model"),
        P("replica", "model"),
        P("model", "replica"),
        P("replica"),
        P("replica"),
    )
    return jax.shard_map(
        local,
        mesh=mesh,
        in_specs=placed,
        out_specs=(
            P(None, "model"),
            P("model", None),
            P(None, "model"),
            P(None, "model"),
            P(None, "model"),
            P("model", None),
            P(),
            P(),
            P("replica", "model"),
            P("model", "replica"),
            P("replica", "model"),
            P("replica", "model"),
            P("replica", "model"),
            P("model", "replica"),
            P("replica"),
            P("replica"),
            P("replica", "model"),
            P("model", "replica"),
            P("replica", "model"),
            P("replica", "model"),
            P("replica", "model"),
            P("model", "replica"),
            P("replica"),
            P("replica"),
        ),
        check_vma=False,
    )
```

```python
import functools

import jax
import jax.numpy as jnp
from jax import lax
from jax.experimental import pallas as pl
from jax.experimental.pallas import tpu as pltpu
from jax.sharding import PartitionSpec as P

learn_rate = 0.025
hold_rate = 0.7
root = 9
MESH = pl.DeviceIdType.MESH


class Group:
    def __init__(self, members, rows):
        self.members = members
        self.rows = rows


GROUPS = (Group((0,), True), Group((1,), False), Group((5,), False), Group((2, 3, 4), True))
A, B = 0, 1
E, G, N, X, U, V, SY, SI, SO, AY, AI, AO = range(12)
SIZES = ((2, 2, 2, 2), (2, 2, 2, 2), (8,), (2, 2, 2, 2))
SUMS = ((B, A, A, A), (A, A, A, A), (A,), (B, B, B, B))
BACK = ((A, B, B, B), (A, A, A, A), (B,), (A, A, A, A))
CHUNKS = ((0, 3), (3, 2), (0, 0), (3, 0), (0, 2), (1, 2), (1, 1), (3, 3), (0, 1), (3, 1), (1, 3), (2, 0), (1, 0))
OWN = (0, 3, 1, 2)
SENT = (((4, 1, 0), (1, 2, 0)), ((4, 2, 3), (1, 4, 6)))
STEP = 16384
END = (
    (E, 0, 3, 1), (SY, 0, 3, 0), (E, 0, 3, 3), (SY, 0, 3, 2), (E, 3, 2, 6), (SI, 3, 2, 6),
    (E, 3, 2, 7), (SI, 3, 2, 7), (E, 0, 3, 5), (E, 0, 0, 7), (E, 0, 3, 7), (E, 3, 0, 7),
    (E, 0, 0, 6), (E, 0, 2, 1), (E, 0, 2, 7), (E, 0, 2, 5), (SY, 0, 3, 4), (SI, 0, 0, 7),
    (E, 0, 2, 3), (E, 1, 2, 5), (E, 1, 2, 3), (E, 3, 0, 6), (E, 3, 3, 6), (E, 3, 3, 7),
    (E, 1, 2, 7), (SI, 3, 0, 7), (E, 0, 1, 3), (E, 0, 1, 5), (E, 3, 1, 7), (SY, 0, 3, 6),
    (E, 3, 1, 6), (E, 1, 3, 7), (E, 1, 3, 3), (E, 1, 3, 5), (E, 2, 0, 7), (E, 2, 0, 5),
    (E, 1, 1, 5), (E, 1, 0, 7), (SI, 3, 1, 7), (E, 1, 0, 5), (E, 2, 0, 3), (E, 1, 1, 7),
    (SY, 1, 0, 6), (E, 1, 0, 3), (E, 1, 1, 3), (E, 1, 2, 1), (E, 1, 3, 1), (SI, 0, 0, 6),
    (E, 1, 1, 1), (E, 0, 0, 5), (G, 0, 3, 2), (E, 0, 1, 7), (E, 0, 0, 4), (SY, 0, 2, 0),
    (E, 1, 0, 1), (E, 3, 2, 5), (E, 3, 2, 4), (SI, 3, 3, 6), (E, 0, 0, 3), (E, 3, 2, 3),
    (E, 2, 0, 1), (E, 0, 0, 2), (G, 0, 3, 4), (E, 0, 1, 1), (E, 3, 1, 5), (E, 3, 2, 2),
    (SY, 0, 2, 6), (E, 3, 3, 5), (E, 3, 0, 5), (SI, 0, 3, 4), (E, 3, 0, 4), (E, 3, 0, 3),
    (E, 3, 1, 3), (E, 3, 3, 3), (E, 3, 1, 4), (G, 0, 3, 6), (E, 3, 0, 2), (E, 3, 3, 4),
    (SY, 0, 2, 4), (SI, 0, 3, 6), (E, 3, 1, 2), (E, 3, 3, 2), (G, 1, 0, 6), (SI, 3, 1, 6),
    (SY, 0, 2, 2), (SI, 1, 0, 6), (SY, 1, 2, 4), (G, 3, 2, 1), (G, 0, 2, 6), (SI, 0, 3, 2),
    (SY, 1, 2, 2), (G, 0, 2, 4), (SI, 3, 0, 6), (G, 0, 0, 1), (SY, 0, 0, 0), (G, 0, 2, 2),
    (SI, 0, 2, 4), (G, 3, 0, 1), (SY, 3, 0, 0), (G, 3, 1, 1), (SI, 3, 3, 7), (G, 1, 2, 4),
    (SY, 0, 1, 2), (SI, 0, 2, 6), (G, 1, 2, 2), (SY, 1, 3, 6), (SI, 0, 2, 2), (N, 0, 0, 0),
    (V, 0, 0, 0), (SY, 1, 2, 6), (X, 0, 0, 0), (SI, 1, 2, 4), (SY, 1, 3, 2), (SI, 1, 2, 2),
    (G, 0, 1, 2), (N, 0, 3, 0), (X, 0, 3, 0), (SY, 0, 1, 4), (U, 0, 0, 0), (SI, 0, 1, 2),
    (G, 1, 3, 6), (SY, 2, 0, 6), (AI, 0, 0, 0), (G, 1, 2, 6), (SY, 1, 0, 4), (U, 0, 3, 0),
    (AI, 0, 3, 0), (G, 1, 3, 2), (AY, 0, 3, 0), (N, 3, 0, 0), (X, 3, 0, 0), (SI, 1, 2, 6),
    (G, 0, 1, 4), (SY, 2, 0, 4), (G, 3, 3, 1), (SI, 0, 1, 4), (G, 2, 0, 6), (AY, 0, 0, 0),
    (SI, 2, 0, 6), (G, 1, 0, 4), (U, 3, 0, 0), (SY, 3, 2, 0), (SI, 1, 3, 6), (SY, 1, 3, 4),
    (AI, 0, 3, 1), (G, 2, 0, 4), (SY, 1, 1, 4), (AI, 3, 0, 0), (N, 0, 2, 0), (X, 0, 2, 0),
    (SY, 2, 0, 2), (N, 3, 2, 0), (SI, 1, 0, 4), (X, 3, 2, 0), (SY, 3, 3, 0), (SI, 2, 0, 4),
    (G, 1, 3, 4), (SY, 1, 1, 6), (U, 0, 2, 0), (SI, 1, 3, 4), (G, 1, 1, 4), (SY, 1, 0, 2),
    (U, 3, 2, 0), (AI, 0, 2, 0), (G, 2, 0, 2), (AY, 0, 2, 0), (N, 3, 3, 0), (AI, 3, 2, 0),
    (X, 3, 3, 0), (SY, 3, 1, 0), (G, 1, 1, 6), (SI, 1, 1, 6), (SY, 1, 1, 2), (SI, 2, 0, 2),
    (G, 1, 0, 2), (SY, 1, 2, 0), (U, 3, 3, 0), (SI, 1, 1, 4), (AY, 3, 0, 0), (N, 3, 1, 0),
    (V, 0, 0, 1), (AI, 3, 3, 0), (X, 3, 1, 0), (AY, 0, 0, 6), (G, 1, 1, 2), (AY, 3, 3, 0),
    (SI, 1, 3, 2), (SI, 1, 0, 2), (N, 1, 2, 0), (AY, 3, 2, 0), (U, 3, 1, 0), (SI, 1, 1, 2),
    (SY, 1, 3, 0), (SY, 1, 1, 0), (SI, 0, 0, 5), (SY, 0, 1, 6), (SI, 0, 0, 4), (SY, 1, 0, 0),
    (SI, 3, 2, 5), (N, 1, 3, 0), (AY, 3, 1, 0), (SI, 3, 2, 4), (SI, 0, 0, 3), (AY, 3, 0, 6),
    (G, 0, 1, 6), (AY, 3, 2, 6), (SI, 3, 2, 3), (SY, 2, 0, 0), (N, 1, 0, 0), (SI, 0, 0, 2),
    (N, 1, 1, 0), (X, 1, 0, 0), (SY, 0, 1, 0), (SI, 3, 1, 5), (AY, 3, 3, 6), (SI, 3, 2, 2),
    (SI, 3, 3, 5), (U, 1, 3, 0), (AY, 1, 3, 0), (U, 1, 1, 0), (U, 1, 0, 0), (SI, 3, 0, 5),
    (AY, 1, 1, 0), (U, 1, 2, 0), (N, 2, 0, 0), (X, 2, 0, 0), (SI, 3, 0, 4), (AY, 1, 0, 0),
    (SI, 3, 0, 3), (AY, 1, 2, 0), (SI, 0, 1, 6), (U, 2, 0, 0), (SI, 3, 1, 3), (AY, 1, 1, 2),
    (SI, 3, 3, 3), (AY, 1, 3, 2), (AI, 1, 1, 0), (AY, 1, 0, 2), (SI, 3, 1, 4), (AY, 2, 0, 0),
    (SI, 3, 0, 2), (AY, 1, 2, 2), (AI, 1, 2, 0), (AI, 1, 3, 0), (V, 0, 0, 2), (AY, 1, 3, 4),
    (SI, 3, 3, 4), (AY, 1, 0, 4), (AI, 3, 1, 0), (AY, 1, 1, 4), (SI, 3, 1, 2), (AY, 0, 0, 2),
    (AI, 2, 0, 0), (AY, 3, 2, 2), (N, 0, 1, 0), (SI, 3, 3, 2), (X, 0, 1, 0), (AY, 1, 2, 4),
    (AI, 1, 0, 0), (AY, 0, 0, 4), (AI, 0, 2, 1), (U, 0, 1, 0), (AY, 3, 2, 4), (AI, 2, 0, 1),
    (AY, 1, 1, 6), (AI, 0, 1, 0), (AY, 0, 1, 0), (AY, 3, 0, 2), (AY, 1, 3, 6), (AY, 1, 2, 6),
    (AI, 0, 1, 1), (AY, 3, 1, 6), (AY, 3, 1, 2), (AY, 3, 0, 4), (AY, 3, 3, 2), (AY, 3, 1, 4),
    (AY, 1, 0, 6), (AY, 3, 3, 4),
)
MID = (
    (E, 0, 3, 1), (SY, 0, 3, 0), (E, 0, 3, 3), (SY, 0, 3, 2), (E, 0, 3, 5), (E, 0, 3, 7),
    (E, 0, 2, 1), (E, 0, 2, 5), (E, 0, 2, 3), (SY, 0, 3, 4), (E, 1, 2, 5), (E, 1, 2, 7),
    (E, 0, 2, 7), (E, 1, 2, 1), (E, 1, 1, 7), (E, 1, 1, 5), (E, 1, 2, 3), (E, 0, 1, 5),
    (E, 0, 1, 7), (E, 0, 1, 3), (E, 1, 1, 3), (SY, 0, 3, 6), (E, 1, 1, 1), (E, 1, 3, 7),
    (E, 1, 3, 3), (E, 2, 0, 7), (E, 2, 0, 1), (E, 2, 0, 5), (G, 3, 2, 6), (SI, 3, 2, 6),
    (E, 1, 0, 7), (E, 1, 0, 1), (E, 1, 0, 5), (SY, 0, 2, 0), (E, 1, 3, 1), (E, 1, 3, 5),
    (E, 2, 0, 3), (G, 3, 2, 7), (SI, 3, 2, 7), (E, 1, 0, 3), (E, 0, 1, 1), (SY, 1, 2, 4),
    (G, 0, 0, 7), (SI, 0, 0, 7), (SY, 1, 0, 6), (G, 3, 0, 7), (SI, 3, 0, 7), (G, 3, 2, 0),
    (SO, 3, 2, 0), (G, 3, 1, 7), (SI, 3, 1, 7), (G, 3, 2, 1), (SY, 0, 2, 4), (SO, 3, 2, 1),
    (G, 0, 0, 6), (SI, 0, 0, 6), (SY, 0, 2, 2), (G, 0, 0, 1), (SO, 0, 0, 1), (G, 3, 3, 6),
    (SI, 3, 3, 6), (G, 3, 0, 1), (SY, 1, 0, 0), (SO, 3, 0, 1), (G, 0, 3, 4), (SI, 0, 3, 4),
    (G, 3, 1, 1), (SO, 3, 1, 1), (SY, 1, 0, 4), (G, 0, 3, 6), (SI, 0, 3, 6), (G, 0, 0, 0),
    (SO, 0, 0, 0), (SY, 1, 2, 6), (G, 3, 1, 6), (SI, 3, 1, 6), (G, 3, 3, 0), (SO, 3, 3, 0),
    (SY, 0, 2, 6), (G, 1, 0, 6), (SI, 1, 0, 6), (SY, 0, 1, 4), (N, 0, 3, 0), (V, 0, 0, 0),
    (X, 0, 3, 0), (G, 0, 3, 0), (SO, 0, 3, 0), (SY, 1, 2, 0), (G, 3, 0, 6), (SI, 3, 0, 6),
    (G, 3, 1, 0), (SO, 3, 1, 0), (SY, 1, 1, 6), (G, 0, 2, 4), (SI, 0, 2, 4), (G, 1, 0, 0),
    (SO, 1, 0, 0), (G, 3, 3, 7), (SI, 3, 3, 7), (U, 0, 3, 0), (AY, 0, 3, 2), (AO, 0, 3, 2),
    (AI, 0, 3, 2), (G, 3, 0, 0), (SO, 3, 0, 0), (G, 0, 2, 6), (SY, 0, 1, 6), (SI, 0, 2, 6),
    (N, 0, 2, 0), (SY, 2, 0, 6), (X, 0, 2, 0), (G, 3, 3, 1), (SO, 3, 3, 1), (G, 1, 2, 4),
    (SI, 1, 2, 4), (SY, 1, 3, 6), (AO, 0, 3, 3), (AI, 0, 3, 3), (AO, 0, 3, 4), (SY, 1, 1, 4),
    (U, 0, 2, 0), (AI, 0, 2, 2), (AO, 0, 2, 2), (G, 0, 2, 0), (SY, 2, 0, 0), (SO, 0, 2, 0),
    (AI, 0, 0, 0), (SY, 0, 1, 2), (AO, 0, 3, 5), (AI, 0, 3, 0), (SY, 1, 2, 2), (AO, 0, 2, 4),
    (G, 1, 2, 6), (SI, 1, 2, 6), (AY, 0, 2, 2), (AO, 0, 0, 6), (G, 0, 1, 4), (SI, 0, 1, 4),
    (AY, 0, 0, 0), (AO, 0, 3, 6), (G, 2, 0, 6), (SI, 2, 0, 6), (SY, 1, 3, 2), (N, 1, 2, 0),
    (G, 1, 3, 6), (SI, 1, 3, 6), (SY, 2, 0, 4), (G, 1, 2, 0), (SO, 1, 2, 0), (AI, 0, 2, 3),
    (AO, 0, 2, 3), (N, 0, 1, 0), (X, 0, 1, 0), (SY, 1, 3, 0), (AI, 0, 3, 1), (G, 2, 0, 0),
    (SO, 2, 0, 0), (AY, 0, 0, 6), (AI, 3, 0, 0), (G, 1, 0, 4), (SY, 1, 3, 4), (SI, 1, 0, 4),
    (U, 0, 1, 0), (AO, 0, 1, 2), (G, 2, 0, 4), (AO, 0, 2, 5), (AI, 0, 1, 2), (SY, 1, 1, 2),
    (G, 1, 3, 0), (SO, 1, 3, 0), (SI, 2, 0, 4), (SY, 2, 0, 2), (AO, 0, 3, 7), (AI, 0, 2, 0),
    (SY, 1, 0, 2), (G, 1, 3, 4), (AO, 3, 0, 6), (AI, 3, 2, 0), (AY, 0, 1, 2), (G, 1, 1, 6),
    (AO, 0, 1, 4), (SI, 1, 1, 6), (SY, 1, 1, 0), (SI, 1, 3, 4), (N, 2, 0, 0), (X, 2, 0, 0),
    (AY, 3, 2, 0), (G, 1, 1, 4), (AO, 0, 2, 6), (SI, 1, 1, 4), (AY, 3, 0, 0), (AO, 3, 2, 6),
    (AI, 3, 3, 0), (AO, 0, 1, 3), (AY, 3, 0, 6), (U, 2, 0, 0), (AO, 2, 0, 2), (AY, 2, 0, 2),
    (AI, 2, 0, 2), (G, 1, 1, 0), (N, 1, 0, 0), (AY, 3, 3, 0), (SO, 1, 1, 0), (AI, 0, 1, 3),
    (N, 1, 3, 0), (N, 1, 1, 0), (SY, 0, 1, 0), (X, 1, 0, 0), (AO, 3, 3, 6), (AY, 3, 2, 6),
    (G, 0, 0, 5), (SI, 0, 0, 5), (AO, 2, 0, 3), (AI, 2, 0, 3), (AY, 3, 3, 6), (AO, 2, 0, 4),
    (G, 0, 0, 4), (SI, 0, 0, 4), (U, 1, 3, 0), (AY, 1, 3, 2), (U, 1, 2, 0), (AO, 0, 1, 5),
    (G, 3, 2, 5), (U, 1, 1, 0), (V, 0, 0, 1), (AY, 1, 2, 2), (SI, 3, 2, 5), (U, 1, 0, 0),
    (G, 3, 2, 4), (AO, 1, 2, 2), (SI, 3, 2, 4), (AY, 1, 1, 2), (G, 0, 0, 3), (AO, 1, 1, 2),
    (AI, 1, 3, 2), (AY, 1, 0, 2), (AI, 1, 2, 2), (AO, 1, 3, 2), (SY, 0, 0, 2), (G, 3, 2, 3),
    (AI, 1, 0, 2), (AO, 1, 0, 2), (G, 3, 1, 5), (SY, 3, 2, 2), (AI, 1, 1, 2), (AO, 2, 0, 5),
    (AY, 1, 3, 4), (G, 3, 3, 5), (SI, 3, 3, 5), (AO, 1, 3, 4), (G, 3, 0, 5), (AY, 1, 2, 4),
    (SI, 3, 0, 5), (AO, 1, 2, 4), (G, 3, 0, 4), (N, 0, 0, 0), (X, 0, 0, 0), (AY, 1, 0, 4),
    (SI, 3, 1, 5), (N, 3, 2, 0), (AO, 1, 0, 4), (X, 3, 2, 0), (SI, 3, 0, 4), (AY, 1, 1, 4),
    (G, 0, 1, 6), (AO, 1, 1, 4), (SI, 0, 1, 6), (U, 0, 0, 0), (AY, 0, 0, 2), (AI, 0, 0, 2),
    (G, 3, 0, 3), (AO, 0, 0, 2), (SY, 3, 0, 2), (G, 3, 3, 3), (U, 3, 2, 0), (G, 3, 1, 3),
    (AI, 3, 2, 2), (AO, 3, 2, 2), (SY, 3, 1, 2), (AI, 1, 1, 0), (AY, 1, 1, 0), (G, 3, 1, 4),
    (G, 0, 1, 0), (SO, 0, 1, 0), (SI, 3, 1, 4), (AY, 3, 2, 2), (AO, 0, 0, 4), (N, 3, 0, 0),
    (X, 3, 0, 0), (AY, 1, 2, 0), (AI, 1, 2, 0), (AO, 3, 2, 4), (SY, 3, 3, 2), (AI, 1, 3, 0),
    (AO, 1, 1, 6), (AY, 1, 3, 0), (G, 3, 3, 4), (SI, 3, 3, 4), (U, 3, 0, 0), (AO, 3, 0, 2),
    (AY, 0, 0, 4), (AI, 3, 0, 2), (AO, 1, 2, 6), (V, 0, 0, 2), (AI, 3, 1, 0), (N, 3, 1, 0),
    (X, 3, 1, 0), (AY, 3, 1, 0), (AO, 1, 3, 6), (AI, 2, 0, 0), (AY, 1, 3, 6), (N, 3, 3, 0),
    (AY, 1, 2, 6), (X, 3, 3, 0), (AO, 3, 0, 4), (U, 3, 1, 0), (AO, 3, 1, 2), (AI, 3, 1, 2),
    (AI, 1, 0, 0), (AY, 1, 1, 6), (AO, 3, 1, 6), (AI, 0, 2, 1), (AY, 3, 0, 2), (AO, 2, 0, 6),
    (U, 3, 3, 0), (AI, 3, 3, 2), (AO, 3, 3, 2), (AY, 3, 2, 4), (AI, 2, 0, 1), (AO, 3, 1, 4),
    (AY, 3, 3, 2), (AI, 0, 1, 0), (AO, 1, 0, 6), (AY, 3, 1, 2), (AO, 0, 2, 7), (AY, 3, 0, 4),
    (AY, 1, 0, 0), (AO, 3, 3, 4), (AY, 1, 0, 6), (AI, 0, 1, 1), (AO, 2, 0, 7), (AY, 3, 3, 4),
    (AO, 0, 1, 6), (AY, 3, 1, 4), (AY, 3, 1, 6), (AO, 0, 1, 7),
)


def lanes_of(shapes, g, ref, i):
    n = len(GROUPS[g].members)
    w = shapes[g][1] // n
    return ref if n == 1 else ref.at[..., i * w : (i + 1) * w]


def finish(shapes, *refs):
    n = len(GROUPS)
    full, own, st = refs[0:n], refs[n : 2 * n], refs[2 * n : 3 * n]
    vectors = refs[3 * n : 3 * n + 6]
    halves, nexts, news = (refs[3 * n + 6 + 8 * k : 3 * n + 14 + 8 * k] for k in range(3))
    sem, vec_sem = refs[3 * n + 30 :]
    for g, group in enumerate(GROUPS):
        w = shapes[g][1]
        for i, a in enumerate(group.members):
            if group.rows:
                pltpu.make_async_copy(lanes_of(shapes, g, full[g], i), halves[a], sem.at[0, g]).start()
            else:
                for b in range(8):
                    dst = halves[a].at[:, b * w : (b + 1) * w]
                    pltpu.make_async_copy(full[g].at[b], dst, sem.at[0, g]).start()
            pltpu.make_async_copy(lanes_of(shapes, g, own[g], i), nexts[a], sem.at[1, g]).start()
            pltpu.make_async_copy(lanes_of(shapes, g, st[g], i), news[a], sem.at[2, g]).start()
    copies = []
    for i, dst in enumerate((*halves[6:], *nexts[6:], *news[6:])):
        copies.append(pltpu.make_async_copy(vectors[i], dst, vec_sem.at[i]))
        copies[-1].start()
    for g in range(n):
        for k, ref in enumerate((full[g], own[g], st[g])):
            pltpu.make_async_copy(ref, ref, sem.at[k, g]).wait()
    for c in copies:
        c.wait()


def kernel(replicas, models, limit, shapes, *refs):
    slopes, slope_norm, slope_bias = refs[0:6], refs[6], refs[7]
    params, param_norm, param_bias = refs[8:14], refs[14], refs[15]
    states, state_norm, state_bias = refs[16:22], refs[22], refs[23]
    groups = range(len(GROUPS))
    n = len(GROUPS)
    full, own, st = refs[24 : 24 + n], refs[24 + n : 24 + 2 * n], refs[24 + 2 * n : 24 + 3 * n]
    half_norm, half_bias, next_norm, next_bias, new_norm, new_bias = refs[24 + 3 * n : 30 + 3 * n]
    scratch = list(refs[30 + 3 * n :])
    take = lambda: [scratch.pop(0) for _ in groups]
    xin, enc, rec, sq, sqr = (take() for _ in range(5))
    vs, vown, vrec, vnext, vag, vh_norm, vh_bias = (scratch.pop(0) for _ in range(7))
    rs_s, rs_r, ag_s, ag_r, n_s, n_r, v_s, v_r, w_s, w_r = (scratch.pop(0) for _ in range(10))
    load_sem, own_sem, st_sem, vown_sem = scratch

    r = lax.axis_index("replica")
    m = lax.axis_index("model")
    y, z = lax.rem(r, 2), r // 2
    side = z // 2
    slab = [(p + side * (3 - 2 * p)) * 2 + (y if d == 0 else 1 - y) for p in range(4) for d in (0, 1)]

    scale = 2.0**13 / (limit * replicas)
    rate = replicas ** (-0.5)

    def encode(x):
        t = x * scale
        t2 = t * t
        t4 = t2 * t2
        return (t4 * t4 * t).astype(jnp.bfloat16)

    def decode(c):
        f = c.astype(jnp.float32)
        a = jnp.exp(jnp.log(jnp.abs(f)) * (1.0 / root)) * (1.0 / scale)
        return jnp.where(f < 0, -a, a)

    lanes = functools.partial(lanes_of, shapes)
    at = {k: i for i, k in enumerate(CHUNKS)}
    unit = lambda g: shapes[g][0] // sum(SIZES[g])
    height = lambda g, c: unit(g) * SIZES[g][c]
    rows = lambda g, c: pl.ds(unit(g) * sum(SIZES[g][:c]), height(g, c))

    def source(g, c, s):
        w = shapes[g][1]
        if GROUPS[g].rows:
            return xin[g].at[slab[s], rows(g, c)]
        return xin[g].at[rows(g, c), pl.ds(pl.multiple_of(slab[s] * w, w), w)]

    def loop(g, c, body):
        h, w = height(g, c), shapes[g][1]
        step = min(h, max(16, STEP // w // 16 * 16))
        while h % step:
            step -= 16
        lax.fori_loop(0, h // step, lambda i, c: (body(pl.ds(pl.multiple_of(i * step, step), step)), c)[1], 0)

    def remote(src, dst, s, d, peer, axis="replica"):
        return pltpu.make_async_remote_copy(
            src_ref=src, dst_ref=dst, send_sem=s, recv_sem=d, device_id={axis: peer}, device_id_type=MESH
        )

    def whole(ref, sem):
        pltpu.make_async_copy(ref, ref, sem).wait()

    barrier = pltpu.get_barrier_semaphore()

    def greet(axis, to):
        pl.semaphore_signal(barrier, inc=1, device_id={axis: to}, device_id_type=MESH)

    @pl.when(z > 0)
    def _():
        greet("replica", r - 2)

    @pl.when(z < 3)
    def _():
        greet("replica", r + 2)

    greet("replica", z * 2 + (1 - y))
    for j in range(1, models):
        greet("model", lax.rem(m + j, models))

    def chunk_of(g, c):
        return xin[g].at[:, rows(g, c)] if GROUPS[g].rows else xin[g].at[rows(g, c)]

    def load(g, c):
        for i, a in enumerate(GROUPS[g].members):
            src = slopes[a].at[:, rows(g, c)] if GROUPS[g].rows else slopes[a].at[rows(g, c)]
            pltpu.make_async_copy(src, lanes(g, chunk_of(g, c), i), load_sem.at[at[g, c]]).start()

    def load_own():
        for g in OWN:
            for i, a in enumerate(GROUPS[g].members):
                pltpu.make_async_copy(params[a], lanes(g, own[g], i), own_sem.at[g]).start()
                pltpu.make_async_copy(states[a], lanes(g, st[g], i), st_sem.at[g]).start()

    for g, c in CHUNKS[:2]:
        load(g, c)
    vs[0:1, :] = slope_norm[...]
    vs[1:2, :] = slope_bias[...]
    for g in groups:
        if not GROUPS[g].rows:
            sq[g][...] = jnp.zeros_like(sq[g])

    def rule(p, s, v):
        s = hold_rate * s + (1.0 - hold_rate) * v * v
        return p - learn_rate * v * lax.rsqrt(s + 1e-06), s

    def fold(x):
        total = x[:, 0:128]
        for k in range(128, x.shape[1], 128):
            total = total + x[:, k : k + 128]
        return jnp.sum(total, axis=1, keepdims=True)

    width = vs.shape[1] // replicas

    def vec_out(j):
        to = lax.rem(r + j, replicas)
        return remote(
            vs.at[:, pl.ds(pl.multiple_of(to * width, width), width)],
            vrec.at[j - 1], v_s.at[j - 1], v_r.at[j - 1], to,
        )

    def vec_back(j):
        return remote(vnext, vag.at[j - 1], w_s.at[j - 1], w_r.at[j - 1], lax.rem(r + j, replicas))

    def vec_start():
        pltpu.make_async_copy(vs.at[:, pl.ds(pl.multiple_of(r * width, width), width)], vown, vown_sem).start()
        for j in range(1, replicas):
            vec_out(j).start()

    def vec_update():
        pltpu.make_async_copy(vown, vown, vown_sem).wait()
        total = vown[...]
        for j in range(1, replicas):
            vec_out(j).wait_recv()
            total = total + vrec[j - 1]
        v = total * rate
        p, s = rule(param_norm[...], state_norm[...], v[0:1, :])
        next_norm[...] = p
        new_norm[...] = s
        vnext[0:1, :] = p
        p, s = rule(param_bias[...], state_bias[...], v[1:2, :])
        next_bias[...] = p
        new_bias[...] = s
        vnext[1:2, :] = p
        for j in range(1, replicas):
            vec_back(j).start()

    def vec_finish():
        vh_norm[pl.ds(r, 1), :] = vnext[0:1, :]
        vh_bias[pl.ds(r, 1), :] = vnext[1:2, :]
        for j in range(1, replicas):
            vec_back(j).wait_recv()
            at = lax.rem(r + replicas - j, replicas)
            vh_norm[pl.ds(at, 1), :] = vag[j - 1, 0:1, :]
            vh_bias[pl.ds(at, 1), :] = vag[j - 1, 1:2, :]
        half_norm[...] = vh_norm[...].astype(jnp.bfloat16)
        half_bias[...] = vh_bias[...].astype(jnp.bfloat16)

    def run(mid, order):
        mine = 1 if mid else 0
        peers = {}
        if mid:
            peers[SO] = peers[AO] = side * 6 + y
            peers[SI] = peers[AI] = (3 - z) * 2 + y
        else:
            peers[SI] = peers[AI] = (1 + side) * 2 + y
        peers[SY] = peers[AY] = z * 2 + (1 - y)
        done = set()
        ahead = list(CHUNKS[2:])

        def kind(g, c):
            return SUMS[g][c]

        def landing(g, c, by, s):
            if kind(g, c) == A:
                return (0, 7, 3)[by] + s // 2
            return (10, 6 + s, s - 2)[by]

        def outgoing(g, c, op, s):
            p = s // 2
            if kind(g, c) == A:
                if op == SY:
                    return p
                return 3 + p if p else 4
            if op == SY:
                return 6
            if not mid:
                return s - 2
            return s - 4 if p >= 2 else 4 + s

        def across(op, s):
            return (3 - s // 2) * 2 + s % 2 if mid and op in (SI, AI) else s

        def send(op, g, c, s):
            by = {SY: 0, SO: 1, SI: 1 if mid else 2}[op]
            slot = landing(g, c, by, across(op, s))
            return remote(
                enc[g].at[outgoing(g, c, op, s), rows(g, c)],
                rec[g].at[slot, rows(g, c)],
                rs_s.at[g],
                rs_r.at[at[g, c], slot],
                peers[op],
            )

        def gather(op, g, c, s):
            to = s + 1 if op == AY else across(op, s)
            ref = full[g].at[slab[s], rows(g, c)]
            link = {AY: 0, AI: 1, AO: 2}[op]
            return remote(ref, ref, ag_s.at[at[g, c], link], ag_r.at[at[g, c], to], peers[op])

        def got(g, c, s):
            if s != mine * 2 and (g, c, s) not in done:
                done.add((g, c, s))
                ref = full[g].at[slab[s], rows(g, c)]
                whole(ref, ag_r.at[at[g, c], s])

        def arrived(g, c, by, s):
            slot = landing(g, c, by, s)
            ref = rec[g].at[slot, rows(g, c)]
            whole(ref, rs_r.at[at[g, c], slot])
            return ref

        def once(key, ref, sem):
            if key not in done:
                done.add(key)
                whole(ref, sem)

        def loaded(g, c):
            while (g, c) in ahead:
                load(*ahead.pop(0))
                if not ahead:
                    load_own()
            once((-1, g, c), chunk_of(g, c), load_sem.at[at[g, c]])

        def parts(g, c, s):
            loaded(g, c)
            by = []
            a, p = kind(g, c) == A, s // 2
            if a or s == mine * 2:
                by.append(0)
            if mid and p >= 1:
                by.append(2)
            if p == mine or (mid and p == 0):
                by.append(1)
            return [arrived(g, c, b, s) for b in by]

        def encode_op(g, c, s, op):
            loaded(g, c)
            src, dst = source(g, c, s), enc[g].at[outgoing(g, c, op, s), rows(g, c)]

            def body(d):
                dst[d, :] = encode(src[d, :])

            loop(g, c, body)

        def add_op(g, c, s):
            src = source(g, c, s)
            op = SY if s // 2 == mine else SO if mid and s < 2 else SI
            dst = enc[g].at[outgoing(g, c, op, s), rows(g, c)]
            got = parts(g, c, s)

            def body(d):
                total = src[d, :]
                for ref in got:
                    total = total + decode(ref[d, :])
                dst[d, :] = encode(total)

            loop(g, c, body)

        def mean_op(g, c):
            acc = source(g, c, mine * 2)
            got = parts(g, c, mine * 2)
            once((-2, g), own[g], own_sem.at[g])
            held = own[g].at[rows(g, c)]
            k = len(GROUPS[g].members)
            w = shapes[g][1] // k

            def mean(d):
                total = acc[d, :]
                for ref in got:
                    total = total + decode(ref[d, :])
                v = total * rate
                acc[d, :] = v
                return v

            if GROUPS[g].rows:
                sums = sq[g].at[rows(g, c)]

                def body(d):
                    v, p = mean(d), held[d, :]
                    v, p = v * v, p * p
                    lane = lax.broadcasted_iota(jnp.int32, (v.shape[0], 128), 1)
                    out = jnp.zeros((v.shape[0], 128), jnp.float32)
                    for i in range(k):
                        cols = slice(i * w, (i + 1) * w)
                        out = jnp.where(lane == 2 * i, fold(p[:, cols]), out)
                        out = jnp.where(lane == 2 * i + 1, fold(v[:, cols]), out)
                    sums[d, :] = out

            else:

                def body(d):
                    v, p = mean(d), held[d, :]
                    sq[g][0] += jnp.sum((p * p).reshape(-1, 8, w), axis=0)
                    sq[g][1] += jnp.sum((v * v).reshape(-1, 8, w), axis=0)

            loop(g, c, body)

        def norms(g, c, j):
            if GROUPS[g].rows:
                src, dst = sq[g].at[rows(g, c)], sqr[g].at[j - 1, rows(g, c)]
            else:
                src, dst = sq[g], sqr[g].at[j - 1]
            return remote(src, dst, n_s.at[at[g, c], j - 1], n_r.at[at[g, c], j - 1], lax.rem(m + j, models), "model")

        def update_op(g, c):
            first = c if GROUPS[g].rows else 0
            for j in range(1, models):
                if (-4, g, first, j) not in done:
                    done.add((-4, g, first, j))
                    norms(g, first, j).wait_recv()
            once((-3, g), st[g], st_sem.at[g])
            acc, half = source(g, c, mine * 2), full[g].at[slab[mine * 2], rows(g, c)]
            held, hold = own[g].at[rows(g, c)], st[g].at[rows(g, c)]
            k = len(GROUPS[g].members)
            w = shapes[g][1] // k

            def put(d, cols, t):
                p, s = rule(held[d, cols], hold[d, cols], acc[d, cols] * t)
                held[d, cols] = p
                hold[d, cols] = s
                half[d, cols] = p.astype(jnp.bfloat16)

            if GROUPS[g].rows:
                sums = [sq[g].at[rows(g, c)]] + [sqr[g].at[j, rows(g, c)] for j in range(models - 1)]

                def body(d):
                    total = sums[0][d, :]
                    for ref in sums[1:]:
                        total = total + ref[d, :]
                    lane = lax.broadcasted_iota(jnp.int32, total.shape, 1)
                    pick = lambda i: jnp.sum(jnp.where(lane == i, total, 0.0), axis=1, keepdims=True)
                    for i in range(k):
                        t = jnp.sqrt(pick(2 * i)) * lax.rsqrt(pick(2 * i + 1) + 1e-06)
                        put(d, slice(i * w, (i + 1) * w), t)

            else:
                total = sq[g][...]
                for j in range(models - 1):
                    total = total + sqr[g][j]
                total = jnp.sum(total, axis=1, keepdims=True)
                t = jnp.sqrt(total[0]) * lax.rsqrt(total[1] + 1e-06)

                def body(d):
                    put(d, slice(None), t)

            loop(g, c, body)

        met = False
        for i, (op, g, c, s) in enumerate(order):
            if ahead and i % 2:
                load(*ahead.pop(0))
                if not ahead:
                    load_own()
            if op not in (E, G) and not met:
                met = True
                pl.semaphore_wait(barrier, models + (2 if mid else 1))
            if op == E:
                encode_op(g, c, s, SY if kind(g, c) == A else SI)
            elif op == G:
                add_op(g, c, s)
            elif op in (SY, SI, SO):
                send(op, g, c, s).start()
            elif op == N:
                mean_op(g, c)
            elif op == X:
                for j in range(1, models):
                    norms(g, c, j).start()
            elif op == U:
                update_op(g, c)
            elif op == V:
                (vec_start, vec_update, vec_finish)[s]()
            else:
                got(g, c, s)
                gather(op, g, c, s).start()

        for g, c in CHUNKS:
            for s in range(8):
                got(g, c, s)
        for g in groups:
            whole(enc[g], rs_s.at[g])
        for g, c in CHUNKS:
            for link, count in enumerate(SENT[mid][BACK[g][c]]):
                if count:
                    whole(full[g].at[pl.ds(0, count), rows(g, c)], ag_s.at[at[g, c], link])
            if GROUPS[g].rows or c == 0:
                for j in range(1, models):
                    norms(g, c, j).wait_send()
        for j in range(1, replicas):
            vec_out(j).wait_send()
            vec_back(j).wait_send()

    end = jnp.logical_or(z == 0, z == 3)

    @pl.when(end)
    def _():
        run(False, END)

    @pl.when(jnp.logical_not(end))
    def _():
        run(True, MID)


def fused(replicas, models, shapes, *args):
    slopes, params = args[0:6], args[8:14]
    f32, bf16 = jnp.float32, jnp.bfloat16
    vec = args[6].shape[1]
    width = vec // replicas
    row = lambda a: a.reshape(1, -1)
    by_rows = [a in g.members and g.rows for a in range(6) for g in GROUPS if a in g.members]
    cut = lambda a, rows: a.reshape(replicas, -1, a.shape[-1]) if rows else a[0]
    args = (
        *(cut(a, rows) for a, rows in zip(slopes, by_rows)), *args[6:14],
        row(args[14]), row(args[15]), *args[16:22], row(args[22]), row(args[23]),
    )
    S = jax.ShapeDtypeStruct
    n, chunks = len(GROUPS), len(CHUNKS)
    held = [((replicas, *s), bf16) for s in shapes] + [(s, f32) for s in shapes] * 2
    held += [((replicas, width), bf16)] * 2 + [((1, width), f32)] * 4
    ANY, VM = pl.BlockSpec(memory_space=pl.ANY), pl.BlockSpec(memory_space=pltpu.VMEM)
    part = [ANY] * 6 + [VM] * 2
    scratch = [
        pltpu.VMEM((replicas, *s) if g.rows else (s[0], s[1] * replicas), f32) for g, s in zip(GROUPS, shapes)
    ]
    scratch += [pltpu.VMEM((7, *s), bf16) for s in shapes]
    scratch += [pltpu.VMEM((11 if B in k else 9, *s), bf16) for k, s in zip(SUMS, shapes)]
    sq = [(s[0], 128) if g.rows else (2, 8, s[1]) for g, s in zip(GROUPS, shapes)]
    scratch += [pltpu.VMEM(s, f32) for s in sq]
    scratch += [pltpu.VMEM((models - 1, *s), f32) for s in sq]
    scratch += [
        pltpu.VMEM((2, vec), f32),
        pltpu.VMEM((2, width), f32),
        pltpu.VMEM((replicas - 1, 2, width), f32),
        pltpu.VMEM((2, width), f32),
        pltpu.VMEM((replicas - 1, 2, width), f32),
        pltpu.VMEM((replicas, width), f32),
        pltpu.VMEM((replicas, width), f32),
    ]
    dma = pltpu.SemaphoreType.DMA
    scratch += [dma((n,)), dma((chunks, 11)), dma((chunks, 3)), dma((chunks, 8))]
    scratch += [dma((chunks, models - 1))] * 2 + [dma((replicas - 1,))] * 4
    scratch += [dma((chunks,))] + [dma((n,))] * 2 + [dma(())]
    out = pl.pallas_call(
        functools.partial(kernel, replicas, models, 4.0, shapes),
        out_shape=[pltpu.VMEM(*h) for h in held],
        in_specs=part * 3,
        out_specs=[VM] * len(held),
        scratch_shapes=scratch,
        compiler_params=pltpu.CompilerParams(
            collective_id=0, has_side_effects=True, vmem_limit_bytes=54 * 1024 * 1024
        ),
    )(*args)
    outs = [
        S((replicas, a.shape[1] // replicas, a.shape[2]) if rows else a.shape[1:], bf16)
        for a, rows in zip(slopes, by_rows)
    ]
    outs += [S((replicas, width), bf16)] * 2
    for _ in range(2):
        outs += [S(a.shape, f32) for a in params] + [S((1, width), f32)] * 2
    out = pl.pallas_call(
        functools.partial(finish, shapes),
        out_shape=outs,
        in_specs=[VM] * len(held),
        out_specs=[ANY] * len(outs),
        scratch_shapes=[dma((3, n)), dma((6,))],
        compiler_params=pltpu.CompilerParams(vmem_limit_bytes=1024 * 1024),
    )(*out)
    flat = lambda a: a.reshape(-1)
    return (
        *(a.reshape(-1, a.shape[-1]) for a in out[0:6]), flat(out[6]), flat(out[7]),
        *out[8:14], flat(out[14]), flat(out[15]),
        *out[16:22], flat(out[22]), flat(out[23]),
    )


def plain(
    slope_up,
    slope_down,
    slope_query,
    slope_key,
    slope_value,
    slope_mixed,
    slope_norm,
    slope_bias,
    param_up,
    param_down,
    param_query,
    param_key,
    param_value,
    param_mixed,
    param_norm,
    param_bias,
    state_up,
    state_down,
    state_query,
    state_key,
    state_value,
    state_mixed,
    state_norm,
    state_bias,
):
    mean_up, mean_down, mean_query, mean_key, mean_value, mean_mixed = (
        lax.psum_scatter(slope_up[0], "replica", scatter_dimension=0, tiled=True),
        lax.psum_scatter(slope_down[0], "replica", scatter_dimension=1, tiled=True),
        lax.psum_scatter(slope_query[0], "replica", scatter_dimension=0, tiled=True),
        lax.psum_scatter(slope_key[0], "replica", scatter_dimension=0, tiled=True),
        lax.psum_scatter(slope_value[0], "replica", scatter_dimension=0, tiled=True),
        lax.psum_scatter(slope_mixed[0], "replica", scatter_dimension=1, tiled=True),
    )
    whole_norm, whole_bias = lax.psum((slope_norm[0], slope_bias[0]), "replica")
    place = lax.axis_index("replica")
    mean_norm = lax.dynamic_slice_in_dim(
        whole_norm, place * param_norm.shape[0], param_norm.shape[0]
    )
    mean_bias = lax.dynamic_slice_in_dim(
        whole_bias, place * param_bias.shape[0], param_bias.shape[0]
    )
    mean_rate = lax.axis_size("replica") ** (-0.5)
    mean_up = mean_up * mean_rate
    mean_down = mean_down * mean_rate
    mean_query = mean_query * mean_rate
    mean_key = mean_key * mean_rate
    mean_value = mean_value * mean_rate
    mean_mixed = mean_mixed * mean_rate
    mean_norm = mean_norm * mean_rate
    mean_bias = mean_bias * mean_rate
    (
        own_up,
        own_down,
        own_query,
        own_key,
        own_value,
        own_mixed,
        slope_up_norm,
        slope_down_norm,
        slope_query_norm,
        slope_key_norm,
        slope_value_norm,
        slope_mixed_norm,
    ) = lax.psum(
        (
            jnp.sum(param_up * param_up, axis=1, keepdims=True),
            jnp.sum(param_down * param_down, axis=0, keepdims=True),
            jnp.sum(param_query * param_query, axis=1, keepdims=True),
            jnp.sum(param_key * param_key, axis=1, keepdims=True),
            jnp.sum(param_value * param_value, axis=1, keepdims=True),
            jnp.sum(param_mixed * param_mixed, axis=0, keepdims=True),
            jnp.sum(mean_up * mean_up, axis=1, keepdims=True),
            jnp.sum(mean_down * mean_down, axis=0, keepdims=True),
            jnp.sum(mean_query * mean_query, axis=1, keepdims=True),
            jnp.sum(mean_key * mean_key, axis=1, keepdims=True),
            jnp.sum(mean_value * mean_value, axis=1, keepdims=True),
            jnp.sum(mean_mixed * mean_mixed, axis=0, keepdims=True),
        ),
        "model",
    )
    mean_up = mean_up * (jnp.sqrt(own_up) * lax.rsqrt(slope_up_norm + 1e-06))
    mean_down = mean_down * (jnp.sqrt(own_down) * lax.rsqrt(slope_down_norm + 1e-06))
    mean_query = mean_query * (jnp.sqrt(own_query) * lax.rsqrt(slope_query_norm + 1e-06))
    mean_key = mean_key * (jnp.sqrt(own_key) * lax.rsqrt(slope_key_norm + 1e-06))
    mean_value = mean_value * (jnp.sqrt(own_value) * lax.rsqrt(slope_value_norm + 1e-06))
    mean_mixed = mean_mixed * (jnp.sqrt(own_mixed) * lax.rsqrt(slope_mixed_norm + 1e-06))
    state_new_up = hold_rate * state_up + (1.0 - hold_rate) * mean_up * mean_up
    next_up = param_up - learn_rate * mean_up * lax.rsqrt(state_new_up + 1e-06)
    state_new_down = hold_rate * state_down + (1.0 - hold_rate) * mean_down * mean_down
    next_down = param_down - learn_rate * mean_down * lax.rsqrt(state_new_down + 1e-06)
    state_new_query = hold_rate * state_query + (1.0 - hold_rate) * mean_query * mean_query
    next_query = param_query - learn_rate * mean_query * lax.rsqrt(state_new_query + 1e-06)
    state_new_key = hold_rate * state_key + (1.0 - hold_rate) * mean_key * mean_key
    next_key = param_key - learn_rate * mean_key * lax.rsqrt(state_new_key + 1e-06)
    state_new_value = hold_rate * state_value + (1.0 - hold_rate) * mean_value * mean_value
    next_value = param_value - learn_rate * mean_value * lax.rsqrt(state_new_value + 1e-06)
    state_new_mixed = hold_rate * state_mixed + (1.0 - hold_rate) * mean_mixed * mean_mixed
    next_mixed = param_mixed - learn_rate * mean_mixed * lax.rsqrt(state_new_mixed + 1e-06)
    state_new_norm = hold_rate * state_norm + (1.0 - hold_rate) * mean_norm * mean_norm
    next_norm = param_norm - learn_rate * mean_norm * lax.rsqrt(state_new_norm + 1e-06)
    state_new_bias = hold_rate * state_bias + (1.0 - hold_rate) * mean_bias * mean_bias
    next_bias = param_bias - learn_rate * mean_bias * lax.rsqrt(state_new_bias + 1e-06)
    half_up, half_down, half_query, half_key, half_value, half_mixed, half_norm, half_bias = (
        lax.all_gather(next_up.astype(jnp.bfloat16), "replica", axis=0, tiled=True),
        lax.all_gather(next_down.astype(jnp.bfloat16), "replica", axis=1, tiled=True),
        lax.all_gather(next_query.astype(jnp.bfloat16), "replica", axis=0, tiled=True),
        lax.all_gather(next_key.astype(jnp.bfloat16), "replica", axis=0, tiled=True),
        lax.all_gather(next_value.astype(jnp.bfloat16), "replica", axis=0, tiled=True),
        lax.all_gather(next_mixed.astype(jnp.bfloat16), "replica", axis=1, tiled=True),
        lax.all_gather(next_norm.astype(jnp.bfloat16), "replica", axis=0, tiled=True),
        lax.all_gather(next_bias.astype(jnp.bfloat16), "replica", axis=0, tiled=True),
    )
    return (
        half_up,
        half_down,
        half_query,
        half_key,
        half_value,
        half_mixed,
        half_norm,
        half_bias,
        next_up,
        next_down,
        next_query,
        next_key,
        next_value,
        next_mixed,
        next_norm,
        next_bias,
        state_new_up,
        state_new_down,
        state_new_query,
        state_new_key,
        state_new_value,
        state_new_mixed,
        state_new_norm,
        state_new_bias,
    )


def solution(mesh):
    replicas, models = mesh.shape["replica"], mesh.shape["model"]

    def local(*args):
        if replicas != 2**3 or any(a.shape[k] % 128 for a in args[8:14] for k in (0, 1)):
            return plain(*args)
        shapes = []
        for g, sizes in zip(GROUPS, SIZES):
            h, w = args[8 + g.members[0]].shape
            shapes.append((h, w * len(g.members)))
            if h % (16 * sum(sizes)) or (w != 128 and not g.rows):
                return plain(*args)
        if args[14].shape[0] % 128:
            return plain(*args)
        return fused(replicas, models, shapes, *args)

    placed = (
        P("replica", None, "model"),
        P("replica", "model", None),
        P("replica", None, "model"),
        P("replica", None, "model"),
        P("replica", None, "model"),
        P("replica", "model", None),
        P("replica", None),
        P("replica", None),
        P("replica", "model"),
        P("model", "replica"),
        P("replica", "model"),
        P("replica", "model"),
        P("replica", "model"),
        P("model", "replica"),
        P("replica"),
        P("replica"),
        P("replica", "model"),
        P("model", "replica"),
        P("replica", "model"),
        P("replica", "model"),
        P("replica", "model"),
        P("model", "replica"),
        P("replica"),
        P("replica"),
    )
    return jax.shard_map(
        local,
        mesh=mesh,
        in_specs=placed,
        out_specs=(
            P(None, "model"),
            P("model", None),
            P(None, "model"),
            P(None, "model"),
            P(None, "model"),
            P("model", None),
            P(),
            P(),
            P("replica", "model"),
            P("model", "replica"),
            P("replica", "model"),
            P("replica", "model"),
            P("replica", "model"),
            P("model", "replica"),
            P("replica"),
            P("replica"),
            P("replica", "model"),
            P("model", "replica"),
            P("replica", "model"),
            P("replica", "model"),
            P("replica", "model"),
            P("model", "replica"),
            P("replica"),
            P("replica"),
        ),
        check_vma=False,
    )
```

```python
import functools

import jax
import jax.numpy as jnp
from jax import lax
from jax.experimental import pallas as pl
from jax.experimental.pallas import tpu as pltpu
from jax.sharding import PartitionSpec as P

learn_rate = 0.025
hold_rate = 0.7
root = 9
MESH = pl.DeviceIdType.MESH


class Group:
    def __init__(self, members, rows):
        self.members = members
        self.rows = rows


GROUPS = (Group((0,), True), Group((1,), False), Group((5,), False), Group((2, 3, 4), True))
A, B = 0, 1
E, G, N, X, U, V, SY, SI, SO, AY, AI, AO = range(12)
SIZES = ((2, 2, 2, 2), (2, 2, 2, 2), (8,), (2, 2, 2, 2))
SUMS = ((B, B, B, A), (A, A, A, A), (A,), (A, B, B, A))
BACK = ((A, A, A, A), (A, B, A, A), (B,), (B, A, A, B))
CHUNKS = ((3, 2), (3, 0), (3, 1), (2, 0), (3, 3), (1, 3), (0, 0), (1, 0), (0, 3), (1, 2), (0, 1), (1, 1), (0, 2))
OWN = (3, 2, 0, 1)
SENT = (((4, 1, 0), (1, 2, 0)), ((4, 2, 3), (1, 4, 6)))
STEP = 16384
END = (
    (E, 3, 2, 6), (SI, 3, 2, 6), (E, 3, 2, 7), (SI, 3, 2, 7), (E, 3, 0, 3), (SY, 3, 0, 2),
    (E, 3, 0, 5), (SY, 3, 0, 4), (E, 3, 1, 7), (E, 3, 1, 6), (E, 2, 0, 5), (E, 2, 0, 3),
    (SI, 3, 1, 7), (E, 3, 3, 3), (E, 3, 3, 7), (SY, 2, 0, 4), (E, 2, 0, 7), (E, 3, 3, 1),
    (E, 0, 0, 7), (E, 2, 0, 1), (E, 3, 3, 5), (SI, 0, 0, 7), (E, 1, 0, 5), (E, 0, 0, 6),
    (SY, 3, 3, 2), (E, 1, 3, 7), (E, 0, 3, 7), (E, 1, 2, 7), (E, 1, 3, 5), (E, 0, 1, 7),
    (SI, 0, 1, 7), (E, 0, 1, 6), (E, 1, 1, 7), (E, 1, 1, 5), (E, 0, 2, 7), (SY, 2, 0, 2),
    (E, 1, 2, 5), (E, 3, 0, 7), (G, 3, 0, 2), (E, 1, 3, 3), (E, 1, 0, 3), (SI, 3, 1, 6),
    (E, 1, 1, 3), (E, 1, 2, 3), (SY, 3, 3, 6), (E, 0, 2, 5), (E, 1, 0, 7), (G, 3, 0, 4),
    (E, 0, 3, 1), (E, 0, 3, 3), (E, 3, 1, 4), (SI, 3, 0, 4), (E, 1, 3, 1), (E, 3, 1, 5),
    (SY, 2, 0, 6), (E, 0, 3, 5), (E, 0, 2, 4), (G, 2, 0, 4), (E, 3, 0, 1), (E, 0, 1, 5),
    (SI, 0, 2, 7), (E, 1, 1, 1), (E, 0, 2, 3), (SY, 3, 3, 0), (E, 0, 2, 2), (E, 3, 1, 2),
    (G, 3, 3, 2), (E, 1, 2, 1), (SI, 0, 1, 6), (E, 3, 1, 3), (E, 1, 0, 1), (E, 0, 1, 3),
    (E, 0, 1, 4), (E, 0, 0, 5), (SY, 2, 0, 0), (E, 0, 1, 2), (E, 0, 2, 6), (G, 2, 0, 2),
    (E, 0, 0, 4), (SI, 2, 0, 4), (E, 0, 0, 3), (E, 0, 0, 2), (SY, 3, 3, 4), (E, 3, 2, 5),
    (E, 3, 2, 4), (G, 3, 3, 6), (E, 3, 2, 3), (E, 3, 2, 2), (SI, 3, 0, 2), (SY, 1, 0, 4),
    (G, 2, 0, 6), (SY, 1, 2, 6), (SI, 0, 0, 6), (G, 3, 2, 1), (SI, 2, 0, 6), (SY, 1, 1, 6),
    (G, 3, 1, 1), (SI, 3, 3, 6), (G, 3, 3, 4), (SY, 3, 1, 0), (SI, 2, 0, 2), (G, 0, 0, 1),
    (G, 1, 0, 4), (SY, 1, 3, 6), (SI, 3, 3, 4), (SY, 1, 1, 4), (G, 0, 1, 1), (G, 1, 2, 6),
    (SI, 1, 0, 4), (SY, 0, 3, 6), (G, 1, 1, 6), (SI, 3, 3, 2), (N, 3, 1, 0), (V, 0, 0, 0),
    (SY, 1, 3, 4), (X, 3, 1, 0), (SI, 1, 2, 6), (G, 0, 2, 1), (G, 1, 3, 6), (SY, 3, 2, 0),
    (SI, 1, 1, 6), (G, 1, 1, 4), (SY, 1, 2, 4), (SI, 1, 3, 6), (SY, 3, 0, 6), (U, 3, 1, 0),
    (G, 0, 3, 6), (AI, 3, 1, 0), (SY, 1, 3, 2), (G, 1, 3, 4), (SI, 1, 3, 4), (SY, 1, 0, 2),
    (N, 3, 2, 0), (X, 3, 2, 0), (SI, 1, 1, 4), (N, 2, 0, 0), (SY, 1, 1, 2), (X, 2, 0, 0),
    (G, 1, 2, 4), (SI, 1, 2, 4), (N, 3, 3, 0), (X, 3, 3, 0), (G, 3, 0, 6), (SY, 1, 2, 2),
    (SI, 0, 2, 5), (U, 3, 2, 0), (SY, 0, 1, 0), (G, 1, 3, 2), (SI, 1, 3, 2), (U, 2, 0, 0),
    (G, 1, 0, 2), (AY, 3, 2, 0), (U, 3, 3, 0), (SI, 3, 0, 6), (G, 1, 1, 2), (SY, 1, 0, 6),
    (SI, 1, 1, 2), (SY, 0, 3, 0), (G, 1, 2, 2), (SI, 1, 0, 2), (SY, 0, 2, 0), (N, 0, 1, 0),
    (X, 0, 1, 0), (SI, 1, 2, 2), (SY, 0, 3, 2), (SI, 3, 1, 4), (G, 1, 0, 6), (SY, 1, 3, 0),
    (SI, 3, 1, 5), (SY, 0, 3, 4), (U, 0, 1, 0), (AI, 3, 2, 0), (SY, 3, 0, 0), (SI, 0, 2, 4),
    (SI, 0, 1, 5), (G, 0, 3, 2), (AY, 3, 3, 0), (SY, 1, 1, 0), (SI, 0, 2, 3), (N, 1, 3, 0),
    (V, 0, 0, 1), (AY, 2, 0, 0), (SI, 0, 2, 2), (G, 0, 3, 4), (SY, 0, 0, 0), (AI, 0, 1, 0),
    (AY, 3, 1, 0), (SI, 1, 0, 6), (N, 1, 1, 0), (AY, 0, 1, 0), (N, 3, 0, 0), (SI, 3, 1, 2),
    (X, 3, 0, 0), (SY, 1, 2, 0), (SI, 3, 1, 3), (SY, 1, 0, 0), (N, 0, 0, 0), (SI, 0, 1, 3),
    (X, 0, 0, 0), (AY, 3, 1, 6), (SI, 0, 1, 4), (U, 3, 0, 0), (AY, 1, 0, 2), (SI, 0, 0, 5),
    (AY, 1, 2, 2), (N, 1, 2, 0), (AI, 3, 3, 1), (U, 0, 0, 0), (AY, 0, 0, 0), (SI, 0, 1, 2),
    (AY, 3, 2, 6), (SI, 0, 3, 4), (AY, 1, 3, 2), (SI, 0, 2, 6), (AY, 1, 0, 4), (SI, 0, 3, 6),
    (AY, 3, 0, 0), (SI, 0, 0, 4), (AY, 1, 3, 4), (SI, 0, 3, 2), (AY, 1, 2, 4), (AI, 0, 0, 0),
    (AY, 0, 1, 6), (SI, 0, 0, 3), (N, 1, 0, 0), (X, 1, 0, 0), (AY, 0, 2, 2), (AI, 3, 3, 0),
    (AI, 2, 0, 1), (AY, 0, 2, 4), (SI, 0, 0, 2), (AY, 3, 1, 2), (U, 1, 0, 0), (U, 1, 2, 0),
    (AY, 1, 0, 0), (U, 1, 1, 0), (U, 1, 3, 0), (SI, 3, 2, 5), (AY, 1, 2, 0), (AI, 3, 0, 0),
    (AY, 0, 1, 2), (AI, 1, 0, 0), (N, 0, 2, 0), (X, 0, 2, 0), (V, 0, 0, 2), (AY, 1, 1, 0),
    (SI, 3, 2, 4), (AY, 1, 3, 0), (SI, 3, 2, 3), (N, 0, 3, 0), (X, 0, 3, 0), (AI, 1, 3, 0),
    (AY, 3, 1, 4), (U, 0, 2, 0), (AI, 0, 2, 0), (AY, 0, 2, 0), (SI, 3, 2, 2), (AY, 0, 3, 2),
    (U, 0, 3, 0), (AI, 1, 2, 0), (AY, 0, 1, 4), (AI, 0, 3, 0), (AY, 0, 3, 0), (AI, 3, 0, 1),
    (AY, 0, 0, 6), (AI, 2, 0, 0), (AY, 0, 3, 4), (AI, 1, 1, 0), (AY, 0, 0, 2), (AI, 1, 1, 1),
    (AY, 1, 0, 6), (AY, 0, 0, 4), (AY, 1, 3, 6), (AY, 0, 2, 6), (AY, 3, 2, 2), (AY, 1, 2, 6),
    (AY, 0, 3, 6), (AY, 3, 2, 4),
)
MID = (
    (E, 3, 0, 5), (SY, 3, 0, 4), (E, 3, 0, 7), (SY, 3, 0, 6), (E, 3, 0, 3), (E, 3, 0, 1),
    (E, 2, 0, 5), (E, 2, 0, 3), (E, 3, 3, 7), (E, 2, 0, 1), (E, 2, 0, 7), (SY, 2, 0, 4),
    (E, 3, 3, 5), (E, 3, 3, 3), (E, 3, 3, 1), (E, 1, 3, 7), (E, 1, 0, 5), (E, 1, 3, 5),
    (E, 1, 3, 1), (SY, 3, 3, 6), (E, 1, 3, 3), (E, 0, 3, 1), (E, 1, 2, 3), (E, 1, 2, 7),
    (E, 1, 2, 5), (E, 1, 2, 1), (E, 1, 1, 7), (E, 1, 1, 1), (E, 1, 1, 5), (SY, 2, 0, 2),
    (G, 3, 2, 6), (SI, 3, 2, 6), (E, 1, 1, 3), (E, 1, 0, 3), (E, 0, 3, 5), (E, 1, 0, 1),
    (E, 0, 3, 7), (SY, 2, 0, 0), (G, 3, 2, 7), (SI, 3, 2, 7), (E, 0, 3, 3), (E, 1, 0, 7),
    (G, 3, 1, 7), (SI, 3, 1, 7), (SY, 2, 0, 6), (G, 0, 0, 7), (SI, 0, 0, 7), (SY, 3, 0, 2),
    (G, 3, 2, 0), (SO, 3, 2, 0), (G, 0, 1, 7), (SI, 0, 1, 7), (G, 3, 2, 1), (SY, 3, 3, 4),
    (SO, 3, 2, 1), (G, 3, 1, 6), (SI, 3, 1, 6), (G, 3, 1, 1), (SY, 3, 3, 2), (SO, 3, 1, 1),
    (G, 3, 0, 4), (SI, 3, 0, 4), (SY, 3, 3, 0), (G, 0, 0, 1), (SO, 0, 0, 1), (SY, 1, 2, 2),
    (G, 0, 2, 7), (SI, 0, 2, 7), (G, 0, 1, 1), (SY, 1, 0, 4), (SO, 0, 1, 1), (G, 0, 1, 6),
    (SI, 0, 1, 6), (G, 3, 1, 0), (SO, 3, 1, 0), (SY, 1, 1, 6), (G, 2, 0, 4), (SI, 2, 0, 4),
    (SY, 1, 3, 6), (N, 3, 0, 0), (V, 0, 0, 0), (X, 3, 0, 0), (G, 0, 2, 1), (SO, 0, 2, 1),
    (SY, 1, 3, 4), (G, 0, 0, 6), (SI, 0, 0, 6), (G, 0, 1, 0), (SO, 0, 1, 0), (SY, 1, 2, 6),
    (G, 2, 0, 6), (SI, 2, 0, 6), (G, 3, 3, 6), (SI, 3, 3, 6), (U, 3, 0, 0), (SY, 1, 1, 0),
    (AO, 3, 0, 2), (AI, 3, 0, 2), (N, 2, 0, 0), (X, 2, 0, 0), (SY, 1, 2, 4), (G, 0, 0, 0),
    (SO, 0, 0, 0), (G, 3, 3, 4), (SI, 3, 3, 4), (SY, 1, 1, 4), (G, 2, 0, 0), (SO, 2, 0, 0),
    (G, 1, 0, 4), (SI, 1, 0, 4), (G, 3, 3, 0), (SY, 1, 2, 0), (SO, 3, 3, 0), (U, 2, 0, 0),
    (AI, 2, 0, 2), (AO, 3, 0, 4), (AY, 2, 0, 2), (AO, 2, 0, 2), (G, 1, 2, 6), (SI, 1, 2, 6),
    (N, 3, 3, 0), (X, 3, 3, 0), (SY, 1, 1, 2), (G, 1, 1, 6), (SI, 1, 1, 6), (AY, 3, 0, 2),
    (G, 1, 3, 6), (SI, 1, 3, 6), (AO, 2, 0, 4), (SY, 1, 3, 0), (AI, 3, 1, 0), (U, 3, 3, 0),
    (AO, 3, 3, 2), (SY, 1, 3, 2), (G, 1, 2, 0), (AO, 2, 0, 3), (AI, 3, 3, 2), (G, 1, 3, 4),
    (AI, 2, 0, 3), (SO, 1, 2, 0), (AY, 3, 3, 2), (G, 1, 1, 0), (G, 1, 1, 4), (SI, 1, 3, 4),
    (SO, 1, 1, 0), (SY, 0, 3, 0), (G, 1, 2, 4), (SI, 1, 2, 4), (SY, 1, 0, 2), (AO, 3, 0, 3),
    (G, 1, 3, 0), (G, 0, 2, 5), (SI, 1, 1, 4), (SY, 3, 0, 0), (SO, 1, 3, 0), (AI, 3, 0, 3),
    (AO, 3, 3, 4), (AY, 3, 1, 0), (G, 3, 0, 6), (AY, 3, 1, 6), (N, 1, 3, 0), (AO, 2, 0, 5),
    (AI, 3, 3, 3), (SY, 0, 3, 4), (SI, 3, 0, 6), (AO, 3, 1, 6), (SY, 1, 0, 0), (N, 1, 0, 0),
    (SI, 0, 2, 5), (AO, 3, 3, 3), (N, 1, 1, 0), (SY, 0, 3, 6), (N, 1, 2, 0), (X, 1, 0, 0),
    (AO, 3, 0, 5), (G, 3, 1, 4), (SI, 3, 1, 4), (SY, 0, 3, 2), (AO, 3, 3, 5), (G, 3, 1, 5),
    (SI, 3, 1, 5), (G, 3, 0, 0), (SO, 3, 0, 0), (SY, 1, 0, 6), (AI, 3, 2, 0), (U, 1, 0, 0),
    (AO, 1, 0, 2), (AI, 1, 0, 2), (AY, 3, 2, 0), (U, 1, 3, 0), (AO, 1, 3, 2), (AI, 1, 3, 2),
    (U, 1, 2, 0), (G, 0, 2, 4), (U, 1, 1, 0), (AY, 1, 0, 2), (AO, 1, 2, 2), (SI, 0, 2, 4),
    (G, 0, 1, 5), (AY, 1, 3, 2), (AO, 1, 1, 2), (AI, 1, 1, 2), (G, 0, 2, 3), (SY, 0, 2, 2),
    (AO, 3, 2, 6), (AI, 1, 2, 2), (AY, 1, 1, 2), (AO, 1, 0, 4), (SI, 0, 1, 5), (AY, 3, 2, 6),
    (AO, 1, 3, 4), (AI, 0, 1, 0), (G, 1, 0, 6), (AY, 0, 1, 0), (AO, 1, 1, 4), (SI, 1, 0, 6),
    (AY, 1, 0, 4), (N, 0, 2, 0), (X, 0, 2, 0), (G, 3, 1, 3), (AO, 1, 2, 4), (SY, 3, 1, 2),
    (AI, 1, 1, 3), (AO, 1, 1, 3), (V, 0, 0, 1), (G, 0, 1, 3), (AY, 1, 2, 2), (G, 0, 1, 4),
    (SI, 0, 1, 4), (AO, 0, 1, 6), (SY, 0, 1, 2), (U, 0, 2, 0), (AI, 0, 2, 2), (G, 0, 0, 5),
    (AO, 0, 2, 2), (G, 1, 0, 0), (AY, 1, 3, 4), (SI, 0, 0, 5), (SO, 1, 0, 0), (AI, 3, 3, 1),
    (N, 3, 1, 0), (AY, 0, 1, 6), (X, 3, 1, 0), (AO, 1, 1, 5), (AY, 0, 2, 2), (G, 0, 3, 4),
    (SI, 0, 3, 4), (AO, 0, 2, 4), (N, 0, 1, 0), (X, 0, 1, 0), (AY, 1, 2, 4), (G, 0, 2, 6),
    (SI, 0, 2, 6), (U, 3, 1, 0), (AO, 3, 1, 2), (AI, 3, 1, 2), (AY, 0, 2, 4), (G, 0, 3, 6),
    (AO, 3, 3, 7), (SI, 0, 3, 6), (AY, 3, 1, 2), (G, 0, 0, 4), (SI, 0, 0, 4), (U, 0, 1, 0),
    (AO, 0, 1, 2), (AY, 0, 1, 2), (N, 0, 3, 0), (X, 0, 3, 0), (AI, 0, 1, 2), (G, 0, 2, 0),
    (SO, 0, 2, 0), (AY, 0, 0, 0), (AO, 3, 1, 4), (AI, 0, 0, 0), (AY, 3, 1, 4), (G, 0, 0, 3),
    (G, 0, 3, 0), (SO, 0, 3, 0), (SY, 0, 0, 2), (AI, 3, 3, 0), (U, 0, 3, 0), (AO, 0, 3, 2),
    (AI, 0, 3, 2), (AY, 0, 3, 2), (AI, 2, 0, 1), (AO, 0, 1, 4), (AY, 0, 1, 4), (AO, 0, 0, 6),
    (AY, 0, 0, 6), (G, 3, 2, 5), (SI, 3, 2, 5), (AO, 3, 3, 6), (N, 0, 0, 0), (X, 0, 0, 0),
    (AI, 3, 0, 0), (AY, 0, 3, 4), (AO, 0, 3, 4), (AI, 1, 0, 0), (AY, 1, 0, 0), (AO, 2, 0, 7),
    (G, 3, 2, 4), (SI, 3, 2, 4), (G, 3, 2, 3), (V, 0, 0, 2), (SY, 3, 2, 2), (U, 0, 0, 0),
    (AI, 0, 0, 2), (AO, 0, 0, 2), (AY, 0, 0, 2), (AO, 3, 0, 6), (AI, 1, 3, 0), (AY, 1, 3, 0),
    (AO, 1, 0, 6), (AI, 0, 2, 0), (AY, 1, 0, 6), (N, 3, 2, 0), (X, 3, 2, 0), (AY, 0, 2, 0),
    (AO, 0, 0, 4), (AI, 1, 2, 0), (AY, 0, 0, 4), (AO, 1, 3, 6), (AI, 0, 3, 0), (AY, 0, 3, 0),
    (AO, 0, 2, 6), (AI, 3, 0, 1), (U, 3, 2, 0), (AO, 3, 2, 2), (AI, 3, 2, 2), (AY, 1, 2, 0),
    (AI, 2, 0, 0), (AO, 1, 2, 6), (AY, 1, 3, 6), (AI, 1, 1, 0), (AO, 0, 3, 6), (AY, 3, 2, 2),
    (AI, 1, 1, 1), (AO, 3, 0, 7), (AY, 0, 3, 6), (AO, 3, 2, 4), (AY, 0, 2, 6), (AO, 2, 0, 6),
    (AY, 3, 2, 4), (AO, 1, 1, 6), (AY, 1, 2, 6), (AO, 1, 1, 7),
)


def lanes_of(shapes, g, ref, i):
    n = len(GROUPS[g].members)
    w = shapes[g][1] // n
    return ref if n == 1 else ref.at[..., i * w : (i + 1) * w]


def finish(shapes, *refs):
    n = len(GROUPS)
    full, own, st = refs[0:n], refs[n : 2 * n], refs[2 * n : 3 * n]
    vectors = refs[3 * n : 3 * n + 6]
    halves, nexts, news = (refs[3 * n + 6 + 8 * k : 3 * n + 14 + 8 * k] for k in range(3))
    sem, vec_sem = refs[3 * n + 30 :]
    for g, group in enumerate(GROUPS):
        w = shapes[g][1]
        for i, a in enumerate(group.members):
            if group.rows:
                pltpu.make_async_copy(lanes_of(shapes, g, full[g], i), halves[a], sem.at[0, g]).start()
            else:
                for b in range(8):
                    dst = halves[a].at[:, b * w : (b + 1) * w]
                    pltpu.make_async_copy(full[g].at[b], dst, sem.at[0, g]).start()
            pltpu.make_async_copy(lanes_of(shapes, g, own[g], i), nexts[a], sem.at[1, g]).start()
            pltpu.make_async_copy(lanes_of(shapes, g, st[g], i), news[a], sem.at[2, g]).start()
    copies = []
    for i, dst in enumerate((*halves[6:], *nexts[6:], *news[6:])):
        copies.append(pltpu.make_async_copy(vectors[i], dst, vec_sem.at[i]))
        copies[-1].start()
    for g in range(n):
        for k, ref in enumerate((full[g], own[g], st[g])):
            pltpu.make_async_copy(ref, ref, sem.at[k, g]).wait()
    for c in copies:
        c.wait()


def kernel(replicas, models, limit, shapes, *refs):
    slopes, slope_norm, slope_bias = refs[0:6], refs[6], refs[7]
    params, param_norm, param_bias = refs[8:14], refs[14], refs[15]
    states, state_norm, state_bias = refs[16:22], refs[22], refs[23]
    groups = range(len(GROUPS))
    n = len(GROUPS)
    full, own, st = refs[24 : 24 + n], refs[24 + n : 24 + 2 * n], refs[24 + 2 * n : 24 + 3 * n]
    half_norm, half_bias, next_norm, next_bias, new_norm, new_bias = refs[24 + 3 * n : 30 + 3 * n]
    scratch = list(refs[30 + 3 * n :])
    take = lambda: [scratch.pop(0) for _ in groups]
    xin, enc, rec, sq, sqr = (take() for _ in range(5))
    vs, vown, vrec, vnext, vag, vh_norm, vh_bias = (scratch.pop(0) for _ in range(7))
    rs_s, rs_r, ag_s, ag_r, n_s, n_r, v_s, v_r, w_s, w_r = (scratch.pop(0) for _ in range(10))
    load_sem, own_sem, st_sem, vown_sem = scratch

    r = lax.axis_index("replica")
    m = lax.axis_index("model")
    y, z = lax.rem(r, 2), r // 2
    side = z // 2
    slab = [(p + side * (3 - 2 * p)) * 2 + (y if d == 0 else 1 - y) for p in range(4) for d in (0, 1)]

    scale = 2.0**13 / (limit * replicas)
    rate = replicas ** (-0.5)

    def encode(x):
        t = x * scale
        t2 = t * t
        t4 = t2 * t2
        return (t4 * t4 * t).astype(jnp.bfloat16)

    def decode(c):
        f = c.astype(jnp.float32)
        a = jnp.exp(jnp.log(jnp.abs(f)) * (1.0 / root)) * (1.0 / scale)
        return jnp.where(f < 0, -a, a)

    lanes = functools.partial(lanes_of, shapes)
    at = {k: i for i, k in enumerate(CHUNKS)}
    unit = lambda g: shapes[g][0] // sum(SIZES[g])
    height = lambda g, c: unit(g) * SIZES[g][c]
    rows = lambda g, c: pl.ds(unit(g) * sum(SIZES[g][:c]), height(g, c))

    def source(g, c, s):
        w = shapes[g][1]
        if GROUPS[g].rows:
            return xin[g].at[slab[s], rows(g, c)]
        return xin[g].at[rows(g, c), pl.ds(pl.multiple_of(slab[s] * w, w), w)]

    def loop(g, c, body):
        h, w = height(g, c), shapes[g][1]
        step = min(h, max(16, STEP // w // 16 * 16))
        while h % step:
            step -= 16
        lax.fori_loop(0, h // step, lambda i, c: (body(pl.ds(pl.multiple_of(i * step, step), step)), c)[1], 0)

    def remote(src, dst, s, d, peer, axis="replica"):
        return pltpu.make_async_remote_copy(
            src_ref=src, dst_ref=dst, send_sem=s, recv_sem=d, device_id={axis: peer}, device_id_type=MESH
        )

    def whole(ref, sem):
        pltpu.make_async_copy(ref, ref, sem).wait()

    barrier = pltpu.get_barrier_semaphore()

    def greet(axis, to):
        pl.semaphore_signal(barrier, inc=1, device_id={axis: to}, device_id_type=MESH)

    @pl.when(z > 0)
    def _():
        greet("replica", r - 2)

    @pl.when(z < 3)
    def _():
        greet("replica", r + 2)

    greet("replica", z * 2 + (1 - y))
    for j in range(1, models):
        greet("model", lax.rem(m + j, models))

    def chunk_of(g, c):
        return xin[g].at[:, rows(g, c)] if GROUPS[g].rows else xin[g].at[rows(g, c)]

    def load(g, c):
        for i, a in enumerate(GROUPS[g].members):
            src = slopes[a].at[:, rows(g, c)] if GROUPS[g].rows else slopes[a].at[rows(g, c)]
            pltpu.make_async_copy(src, lanes(g, chunk_of(g, c), i), load_sem.at[at[g, c]]).start()

    def load_own():
        for g in OWN:
            for i, a in enumerate(GROUPS[g].members):
                pltpu.make_async_copy(params[a], lanes(g, own[g], i), own_sem.at[g]).start()
                pltpu.make_async_copy(states[a], lanes(g, st[g], i), st_sem.at[g]).start()

    for g, c in CHUNKS[:2]:
        load(g, c)
    vs[0:1, :] = slope_norm[...]
    vs[1:2, :] = slope_bias[...]
    for g in groups:
        if not GROUPS[g].rows:
            sq[g][...] = jnp.zeros_like(sq[g])

    def rule(p, s, v):
        s = hold_rate * s + (1.0 - hold_rate) * v * v
        return p - learn_rate * v * lax.rsqrt(s + 1e-06), s

    def fold(x):
        total = x[:, 0:128]
        for k in range(128, x.shape[1], 128):
            total = total + x[:, k : k + 128]
        return jnp.sum(total, axis=1, keepdims=True)

    width = vs.shape[1] // replicas

    def vec_out(j):
        to = lax.rem(r + j, replicas)
        return remote(
            vs.at[:, pl.ds(pl.multiple_of(to * width, width), width)],
            vrec.at[j - 1], v_s.at[j - 1], v_r.at[j - 1], to,
        )

    def vec_back(j):
        return remote(vnext, vag.at[j - 1], w_s.at[j - 1], w_r.at[j - 1], lax.rem(r + j, replicas))

    def vec_start():
        pltpu.make_async_copy(vs.at[:, pl.ds(pl.multiple_of(r * width, width), width)], vown, vown_sem).start()
        for j in range(1, replicas):
            vec_out(j).start()

    def vec_update():
        pltpu.make_async_copy(vown, vown, vown_sem).wait()
        total = vown[...]
        for j in range(1, replicas):
            vec_out(j).wait_recv()
            total = total + vrec[j - 1]
        v = total * rate
        p, s = rule(param_norm[...], state_norm[...], v[0:1, :])
        next_norm[...] = p
        new_norm[...] = s
        vnext[0:1, :] = p
        p, s = rule(param_bias[...], state_bias[...], v[1:2, :])
        next_bias[...] = p
        new_bias[...] = s
        vnext[1:2, :] = p
        for j in range(1, replicas):
            vec_back(j).start()

    def vec_finish():
        vh_norm[pl.ds(r, 1), :] = vnext[0:1, :]
        vh_bias[pl.ds(r, 1), :] = vnext[1:2, :]
        for j in range(1, replicas):
            vec_back(j).wait_recv()
            at = lax.rem(r + replicas - j, replicas)
            vh_norm[pl.ds(at, 1), :] = vag[j - 1, 0:1, :]
            vh_bias[pl.ds(at, 1), :] = vag[j - 1, 1:2, :]
        half_norm[...] = vh_norm[...].astype(jnp.bfloat16)
        half_bias[...] = vh_bias[...].astype(jnp.bfloat16)

    def run(mid, order):
        mine = 1 if mid else 0
        peers = {}
        if mid:
            peers[SO] = peers[AO] = side * 6 + y
            peers[SI] = peers[AI] = (3 - z) * 2 + y
        else:
            peers[SI] = peers[AI] = (1 + side) * 2 + y
        peers[SY] = peers[AY] = z * 2 + (1 - y)
        done = set()
        ahead = list(CHUNKS[2:])

        def kind(g, c):
            return SUMS[g][c]

        def landing(g, c, by, s):
            if kind(g, c) == A:
                return (0, 7, 3)[by] + s // 2
            return (10, 6 + s, s - 2)[by]

        def outgoing(g, c, op, s):
            p = s // 2
            if kind(g, c) == A:
                if op == SY:
                    return p
                return 3 + p if p else 4
            if op == SY:
                return 6
            if not mid:
                return s - 2
            return s - 4 if p >= 2 else 4 + s

        def across(op, s):
            return (3 - s // 2) * 2 + s % 2 if mid and op in (SI, AI) else s

        def send(op, g, c, s):
            by = {SY: 0, SO: 1, SI: 1 if mid else 2}[op]
            slot = landing(g, c, by, across(op, s))
            return remote(
                enc[g].at[outgoing(g, c, op, s), rows(g, c)],
                rec[g].at[slot, rows(g, c)],
                rs_s.at[g],
                rs_r.at[at[g, c], slot],
                peers[op],
            )

        def gather(op, g, c, s):
            to = s + 1 if op == AY else across(op, s)
            ref = full[g].at[slab[s], rows(g, c)]
            link = {AY: 0, AI: 1, AO: 2}[op]
            return remote(ref, ref, ag_s.at[at[g, c], link], ag_r.at[at[g, c], to], peers[op])

        def got(g, c, s):
            if s != mine * 2 and (g, c, s) not in done:
                done.add((g, c, s))
                ref = full[g].at[slab[s], rows(g, c)]
                whole(ref, ag_r.at[at[g, c], s])

        def arrived(g, c, by, s):
            slot = landing(g, c, by, s)
            ref = rec[g].at[slot, rows(g, c)]
            whole(ref, rs_r.at[at[g, c], slot])
            return ref

        def once(key, ref, sem):
            if key not in done:
                done.add(key)
                whole(ref, sem)

        def loaded(g, c):
            while (g, c) in ahead:
                load(*ahead.pop(0))
                if not ahead:
                    load_own()
            once((-1, g, c), chunk_of(g, c), load_sem.at[at[g, c]])

        def parts(g, c, s):
            loaded(g, c)
            by = []
            a, p = kind(g, c) == A, s // 2
            if a or s == mine * 2:
                by.append(0)
            if mid and p >= 1:
                by.append(2)
            if p == mine or (mid and p == 0):
                by.append(1)
            return [arrived(g, c, b, s) for b in by]

        def encode_op(g, c, s, op):
            loaded(g, c)
            src, dst = source(g, c, s), enc[g].at[outgoing(g, c, op, s), rows(g, c)]

            def body(d):
                dst[d, :] = encode(src[d, :])

            loop(g, c, body)

        def add_op(g, c, s):
            src = source(g, c, s)
            op = SY if s // 2 == mine else SO if mid and s < 2 else SI
            dst = enc[g].at[outgoing(g, c, op, s), rows(g, c)]
            got = parts(g, c, s)

            def body(d):
                total = src[d, :]
                for ref in got:
                    total = total + decode(ref[d, :])
                dst[d, :] = encode(total)

            loop(g, c, body)

        def mean_op(g, c):
            acc = source(g, c, mine * 2)
            got = parts(g, c, mine * 2)
            once((-2, g), own[g], own_sem.at[g])
            held = own[g].at[rows(g, c)]
            k = len(GROUPS[g].members)
            w = shapes[g][1] // k

            def mean(d):
                total = acc[d, :]
                for ref in got:
                    total = total + decode(ref[d, :])
                v = total * rate
                acc[d, :] = v
                return v

            if GROUPS[g].rows:
                sums = sq[g].at[rows(g, c)]

                def body(d):
                    v, p = mean(d), held[d, :]
                    v, p = v * v, p * p
                    lane = lax.broadcasted_iota(jnp.int32, (v.shape[0], 128), 1)
                    out = jnp.zeros((v.shape[0], 128), jnp.float32)
                    for i in range(k):
                        cols = slice(i * w, (i + 1) * w)
                        out = jnp.where(lane == 2 * i, fold(p[:, cols]), out)
                        out = jnp.where(lane == 2 * i + 1, fold(v[:, cols]), out)
                    sums[d, :] = out

            else:

                def body(d):
                    v, p = mean(d), held[d, :]
                    sq[g][0] += jnp.sum((p * p).reshape(-1, 8, w), axis=0)
                    sq[g][1] += jnp.sum((v * v).reshape(-1, 8, w), axis=0)

            loop(g, c, body)

        def norms(g, c, j):
            if GROUPS[g].rows:
                src, dst = sq[g].at[rows(g, c)], sqr[g].at[j - 1, rows(g, c)]
            else:
                src, dst = sq[g], sqr[g].at[j - 1]
            return remote(src, dst, n_s.at[at[g, c], j - 1], n_r.at[at[g, c], j - 1], lax.rem(m + j, models), "model")

        def update_op(g, c):
            first = c if GROUPS[g].rows else 0
            for j in range(1, models):
                if (-4, g, first, j) not in done:
                    done.add((-4, g, first, j))
                    norms(g, first, j).wait_recv()
            once((-3, g), st[g], st_sem.at[g])
            acc, half = source(g, c, mine * 2), full[g].at[slab[mine * 2], rows(g, c)]
            held, hold = own[g].at[rows(g, c)], st[g].at[rows(g, c)]
            k = len(GROUPS[g].members)
            w = shapes[g][1] // k

            def put(d, cols, t):
                p, s = rule(held[d, cols], hold[d, cols], acc[d, cols] * t)
                held[d, cols] = p
                hold[d, cols] = s
                half[d, cols] = p.astype(jnp.bfloat16)

            if GROUPS[g].rows:
                sums = [sq[g].at[rows(g, c)]] + [sqr[g].at[j, rows(g, c)] for j in range(models - 1)]

                def body(d):
                    total = sums[0][d, :]
                    for ref in sums[1:]:
                        total = total + ref[d, :]
                    lane = lax.broadcasted_iota(jnp.int32, total.shape, 1)
                    pick = lambda i: jnp.sum(jnp.where(lane == i, total, 0.0), axis=1, keepdims=True)
                    for i in range(k):
                        t = jnp.sqrt(pick(2 * i)) * lax.rsqrt(pick(2 * i + 1) + 1e-06)
                        put(d, slice(i * w, (i + 1) * w), t)

            else:
                total = sq[g][...]
                for j in range(models - 1):
                    total = total + sqr[g][j]
                total = jnp.sum(total, axis=1, keepdims=True)
                t = jnp.sqrt(total[0]) * lax.rsqrt(total[1] + 1e-06)

                def body(d):
                    put(d, slice(None), t)

            loop(g, c, body)

        met = False
        for i, (op, g, c, s) in enumerate(order):
            if ahead and i % 2:
                load(*ahead.pop(0))
                if not ahead:
                    load_own()
            if op not in (E, G) and not met:
                met = True
                pl.semaphore_wait(barrier, models + (2 if mid else 1))
            if op == E:
                encode_op(g, c, s, SY if kind(g, c) == A else SI)
            elif op == G:
                add_op(g, c, s)
            elif op in (SY, SI, SO):
                send(op, g, c, s).start()
            elif op == N:
                mean_op(g, c)
            elif op == X:
                for j in range(1, models):
                    norms(g, c, j).start()
            elif op == U:
                update_op(g, c)
            elif op == V:
                (vec_start, vec_update, vec_finish)[s]()
            else:
                got(g, c, s)
                gather(op, g, c, s).start()

        for g, c in CHUNKS:
            for s in range(8):
                got(g, c, s)
        for g in groups:
            whole(enc[g], rs_s.at[g])
        for g, c in CHUNKS:
            for link, count in enumerate(SENT[mid][BACK[g][c]]):
                if count:
                    whole(full[g].at[pl.ds(0, count), rows(g, c)], ag_s.at[at[g, c], link])
            if GROUPS[g].rows or c == 0:
                for j in range(1, models):
                    norms(g, c, j).wait_send()
        for j in range(1, replicas):
            vec_out(j).wait_send()
            vec_back(j).wait_send()

    end = jnp.logical_or(z == 0, z == 3)

    @pl.when(end)
    def _():
        run(False, END)

    @pl.when(jnp.logical_not(end))
    def _():
        run(True, MID)


def fused(replicas, models, shapes, *args):
    slopes, params = args[0:6], args[8:14]
    f32, bf16 = jnp.float32, jnp.bfloat16
    vec = args[6].shape[1]
    width = vec // replicas
    row = lambda a: a.reshape(1, -1)
    by_rows = [a in g.members and g.rows for a in range(6) for g in GROUPS if a in g.members]
    cut = lambda a, rows: a.reshape(replicas, -1, a.shape[-1]) if rows else a[0]
    args = (
        *(cut(a, rows) for a, rows in zip(slopes, by_rows)), *args[6:14],
        row(args[14]), row(args[15]), *args[16:22], row(args[22]), row(args[23]),
    )
    S = jax.ShapeDtypeStruct
    n, chunks = len(GROUPS), len(CHUNKS)
    held = [((replicas, *s), bf16) for s in shapes] + [(s, f32) for s in shapes] * 2
    held += [((replicas, width), bf16)] * 2 + [((1, width), f32)] * 4
    ANY, VM = pl.BlockSpec(memory_space=pl.ANY), pl.BlockSpec(memory_space=pltpu.VMEM)
    part = [ANY] * 6 + [VM] * 2
    scratch = [
        pltpu.VMEM((replicas, *s) if g.rows else (s[0], s[1] * replicas), f32) for g, s in zip(GROUPS, shapes)
    ]
    scratch += [pltpu.VMEM((7, *s), bf16) for s in shapes]
    scratch += [pltpu.VMEM((11 if B in k else 9, *s), bf16) for k, s in zip(SUMS, shapes)]
    sq = [(s[0], 128) if g.rows else (2, 8, s[1]) for g, s in zip(GROUPS, shapes)]
    scratch += [pltpu.VMEM(s, f32) for s in sq]
    scratch += [pltpu.VMEM((models - 1, *s), f32) for s in sq]
    scratch += [
        pltpu.VMEM((2, vec), f32),
        pltpu.VMEM((2, width), f32),
        pltpu.VMEM((replicas - 1, 2, width), f32),
        pltpu.VMEM((2, width), f32),
        pltpu.VMEM((replicas - 1, 2, width), f32),
        pltpu.VMEM((replicas, width), f32),
        pltpu.VMEM((replicas, width), f32),
    ]
    dma = pltpu.SemaphoreType.DMA
    scratch += [dma((n,)), dma((chunks, 11)), dma((chunks, 3)), dma((chunks, 8))]
    scratch += [dma((chunks, models - 1))] * 2 + [dma((replicas - 1,))] * 4
    scratch += [dma((chunks,))] + [dma((n,))] * 2 + [dma(())]
    out = pl.pallas_call(
        functools.partial(kernel, replicas, models, 4.0, shapes),
        out_shape=[pltpu.VMEM(*h) for h in held],
        in_specs=part * 3,
        out_specs=[VM] * len(held),
        scratch_shapes=scratch,
        compiler_params=pltpu.CompilerParams(
            collective_id=0, has_side_effects=True, vmem_limit_bytes=54 * 1024 * 1024
        ),
    )(*args)
    outs = [
        S((replicas, a.shape[1] // replicas, a.shape[2]) if rows else a.shape[1:], bf16)
        for a, rows in zip(slopes, by_rows)
    ]
    outs += [S((replicas, width), bf16)] * 2
    for _ in range(2):
        outs += [S(a.shape, f32) for a in params] + [S((1, width), f32)] * 2
    out = pl.pallas_call(
        functools.partial(finish, shapes),
        out_shape=outs,
        in_specs=[VM] * len(held),
        out_specs=[ANY] * len(outs),
        scratch_shapes=[dma((3, n)), dma((6,))],
        compiler_params=pltpu.CompilerParams(vmem_limit_bytes=1024 * 1024),
    )(*out)
    flat = lambda a: a.reshape(-1)
    return (
        *(a.reshape(-1, a.shape[-1]) for a in out[0:6]), flat(out[6]), flat(out[7]),
        *out[8:14], flat(out[14]), flat(out[15]),
        *out[16:22], flat(out[22]), flat(out[23]),
    )


def plain(
    slope_up,
    slope_down,
    slope_query,
    slope_key,
    slope_value,
    slope_mixed,
    slope_norm,
    slope_bias,
    param_up,
    param_down,
    param_query,
    param_key,
    param_value,
    param_mixed,
    param_norm,
    param_bias,
    state_up,
    state_down,
    state_query,
    state_key,
    state_value,
    state_mixed,
    state_norm,
    state_bias,
):
    mean_up, mean_down, mean_query, mean_key, mean_value, mean_mixed = (
        lax.psum_scatter(slope_up[0], "replica", scatter_dimension=0, tiled=True),
        lax.psum_scatter(slope_down[0], "replica", scatter_dimension=1, tiled=True),
        lax.psum_scatter(slope_query[0], "replica", scatter_dimension=0, tiled=True),
        lax.psum_scatter(slope_key[0], "replica", scatter_dimension=0, tiled=True),
        lax.psum_scatter(slope_value[0], "replica", scatter_dimension=0, tiled=True),
        lax.psum_scatter(slope_mixed[0], "replica", scatter_dimension=1, tiled=True),
    )
    whole_norm, whole_bias = lax.psum((slope_norm[0], slope_bias[0]), "replica")
    place = lax.axis_index("replica")
    mean_norm = lax.dynamic_slice_in_dim(
        whole_norm, place * param_norm.shape[0], param_norm.shape[0]
    )
    mean_bias = lax.dynamic_slice_in_dim(
        whole_bias, place * param_bias.shape[0], param_bias.shape[0]
    )
    mean_rate = lax.axis_size("replica") ** (-0.5)
    mean_up = mean_up * mean_rate
    mean_down = mean_down * mean_rate
    mean_query = mean_query * mean_rate
    mean_key = mean_key * mean_rate
    mean_value = mean_value * mean_rate
    mean_mixed = mean_mixed * mean_rate
    mean_norm = mean_norm * mean_rate
    mean_bias = mean_bias * mean_rate
    (
        own_up,
        own_down,
        own_query,
        own_key,
        own_value,
        own_mixed,
        slope_up_norm,
        slope_down_norm,
        slope_query_norm,
        slope_key_norm,
        slope_value_norm,
        slope_mixed_norm,
    ) = lax.psum(
        (
            jnp.sum(param_up * param_up, axis=1, keepdims=True),
            jnp.sum(param_down * param_down, axis=0, keepdims=True),
            jnp.sum(param_query * param_query, axis=1, keepdims=True),
            jnp.sum(param_key * param_key, axis=1, keepdims=True),
            jnp.sum(param_value * param_value, axis=1, keepdims=True),
            jnp.sum(param_mixed * param_mixed, axis=0, keepdims=True),
            jnp.sum(mean_up * mean_up, axis=1, keepdims=True),
            jnp.sum(mean_down * mean_down, axis=0, keepdims=True),
            jnp.sum(mean_query * mean_query, axis=1, keepdims=True),
            jnp.sum(mean_key * mean_key, axis=1, keepdims=True),
            jnp.sum(mean_value * mean_value, axis=1, keepdims=True),
            jnp.sum(mean_mixed * mean_mixed, axis=0, keepdims=True),
        ),
        "model",
    )
    mean_up = mean_up * (jnp.sqrt(own_up) * lax.rsqrt(slope_up_norm + 1e-06))
    mean_down = mean_down * (jnp.sqrt(own_down) * lax.rsqrt(slope_down_norm + 1e-06))
    mean_query = mean_query * (jnp.sqrt(own_query) * lax.rsqrt(slope_query_norm + 1e-06))
    mean_key = mean_key * (jnp.sqrt(own_key) * lax.rsqrt(slope_key_norm + 1e-06))
    mean_value = mean_value * (jnp.sqrt(own_value) * lax.rsqrt(slope_value_norm + 1e-06))
    mean_mixed = mean_mixed * (jnp.sqrt(own_mixed) * lax.rsqrt(slope_mixed_norm + 1e-06))
    state_new_up = hold_rate * state_up + (1.0 - hold_rate) * mean_up * mean_up
    next_up = param_up - learn_rate * mean_up * lax.rsqrt(state_new_up + 1e-06)
    state_new_down = hold_rate * state_down + (1.0 - hold_rate) * mean_down * mean_down
    next_down = param_down - learn_rate * mean_down * lax.rsqrt(state_new_down + 1e-06)
    state_new_query = hold_rate * state_query + (1.0 - hold_rate) * mean_query * mean_query
    next_query = param_query - learn_rate * mean_query * lax.rsqrt(state_new_query + 1e-06)
    state_new_key = hold_rate * state_key + (1.0 - hold_rate) * mean_key * mean_key
    next_key = param_key - learn_rate * mean_key * lax.rsqrt(state_new_key + 1e-06)
    state_new_value = hold_rate * state_value + (1.0 - hold_rate) * mean_value * mean_value
    next_value = param_value - learn_rate * mean_value * lax.rsqrt(state_new_value + 1e-06)
    state_new_mixed = hold_rate * state_mixed + (1.0 - hold_rate) * mean_mixed * mean_mixed
    next_mixed = param_mixed - learn_rate * mean_mixed * lax.rsqrt(state_new_mixed + 1e-06)
    state_new_norm = hold_rate * state_norm + (1.0 - hold_rate) * mean_norm * mean_norm
    next_norm = param_norm - learn_rate * mean_norm * lax.rsqrt(state_new_norm + 1e-06)
    state_new_bias = hold_rate * state_bias + (1.0 - hold_rate) * mean_bias * mean_bias
    next_bias = param_bias - learn_rate * mean_bias * lax.rsqrt(state_new_bias + 1e-06)
    half_up, half_down, half_query, half_key, half_value, half_mixed, half_norm, half_bias = (
        lax.all_gather(next_up.astype(jnp.bfloat16), "replica", axis=0, tiled=True),
        lax.all_gather(next_down.astype(jnp.bfloat16), "replica", axis=1, tiled=True),
        lax.all_gather(next_query.astype(jnp.bfloat16), "replica", axis=0, tiled=True),
        lax.all_gather(next_key.astype(jnp.bfloat16), "replica", axis=0, tiled=True),
        lax.all_gather(next_value.astype(jnp.bfloat16), "replica", axis=0, tiled=True),
        lax.all_gather(next_mixed.astype(jnp.bfloat16), "replica", axis=1, tiled=True),
        lax.all_gather(next_norm.astype(jnp.bfloat16), "replica", axis=0, tiled=True),
        lax.all_gather(next_bias.astype(jnp.bfloat16), "replica", axis=0, tiled=True),
    )
    return (
        half_up,
        half_down,
        half_query,
        half_key,
        half_value,
        half_mixed,
        half_norm,
        half_bias,
        next_up,
        next_down,
        next_query,
        next_key,
        next_value,
        next_mixed,
        next_norm,
        next_bias,
        state_new_up,
        state_new_down,
        state_new_query,
        state_new_key,
        state_new_value,
        state_new_mixed,
        state_new_norm,
        state_new_bias,
    )


def solution(mesh):
    replicas, models = mesh.shape["replica"], mesh.shape["model"]

    def local(*args):
        if replicas != 2**3 or any(a.shape[k] % 128 for a in args[8:14] for k in (0, 1)):
            return plain(*args)
        shapes = []
        for g, sizes in zip(GROUPS, SIZES):
            h, w = args[8 + g.members[0]].shape
            shapes.append((h, w * len(g.members)))
            if h % (16 * sum(sizes)) or (w != 128 and not g.rows):
                return plain(*args)
        if args[14].shape[0] % 128:
            return plain(*args)
        return fused(replicas, models, shapes, *args)

    placed = (
        P("replica", None, "model"),
        P("replica", "model", None),
        P("replica", None, "model"),
        P("replica", None, "model"),
        P("replica", None, "model"),
        P("replica", "model", None),
        P("replica", None),
        P("replica", None),
        P("replica", "model"),
        P("model", "replica"),
        P("replica", "model"),
        P("replica", "model"),
        P("replica", "model"),
        P("model", "replica"),
        P("replica"),
        P("replica"),
        P("replica", "model"),
        P("model", "replica"),
        P("replica", "model"),
        P("replica", "model"),
        P("replica", "model"),
        P("model", "replica"),
        P("replica"),
        P("replica"),
    )
    return jax.shard_map(
        local,
        mesh=mesh,
        in_specs=placed,
        out_specs=(
            P(None, "model"),
            P("model", None),
            P(None, "model"),
            P(None, "model"),
            P(None, "model"),
            P("model", None),
            P(),
            P(),
            P("replica", "model"),
            P("model", "replica"),
            P("replica", "model"),
            P("replica", "model"),
            P("replica", "model"),
            P("model", "replica"),
            P("replica"),
            P("replica"),
            P("replica", "model"),
            P("model", "replica"),
            P("replica", "model"),
            P("replica", "model"),
            P("replica", "model"),
            P("model", "replica"),
            P("replica"),
            P("replica"),
        ),
        check_vma=False,
    )
```

```python
import functools

import jax
import jax.numpy as jnp
from jax import lax
from jax.experimental import pallas as pl
from jax.experimental.pallas import tpu as pltpu
from jax.sharding import PartitionSpec as P

learn_rate = 0.025
hold_rate = 0.7
root = 9
MESH = pl.DeviceIdType.MESH


class Group:
    def __init__(self, members, rows):
        self.members = members
        self.rows = rows


GROUPS = (Group((0,), True), Group((1,), False), Group((5,), False), Group((2, 3, 4), True))
A, B = 0, 1
E, G, N, X, U, V, SY, SI, SO, AY, AI, AO = range(12)
SIZES = ((2, 2, 2, 2), (2, 2, 2, 2), (8,), (2, 2, 2, 2))
SUMS = ((B, B, B, A), (A, A, A, A), (A,), (A, B, B, A))
BACK = ((A, A, A, A), (A, B, A, A), (B,), (B, A, A, B))
CHUNKS = ((3, 2), (3, 0), (3, 1), (2, 0), (3, 3), (1, 3), (0, 0), (1, 0), (0, 3), (1, 2), (0, 1), (1, 1), (0, 2))
OWN = (3, 2, 0, 1)
SENT = (((4, 1, 0), (1, 2, 0)), ((4, 2, 3), (1, 4, 6)))
STEP = 16384
END = (
    (E, 3, 2, 6), (SI, 3, 2, 6), (E, 3, 2, 7), (SI, 3, 2, 7), (E, 3, 0, 3), (SY, 3, 0, 2),
    (E, 3, 0, 5), (SY, 3, 0, 4), (E, 3, 1, 7), (E, 3, 1, 6), (E, 2, 0, 5), (E, 2, 0, 3),
    (SI, 3, 1, 7), (E, 3, 3, 3), (E, 3, 3, 7), (SY, 2, 0, 4), (E, 2, 0, 7), (E, 3, 3, 1),
    (E, 0, 0, 7), (E, 2, 0, 1), (E, 3, 3, 5), (SI, 0, 0, 7), (E, 1, 0, 5), (E, 0, 0, 6),
    (SY, 3, 3, 2), (E, 1, 3, 7), (E, 0, 3, 7), (E, 1, 2, 7), (E, 1, 3, 5), (E, 0, 1, 7),
    (SI, 0, 1, 7), (E, 0, 1, 6), (E, 1, 1, 7), (E, 1, 1, 5), (E, 0, 2, 7), (SY, 2, 0, 2),
    (E, 1, 2, 5), (E, 3, 0, 7), (G, 3, 0, 2), (E, 1, 3, 3), (E, 1, 0, 3), (SI, 3, 1, 6),
    (E, 1, 1, 3), (E, 1, 2, 3), (SY, 3, 3, 6), (E, 0, 2, 5), (E, 1, 0, 7), (G, 3, 0, 4),
    (E, 0, 3, 1), (E, 0, 3, 3), (E, 3, 1, 4), (SI, 3, 0, 4), (E, 1, 3, 1), (E, 3, 1, 5),
    (SY, 2, 0, 6), (E, 0, 3, 5), (E, 0, 2, 4), (G, 2, 0, 4), (E, 3, 0, 1), (E, 0, 1, 5),
    (SI, 0, 2, 7), (E, 1, 1, 1), (E, 0, 2, 3), (SY, 3, 3, 0), (E, 0, 2, 2), (E, 3, 1, 2),
    (G, 3, 3, 2), (E, 1, 2, 1), (SI, 0, 1, 6), (E, 3, 1, 3), (E, 1, 0, 1), (E, 0, 1, 3),
    (E, 0, 1, 4), (E, 0, 0, 5), (SY, 2, 0, 0), (E, 0, 1, 2), (E, 0, 2, 6), (G, 2, 0, 2),
    (E, 0, 0, 4), (SI, 2, 0, 4), (E, 0, 0, 3), (E, 0, 0, 2), (SY, 3, 3, 4), (E, 3, 2, 5),
    (E, 3, 2, 4), (G, 3, 3, 6), (E, 3, 2, 3), (E, 3, 2, 2), (SI, 3, 0, 2), (SY, 1, 0, 4),
    (G, 2, 0, 6), (SY, 1, 2, 6), (SI, 0, 0, 6), (G, 3, 2, 1), (SI, 2, 0, 6), (SY, 1, 1, 6),
    (G, 3, 1, 1), (SI, 3, 3, 6), (G, 3, 3, 4), (SY, 3, 1, 0), (SI, 2, 0, 2), (G, 0, 0, 1),
    (G, 1, 0, 4), (SY, 1, 3, 6), (SI, 3, 3, 4), (SY, 1, 1, 4), (G, 0, 1, 1), (G, 1, 2, 6),
    (SI, 1, 0, 4), (SY, 0, 3, 6), (G, 1, 1, 6), (SI, 3, 3, 2), (N, 3, 1, 0), (V, 0, 0, 0),
    (SY, 1, 3, 4), (X, 3, 1, 0), (SI, 1, 2, 6), (G, 0, 2, 1), (G, 1, 3, 6), (SY, 3, 2, 0),
    (SI, 1, 1, 6), (G, 1, 1, 4), (SY, 1, 2, 4), (SI, 1, 3, 6), (SY, 3, 0, 6), (U, 3, 1, 0),
    (G, 0, 3, 6), (AI, 3, 1, 0), (SY, 1, 3, 2), (G, 1, 3, 4), (SI, 1, 3, 4), (SY, 1, 0, 2),
    (N, 3, 2, 0), (X, 3, 2, 0), (SI, 1, 1, 4), (N, 2, 0, 0), (SY, 1, 1, 2), (X, 2, 0, 0),
    (G, 1, 2, 4), (SI, 1, 2, 4), (N, 3, 3, 0), (X, 3, 3, 0), (G, 3, 0, 6), (SY, 1, 2, 2),
    (SI, 0, 2, 5), (U, 3, 2, 0), (SY, 0, 1, 0), (G, 1, 3, 2), (SI, 1, 3, 2), (U, 2, 0, 0),
    (G, 1, 0, 2), (AY, 3, 2, 0), (U, 3, 3, 0), (SI, 3, 0, 6), (G, 1, 1, 2), (SY, 1, 0, 6),
    (SI, 1, 1, 2), (SY, 0, 3, 0), (G, 1, 2, 2), (SI, 1, 0, 2), (SY, 0, 2, 0), (N, 0, 1, 0),
    (X, 0, 1, 0), (SI, 1, 2, 2), (SY, 0, 3, 2), (SI, 3, 1, 4), (G, 1, 0, 6), (SY, 1, 3, 0),
    (SI, 3, 1, 5), (SY, 0, 3, 4), (U, 0, 1, 0), (AI, 3, 2, 0), (SY, 3, 0, 0), (SI, 0, 2, 4),
    (SI, 0, 1, 5), (G, 0, 3, 2), (AY, 3, 3, 0), (SY, 1, 1, 0), (SI, 0, 2, 3), (N, 1, 3, 0),
    (V, 0, 0, 1), (AY, 2, 0, 0), (SI, 0, 2, 2), (G, 0, 3, 4), (SY, 0, 0, 0), (AI, 0, 1, 0),
    (AY, 3, 1, 0), (SI, 1, 0, 6), (N, 1, 1, 0), (AY, 0, 1, 0), (N, 3, 0, 0), (SI, 3, 1, 2),
    (X, 3, 0, 0), (SY, 1, 2, 0), (SI, 3, 1, 3), (SY, 1, 0, 0), (N, 0, 0, 0), (SI, 0, 1, 3),
    (X, 0, 0, 0), (AY, 3, 1, 6), (SI, 0, 1, 4), (U, 3, 0, 0), (AY, 1, 0, 2), (SI, 0, 0, 5),
    (AY, 1, 2, 2), (N, 1, 2, 0), (AI, 3, 3, 1), (U, 0, 0, 0), (AY, 0, 0, 0), (SI, 0, 1, 2),
    (AY, 3, 2, 6), (SI, 0, 3, 4), (AY, 1, 3, 2), (SI, 0, 2, 6), (AY, 1, 0, 4), (SI, 0, 3, 6),
    (AY, 3, 0, 0), (SI, 0, 0, 4), (AY, 1, 3, 4), (SI, 0, 3, 2), (AY, 1, 2, 4), (AI, 0, 0, 0),
    (AY, 0, 1, 6), (SI, 0, 0, 3), (N, 1, 0, 0), (X, 1, 0, 0), (AY, 0, 2, 2), (AI, 3, 3, 0),
    (AI, 2, 0, 1), (AY, 0, 2, 4), (SI, 0, 0, 2), (AY, 3, 1, 2), (U, 1, 0, 0), (U, 1, 2, 0),
    (AY, 1, 0, 0), (U, 1, 1, 0), (U, 1, 3, 0), (SI, 3, 2, 5), (AY, 1, 2, 0), (AI, 3, 0, 0),
    (AY, 0, 1, 2), (AI, 1, 0, 0), (N, 0, 2, 0), (X, 0, 2, 0), (V, 0, 0, 2), (AY, 1, 1, 0),
    (SI, 3, 2, 4), (AY, 1, 3, 0), (SI, 3, 2, 3), (N, 0, 3, 0), (X, 0, 3, 0), (AI, 1, 3, 0),
    (AY, 3, 1, 4), (U, 0, 2, 0), (AI, 0, 2, 0), (AY, 0, 2, 0), (SI, 3, 2, 2), (AY, 0, 3, 2),
    (U, 0, 3, 0), (AI, 1, 2, 0), (AY, 0, 1, 4), (AI, 0, 3, 0), (AY, 0, 3, 0), (AI, 3, 0, 1),
    (AY, 0, 0, 6), (AI, 2, 0, 0), (AY, 0, 3, 4), (AI, 1, 1, 0), (AY, 0, 0, 2), (AI, 1, 1, 1),
    (AY, 1, 0, 6), (AY, 0, 0, 4), (AY, 1, 3, 6), (AY, 0, 2, 6), (AY, 3, 2, 2), (AY, 1, 2, 6),
    (AY, 0, 3, 6), (AY, 3, 2, 4),
)
MID = (
    (E, 3, 0, 5), (SY, 3, 0, 4), (E, 3, 0, 7), (SY, 3, 0, 6), (E, 3, 0, 3), (E, 3, 0, 1),
    (E, 2, 0, 5), (E, 2, 0, 3), (E, 3, 3, 7), (E, 2, 0, 1), (E, 2, 0, 7), (SY, 2, 0, 4),
    (E, 3, 3, 5), (E, 3, 3, 3), (E, 3, 3, 1), (E, 1, 3, 7), (E, 1, 0, 5), (E, 1, 3, 5),
    (E, 1, 3, 1), (SY, 3, 3, 6), (E, 1, 3, 3), (E, 0, 3, 1), (E, 1, 2, 3), (E, 1, 2, 7),
    (E, 1, 2, 5), (E, 1, 2, 1), (E, 1, 1, 7), (E, 1, 1, 1), (E, 1, 1, 5), (SY, 2, 0, 2),
    (G, 3, 2, 6), (SI, 3, 2, 6), (E, 1, 1, 3), (E, 1, 0, 3), (E, 0, 3, 5), (E, 1, 0, 1),
    (E, 0, 3, 7), (SY, 2, 0, 0), (G, 3, 2, 7), (SI, 3, 2, 7), (E, 0, 3, 3), (E, 1, 0, 7),
    (G, 3, 1, 7), (SI, 3, 1, 7), (SY, 2, 0, 6), (G, 0, 0, 7), (SI, 0, 0, 7), (SY, 3, 0, 2),
    (G, 3, 2, 0), (SO, 3, 2, 0), (G, 0, 1, 7), (SI, 0, 1, 7), (G, 3, 2, 1), (SY, 3, 3, 4),
    (SO, 3, 2, 1), (G, 3, 1, 6), (SI, 3, 1, 6), (G, 3, 1, 1), (SY, 3, 3, 2), (SO, 3, 1, 1),
    (G, 3, 0, 4), (SI, 3, 0, 4), (SY, 3, 3, 0), (G, 0, 0, 1), (SO, 0, 0, 1), (SY, 1, 2, 2),
    (G, 0, 2, 7), (SI, 0, 2, 7), (G, 0, 1, 1), (SY, 1, 0, 4), (SO, 0, 1, 1), (G, 0, 1, 6),
    (SI, 0, 1, 6), (G, 3, 1, 0), (SO, 3, 1, 0), (SY, 1, 1, 6), (G, 2, 0, 4), (SI, 2, 0, 4),
    (SY, 1, 3, 6), (N, 3, 0, 0), (V, 0, 0, 0), (X, 3, 0, 0), (G, 0, 2, 1), (SO, 0, 2, 1),
    (SY, 1, 3, 4), (G, 0, 0, 6), (SI, 0, 0, 6), (G, 0, 1, 0), (SO, 0, 1, 0), (SY, 1, 2, 6),
    (G, 2, 0, 6), (SI, 2, 0, 6), (G, 3, 3, 6), (SI, 3, 3, 6), (U, 3, 0, 0), (SY, 1, 1, 0),
    (AO, 3, 0, 2), (AI, 3, 0, 2), (N, 2, 0, 0), (X, 2, 0, 0), (SY, 1, 2, 4), (G, 0, 0, 0),
    (SO, 0, 0, 0), (G, 3, 3, 4), (SI, 3, 3, 4), (SY, 1, 1, 4), (G, 2, 0, 0), (SO, 2, 0, 0),
    (G, 1, 0, 4), (SI, 1, 0, 4), (G, 3, 3, 0), (SY, 1, 2, 0), (SO, 3, 3, 0), (U, 2, 0, 0),
    (AI, 2, 0, 2), (AO, 3, 0, 4), (AY, 2, 0, 2), (AO, 2, 0, 2), (G, 1, 2, 6), (SI, 1, 2, 6),
    (N, 3, 3, 0), (X, 3, 3, 0), (SY, 1, 1, 2), (G, 1, 1, 6), (SI, 1, 1, 6), (AY, 3, 0, 2),
    (G, 1, 3, 6), (SI, 1, 3, 6), (AO, 2, 0, 4), (SY, 1, 3, 0), (AI, 3, 1, 0), (U, 3, 3, 0),
    (AO, 3, 3, 2), (SY, 1, 3, 2), (G, 1, 2, 0), (AO, 2, 0, 3), (AI, 3, 3, 2), (G, 1, 3, 4),
    (AI, 2, 0, 3), (SO, 1, 2, 0), (AY, 3, 3, 2), (G, 1, 1, 0), (G, 1, 1, 4), (SI, 1, 3, 4),
    (SO, 1, 1, 0), (SY, 0, 3, 0), (G, 1, 2, 4), (SI, 1, 2, 4), (SY, 1, 0, 2), (AO, 3, 0, 3),
    (G, 1, 3, 0), (G, 0, 2, 5), (SI, 1, 1, 4), (SY, 3, 0, 0), (SO, 1, 3, 0), (AI, 3, 0, 3),
    (AO, 3, 3, 4), (AY, 3, 1, 0), (G, 3, 0, 6), (AY, 3, 1, 6), (N, 1, 3, 0), (AO, 2, 0, 5),
    (AI, 3, 3, 3), (SY, 0, 3, 4), (SI, 3, 0, 6), (AO, 3, 1, 6), (SY, 1, 0, 0), (N, 1, 0, 0),
    (SI, 0, 2, 5), (AO, 3, 3, 3), (N, 1, 1, 0), (SY, 0, 3, 6), (N, 1, 2, 0), (X, 1, 0, 0),
    (AO, 3, 0, 5), (G, 3, 1, 4), (SI, 3, 1, 4), (SY, 0, 3, 2), (AO, 3, 3, 5), (G, 3, 1, 5),
    (SI, 3, 1, 5), (G, 3, 0, 0), (SO, 3, 0, 0), (SY, 1, 0, 6), (AI, 3, 2, 0), (U, 1, 0, 0),
    (AO, 1, 0, 2), (AI, 1, 0, 2), (AY, 3, 2, 0), (U, 1, 3, 0), (AO, 1, 3, 2), (AI, 1, 3, 2),
    (U, 1, 2, 0), (G, 0, 2, 4), (U, 1, 1, 0), (AY, 1, 0, 2), (AO, 1, 2, 2), (SI, 0, 2, 4),
    (G, 0, 1, 5), (AY, 1, 3, 2), (AO, 1, 1, 2), (AI, 1, 1, 2), (G, 0, 2, 3), (SY, 0, 2, 2),
    (AO, 3, 2, 6), (AI, 1, 2, 2), (AY, 1, 1, 2), (AO, 1, 0, 4), (SI, 0, 1, 5), (AY, 3, 2, 6),
    (AO, 1, 3, 4), (AI, 0, 1, 0), (G, 1, 0, 6), (AY, 0, 1, 0), (AO, 1, 1, 4), (SI, 1, 0, 6),
    (AY, 1, 0, 4), (N, 0, 2, 0), (X, 0, 2, 0), (G, 3, 1, 3), (AO, 1, 2, 4), (SY, 3, 1, 2),
    (AI, 1, 1, 3), (AO, 1, 1, 3), (V, 0, 0, 1), (G, 0, 1, 3), (AY, 1, 2, 2), (G, 0, 1, 4),
    (SI, 0, 1, 4), (AO, 0, 1, 6), (SY, 0, 1, 2), (U, 0, 2, 0), (AI, 0, 2, 2), (G, 0, 0, 5),
    (AO, 0, 2, 2), (G, 1, 0, 0), (AY, 1, 3, 4), (SI, 0, 0, 5), (SO, 1, 0, 0), (AI, 3, 3, 1),
    (N, 3, 1, 0), (AY, 0, 1, 6), (X, 3, 1, 0), (AO, 1, 1, 5), (AY, 0, 2, 2), (G, 0, 3, 4),
    (SI, 0, 3, 4), (AO, 0, 2, 4), (N, 0, 1, 0), (X, 0, 1, 0), (AY, 1, 2, 4), (G, 0, 2, 6),
    (SI, 0, 2, 6), (U, 3, 1, 0), (AO, 3, 1, 2), (AI, 3, 1, 2), (AY, 0, 2, 4), (G, 0, 3, 6),
    (AO, 3, 3, 7), (SI, 0, 3, 6), (AY, 3, 1, 2), (G, 0, 0, 4), (SI, 0, 0, 4), (U, 0, 1, 0),
    (AO, 0, 1, 2), (AY, 0, 1, 2), (N, 0, 3, 0), (X, 0, 3, 0), (AI, 0, 1, 2), (G, 0, 2, 0),
    (SO, 0, 2, 0), (AY, 0, 0, 0), (AO, 3, 1, 4), (AI, 0, 0, 0), (AY, 3, 1, 4), (G, 0, 0, 3),
    (G, 0, 3, 0), (SO, 0, 3, 0), (SY, 0, 0, 2), (AI, 3, 3, 0), (U, 0, 3, 0), (AO, 0, 3, 2),
    (AI, 0, 3, 2), (AY, 0, 3, 2), (AI, 2, 0, 1), (AO, 0, 1, 4), (AY, 0, 1, 4), (AO, 0, 0, 6),
    (AY, 0, 0, 6), (G, 3, 2, 5), (SI, 3, 2, 5), (AO, 3, 3, 6), (N, 0, 0, 0), (X, 0, 0, 0),
    (AI, 3, 0, 0), (AY, 0, 3, 4), (AO, 0, 3, 4), (AI, 1, 0, 0), (AY, 1, 0, 0), (AO, 2, 0, 7),
    (G, 3, 2, 4), (SI, 3, 2, 4), (G, 3, 2, 3), (V, 0, 0, 2), (SY, 3, 2, 2), (U, 0, 0, 0),
    (AI, 0, 0, 2), (AO, 0, 0, 2), (AY, 0, 0, 2), (AO, 3, 0, 6), (AI, 1, 3, 0), (AY, 1, 3, 0),
    (AO, 1, 0, 6), (AI, 0, 2, 0), (AY, 1, 0, 6), (N, 3, 2, 0), (X, 3, 2, 0), (AY, 0, 2, 0),
    (AO, 0, 0, 4), (AI, 1, 2, 0), (AY, 0, 0, 4), (AO, 1, 3, 6), (AI, 0, 3, 0), (AY, 0, 3, 0),
    (AO, 0, 2, 6), (AI, 3, 0, 1), (U, 3, 2, 0), (AO, 3, 2, 2), (AI, 3, 2, 2), (AY, 1, 2, 0),
    (AI, 2, 0, 0), (AO, 1, 2, 6), (AY, 1, 3, 6), (AI, 1, 1, 0), (AO, 0, 3, 6), (AY, 3, 2, 2),
    (AI, 1, 1, 1), (AO, 3, 0, 7), (AY, 0, 3, 6), (AO, 3, 2, 4), (AY, 0, 2, 6), (AO, 2, 0, 6),
    (AY, 3, 2, 4), (AO, 1, 1, 6), (AY, 1, 2, 6), (AO, 1, 1, 7),
)


def lanes_of(shapes, g, ref, i):
    n = len(GROUPS[g].members)
    w = shapes[g][1] // n
    return ref if n == 1 else ref.at[..., i * w : (i + 1) * w]


def finish(shapes, *refs):
    n = len(GROUPS)
    full, own, st = refs[0:n], refs[n : 2 * n], refs[2 * n : 3 * n]
    vectors = refs[3 * n : 3 * n + 6]
    halves, nexts, news = (refs[3 * n + 6 + 8 * k : 3 * n + 14 + 8 * k] for k in range(3))
    sem, vec_sem = refs[3 * n + 30 :]
    for g, group in enumerate(GROUPS):
        w = shapes[g][1]
        for i, a in enumerate(group.members):
            if group.rows:
                pltpu.make_async_copy(lanes_of(shapes, g, full[g], i), halves[a], sem.at[0, g]).start()
            else:
                for b in range(8):
                    dst = halves[a].at[:, b * w : (b + 1) * w]
                    pltpu.make_async_copy(full[g].at[b], dst, sem.at[0, g]).start()
            pltpu.make_async_copy(lanes_of(shapes, g, own[g], i), nexts[a], sem.at[1, g]).start()
            pltpu.make_async_copy(lanes_of(shapes, g, st[g], i), news[a], sem.at[2, g]).start()
    copies = []
    for i, dst in enumerate((*halves[6:], *nexts[6:], *news[6:])):
        copies.append(pltpu.make_async_copy(vectors[i], dst, vec_sem.at[i]))
        copies[-1].start()
    for g in range(n):
        for k, ref in enumerate((full[g], own[g], st[g])):
            pltpu.make_async_copy(ref, ref, sem.at[k, g]).wait()
    for c in copies:
        c.wait()


def kernel(replicas, models, limit, shapes, *refs):
    slopes, params, states = refs[0:6], refs[8:14], refs[16:22]
    vectors = [refs[i] for i in (6, 7, 14, 15, 22, 23)]
    groups = range(len(GROUPS))
    n = len(GROUPS)
    full, own, st = refs[24 : 24 + n], refs[24 + n : 24 + 2 * n], refs[24 + 2 * n : 24 + 3 * n]
    half_norm, half_bias, next_norm, next_bias, new_norm, new_bias = refs[24 + 3 * n : 30 + 3 * n]
    scratch = list(refs[30 + 3 * n :])
    take = lambda: [scratch.pop(0) for _ in groups]
    xin, enc, rec, sq, sqr = (take() for _ in range(5))
    vs, vown, vrec, vnext, vag, vh_norm, vh_bias = (scratch.pop(0) for _ in range(7))
    rs_s, rs_r, ag_s, ag_r, n_s, n_r, v_s, v_r, w_s, w_r = (scratch.pop(0) for _ in range(10))
    load_sem, own_sem, st_sem, vown_sem, vec_sem = scratch[0:5]
    slope_norm, slope_bias, param_norm, param_bias, state_norm, state_bias = small = scratch[5:]

    r = lax.axis_index("replica")
    m = lax.axis_index("model")
    y, z = lax.rem(r, 2), r // 2
    side = z // 2
    slab = [(p + side * (3 - 2 * p)) * 2 + (y if d == 0 else 1 - y) for p in range(4) for d in (0, 1)]

    scale = 2.0**13 / (limit * replicas)
    rate = replicas ** (-0.5)

    def encode(x):
        t = x * scale
        t2 = t * t
        t4 = t2 * t2
        return (t4 * t4 * t).astype(jnp.bfloat16)

    def decode(c):
        f = c.astype(jnp.float32)
        a = jnp.exp(jnp.log(jnp.abs(f)) * (1.0 / root)) * (1.0 / scale)
        return jnp.where(f < 0, -a, a)

    lanes = functools.partial(lanes_of, shapes)
    at = {k: i for i, k in enumerate(CHUNKS)}
    unit = lambda g: shapes[g][0] // sum(SIZES[g])
    height = lambda g, c: unit(g) * SIZES[g][c]
    rows = lambda g, c: pl.ds(unit(g) * sum(SIZES[g][:c]), height(g, c))

    def source(g, c, s):
        w = shapes[g][1]
        if GROUPS[g].rows:
            return xin[g].at[slab[s], rows(g, c)]
        return xin[g].at[rows(g, c), pl.ds(pl.multiple_of(slab[s] * w, w), w)]

    def loop(g, c, body):
        h, w = height(g, c), shapes[g][1]
        step = min(h, max(16, STEP // w // 16 * 16))
        while h % step:
            step -= 16
        lax.fori_loop(0, h // step, lambda i, c: (body(pl.ds(pl.multiple_of(i * step, step), step)), c)[1], 0)

    def remote(src, dst, s, d, peer, axis="replica"):
        return pltpu.make_async_remote_copy(
            src_ref=src, dst_ref=dst, send_sem=s, recv_sem=d, device_id={axis: peer}, device_id_type=MESH
        )

    def whole(ref, sem):
        pltpu.make_async_copy(ref, ref, sem).wait()

    barrier = pltpu.get_barrier_semaphore()

    def greet(axis, to):
        pl.semaphore_signal(barrier, inc=1, device_id={axis: to}, device_id_type=MESH)

    @pl.when(z > 0)
    def _():
        greet("replica", r - 2)

    @pl.when(z < 3)
    def _():
        greet("replica", r + 2)

    greet("replica", z * 2 + (1 - y))
    for j in range(1, models):
        greet("model", lax.rem(m + j, models))

    def chunk_of(g, c):
        return xin[g].at[:, rows(g, c)] if GROUPS[g].rows else xin[g].at[rows(g, c)]

    def load(g, c):
        for i, a in enumerate(GROUPS[g].members):
            src = slopes[a].at[:, rows(g, c)] if GROUPS[g].rows else slopes[a].at[rows(g, c)]
            pltpu.make_async_copy(src, lanes(g, chunk_of(g, c), i), load_sem.at[at[g, c]]).start()

    def load_own():
        for g in OWN:
            for i, a in enumerate(GROUPS[g].members):
                pltpu.make_async_copy(params[a], lanes(g, own[g], i), own_sem.at[g]).start()
                pltpu.make_async_copy(states[a], lanes(g, st[g], i), st_sem.at[g]).start()
        for i, ref in enumerate(vectors):
            pltpu.make_async_copy(ref, small[i], vec_sem.at[i]).start()

    for g, c in CHUNKS[:2]:
        load(g, c)
    for g in groups:
        if not GROUPS[g].rows:
            sq[g][...] = jnp.zeros_like(sq[g])

    def rule(p, s, v):
        s = hold_rate * s + (1.0 - hold_rate) * v * v
        return p - learn_rate * v * lax.rsqrt(s + 1e-06), s

    def fold(x):
        total = x[:, 0:128]
        for k in range(128, x.shape[1], 128):
            total = total + x[:, k : k + 128]
        return jnp.sum(total, axis=1, keepdims=True)

    width = vs.shape[1] // replicas

    def vec_out(j):
        to = lax.rem(r + j, replicas)
        return remote(
            vs.at[:, pl.ds(pl.multiple_of(to * width, width), width)],
            vrec.at[j - 1], v_s.at[j - 1], v_r.at[j - 1], to,
        )

    def vec_back(j):
        return remote(vnext, vag.at[j - 1], w_s.at[j - 1], w_r.at[j - 1], lax.rem(r + j, replicas))

    def vec_start():
        for i, ref in enumerate(vectors):
            pltpu.make_async_copy(ref, small[i], vec_sem.at[i]).wait()
        vs[0:1, :] = slope_norm[...]
        vs[1:2, :] = slope_bias[...]
        pltpu.make_async_copy(vs.at[:, pl.ds(pl.multiple_of(r * width, width), width)], vown, vown_sem).start()
        for j in range(1, replicas):
            vec_out(j).start()

    def vec_update():
        pltpu.make_async_copy(vown, vown, vown_sem).wait()
        total = vown[...]
        for j in range(1, replicas):
            vec_out(j).wait_recv()
            total = total + vrec[j - 1]
        v = total * rate
        p, s = rule(param_norm[...], state_norm[...], v[0:1, :])
        next_norm[...] = p
        new_norm[...] = s
        vnext[0:1, :] = p
        p, s = rule(param_bias[...], state_bias[...], v[1:2, :])
        next_bias[...] = p
        new_bias[...] = s
        vnext[1:2, :] = p
        for j in range(1, replicas):
            vec_back(j).start()

    def vec_finish():
        vh_norm[pl.ds(r, 1), :] = vnext[0:1, :]
        vh_bias[pl.ds(r, 1), :] = vnext[1:2, :]
        for j in range(1, replicas):
            vec_back(j).wait_recv()
            at = lax.rem(r + replicas - j, replicas)
            vh_norm[pl.ds(at, 1), :] = vag[j - 1, 0:1, :]
            vh_bias[pl.ds(at, 1), :] = vag[j - 1, 1:2, :]
        half_norm[...] = vh_norm[...].astype(jnp.bfloat16)
        half_bias[...] = vh_bias[...].astype(jnp.bfloat16)

    def run(mid, order):
        mine = 1 if mid else 0
        peers = {}
        if mid:
            peers[SO] = peers[AO] = side * 6 + y
            peers[SI] = peers[AI] = (3 - z) * 2 + y
        else:
            peers[SI] = peers[AI] = (1 + side) * 2 + y
        peers[SY] = peers[AY] = z * 2 + (1 - y)
        done = set()
        ahead = list(CHUNKS[2:])

        def kind(g, c):
            return SUMS[g][c]

        def landing(g, c, by, s):
            if kind(g, c) == A:
                return (0, 7, 3)[by] + s // 2
            return (10, 6 + s, s - 2)[by]

        def outgoing(g, c, op, s):
            p = s // 2
            if kind(g, c) == A:
                if op == SY:
                    return p
                return 3 + p if p else 4
            if op == SY:
                return 6
            if not mid:
                return s - 2
            return s - 4 if p >= 2 else 4 + s

        def across(op, s):
            return (3 - s // 2) * 2 + s % 2 if mid and op in (SI, AI) else s

        def send(op, g, c, s):
            by = {SY: 0, SO: 1, SI: 1 if mid else 2}[op]
            slot = landing(g, c, by, across(op, s))
            return remote(
                enc[g].at[outgoing(g, c, op, s), rows(g, c)],
                rec[g].at[slot, rows(g, c)],
                rs_s.at[g],
                rs_r.at[at[g, c], slot],
                peers[op],
            )

        def gather(op, g, c, s):
            to = s + 1 if op == AY else across(op, s)
            ref = full[g].at[slab[s], rows(g, c)]
            link = {AY: 0, AI: 1, AO: 2}[op]
            return remote(ref, ref, ag_s.at[at[g, c], link], ag_r.at[at[g, c], to], peers[op])

        def got(g, c, s):
            if s != mine * 2 and (g, c, s) not in done:
                done.add((g, c, s))
                ref = full[g].at[slab[s], rows(g, c)]
                whole(ref, ag_r.at[at[g, c], s])

        def arrived(g, c, by, s):
            slot = landing(g, c, by, s)
            ref = rec[g].at[slot, rows(g, c)]
            whole(ref, rs_r.at[at[g, c], slot])
            return ref

        def once(key, ref, sem):
            if key not in done:
                done.add(key)
                whole(ref, sem)

        def loaded(g, c):
            while (g, c) in ahead:
                load(*ahead.pop(0))
                if not ahead:
                    load_own()
            once((-1, g, c), chunk_of(g, c), load_sem.at[at[g, c]])

        def parts(g, c, s):
            loaded(g, c)
            by = []
            a, p = kind(g, c) == A, s // 2
            if a or s == mine * 2:
                by.append(0)
            if mid and p >= 1:
                by.append(2)
            if p == mine or (mid and p == 0):
                by.append(1)
            return [arrived(g, c, b, s) for b in by]

        def encode_op(g, c, s, op):
            loaded(g, c)
            src, dst = source(g, c, s), enc[g].at[outgoing(g, c, op, s), rows(g, c)]

            def body(d):
                dst[d, :] = encode(src[d, :])

            loop(g, c, body)

        def add_op(g, c, s):
            src = source(g, c, s)
            op = SY if s // 2 == mine else SO if mid and s < 2 else SI
            dst = enc[g].at[outgoing(g, c, op, s), rows(g, c)]
            got = parts(g, c, s)

            def body(d):
                total = src[d, :]
                for ref in got:
                    total = total + decode(ref[d, :])
                dst[d, :] = encode(total)

            loop(g, c, body)

        def mean_op(g, c):
            acc = source(g, c, mine * 2)
            got = parts(g, c, mine * 2)
            once((-2, g), own[g], own_sem.at[g])
            held = own[g].at[rows(g, c)]
            k = len(GROUPS[g].members)
            w = shapes[g][1] // k

            def mean(d):
                total = acc[d, :]
                for ref in got:
                    total = total + decode(ref[d, :])
                v = total * rate
                acc[d, :] = v
                return v

            if GROUPS[g].rows:
                sums = sq[g].at[rows(g, c)]

                def body(d):
                    v, p = mean(d), held[d, :]
                    v, p = v * v, p * p
                    lane = lax.broadcasted_iota(jnp.int32, (v.shape[0], 128), 1)
                    out = jnp.zeros((v.shape[0], 128), jnp.float32)
                    for i in range(k):
                        cols = slice(i * w, (i + 1) * w)
                        out = jnp.where(lane == 2 * i, fold(p[:, cols]), out)
                        out = jnp.where(lane == 2 * i + 1, fold(v[:, cols]), out)
                    sums[d, :] = out

            else:

                def body(d):
                    v, p = mean(d), held[d, :]
                    sq[g][0] += jnp.sum((p * p).reshape(-1, 8, w), axis=0)
                    sq[g][1] += jnp.sum((v * v).reshape(-1, 8, w), axis=0)

            loop(g, c, body)

        def norms(g, c, j):
            if GROUPS[g].rows:
                src, dst = sq[g].at[rows(g, c)], sqr[g].at[j - 1, rows(g, c)]
            else:
                src, dst = sq[g], sqr[g].at[j - 1]
            return remote(src, dst, n_s.at[at[g, c], j - 1], n_r.at[at[g, c], j - 1], lax.rem(m + j, models), "model")

        def update_op(g, c):
            first = c if GROUPS[g].rows else 0
            for j in range(1, models):
                if (-4, g, first, j) not in done:
                    done.add((-4, g, first, j))
                    norms(g, first, j).wait_recv()
            once((-3, g), st[g], st_sem.at[g])
            acc, half = source(g, c, mine * 2), full[g].at[slab[mine * 2], rows(g, c)]
            held, hold = own[g].at[rows(g, c)], st[g].at[rows(g, c)]
            k = len(GROUPS[g].members)
            w = shapes[g][1] // k

            def put(d, cols, t):
                p, s = rule(held[d, cols], hold[d, cols], acc[d, cols] * t)
                held[d, cols] = p
                hold[d, cols] = s
                half[d, cols] = p.astype(jnp.bfloat16)

            if GROUPS[g].rows:
                sums = [sq[g].at[rows(g, c)]] + [sqr[g].at[j, rows(g, c)] for j in range(models - 1)]

                def body(d):
                    total = sums[0][d, :]
                    for ref in sums[1:]:
                        total = total + ref[d, :]
                    lane = lax.broadcasted_iota(jnp.int32, total.shape, 1)
                    pick = lambda i: jnp.sum(jnp.where(lane == i, total, 0.0), axis=1, keepdims=True)
                    for i in range(k):
                        t = jnp.sqrt(pick(2 * i)) * lax.rsqrt(pick(2 * i + 1) + 1e-06)
                        put(d, slice(i * w, (i + 1) * w), t)

            else:
                total = sq[g][...]
                for j in range(models - 1):
                    total = total + sqr[g][j]
                total = jnp.sum(total, axis=1, keepdims=True)
                t = jnp.sqrt(total[0]) * lax.rsqrt(total[1] + 1e-06)

                def body(d):
                    put(d, slice(None), t)

            loop(g, c, body)

        met = False
        for i, (op, g, c, s) in enumerate(order):
            if ahead and i % 2:
                load(*ahead.pop(0))
                if not ahead:
                    load_own()
            if op not in (E, G) and not met:
                met = True
                pl.semaphore_wait(barrier, models + (2 if mid else 1))
            if op == E:
                encode_op(g, c, s, SY if kind(g, c) == A else SI)
            elif op == G:
                add_op(g, c, s)
            elif op in (SY, SI, SO):
                send(op, g, c, s).start()
            elif op == N:
                mean_op(g, c)
            elif op == X:
                for j in range(1, models):
                    norms(g, c, j).start()
            elif op == U:
                update_op(g, c)
            elif op == V:
                (vec_start, vec_update, vec_finish)[s]()
            else:
                got(g, c, s)
                gather(op, g, c, s).start()

        for g, c in CHUNKS:
            for s in range(8):
                got(g, c, s)
        for g in groups:
            whole(enc[g], rs_s.at[g])
        for g, c in CHUNKS:
            for link, count in enumerate(SENT[mid][BACK[g][c]]):
                if count:
                    whole(full[g].at[pl.ds(0, count), rows(g, c)], ag_s.at[at[g, c], link])
            if GROUPS[g].rows or c == 0:
                for j in range(1, models):
                    norms(g, c, j).wait_send()
        for j in range(1, replicas):
            vec_out(j).wait_send()
            vec_back(j).wait_send()

    end = jnp.logical_or(z == 0, z == 3)

    @pl.when(end)
    def _():
        run(False, END)

    @pl.when(jnp.logical_not(end))
    def _():
        run(True, MID)


def fused(replicas, models, shapes, *args):
    slopes, params = args[0:6], args[8:14]
    f32, bf16 = jnp.float32, jnp.bfloat16
    vec = args[6].shape[1]
    width = vec // replicas
    row = lambda a: a.reshape(1, -1)
    by_rows = [a in g.members and g.rows for a in range(6) for g in GROUPS if a in g.members]
    cut = lambda a, rows: a.reshape(replicas, -1, a.shape[-1]) if rows else a[0]
    args = (
        *(cut(a, rows) for a, rows in zip(slopes, by_rows)), *args[6:14],
        row(args[14]), row(args[15]), *args[16:22], row(args[22]), row(args[23]),
    )
    S = jax.ShapeDtypeStruct
    n, chunks = len(GROUPS), len(CHUNKS)
    held = [((replicas, *s), bf16) for s in shapes] + [(s, f32) for s in shapes] * 2
    held += [((replicas, width), bf16)] * 2 + [((1, width), f32)] * 4
    ANY, VM = pl.BlockSpec(memory_space=pl.ANY), pl.BlockSpec(memory_space=pltpu.VMEM)
    part = [ANY] * 8
    scratch = [
        pltpu.VMEM((replicas, *s) if g.rows else (s[0], s[1] * replicas), f32) for g, s in zip(GROUPS, shapes)
    ]
    scratch += [pltpu.VMEM((7, *s), bf16) for s in shapes]
    scratch += [pltpu.VMEM((11 if B in k else 9, *s), bf16) for k, s in zip(SUMS, shapes)]
    sq = [(s[0], 128) if g.rows else (2, 8, s[1]) for g, s in zip(GROUPS, shapes)]
    scratch += [pltpu.VMEM(s, f32) for s in sq]
    scratch += [pltpu.VMEM((models - 1, *s), f32) for s in sq]
    scratch += [
        pltpu.VMEM((2, vec), f32),
        pltpu.VMEM((2, width), f32),
        pltpu.VMEM((replicas - 1, 2, width), f32),
        pltpu.VMEM((2, width), f32),
        pltpu.VMEM((replicas - 1, 2, width), f32),
        pltpu.VMEM((replicas, width), f32),
        pltpu.VMEM((replicas, width), f32),
    ]
    dma = pltpu.SemaphoreType.DMA
    scratch += [dma((n,)), dma((chunks, 11)), dma((chunks, 3)), dma((chunks, 8))]
    scratch += [dma((chunks, models - 1))] * 2 + [dma((replicas - 1,))] * 4
    scratch += [dma((chunks,))] + [dma((n,))] * 2 + [dma(()), dma((6,))]
    scratch += [pltpu.VMEM((1, vec), f32)] * 2 + [pltpu.VMEM((1, width), f32)] * 4
    out = pl.pallas_call(
        functools.partial(kernel, replicas, models, 4.0, shapes),
        out_shape=[pltpu.VMEM(*h) for h in held],
        in_specs=part * 3,
        out_specs=[VM] * len(held),
        scratch_shapes=scratch,
        compiler_params=pltpu.CompilerParams(
            collective_id=0, has_side_effects=True, vmem_limit_bytes=54 * 1024 * 1024
        ),
    )(*args)
    outs = [
        S((replicas, a.shape[1] // replicas, a.shape[2]) if rows else a.shape[1:], bf16)
        for a, rows in zip(slopes, by_rows)
    ]
    outs += [S((replicas, width), bf16)] * 2
    for _ in range(2):
        outs += [S(a.shape, f32) for a in params] + [S((1, width), f32)] * 2
    out = pl.pallas_call(
        functools.partial(finish, shapes),
        out_shape=outs,
        in_specs=[VM] * len(held),
        out_specs=[ANY] * len(outs),
        scratch_shapes=[dma((3, n)), dma((6,))],
        compiler_params=pltpu.CompilerParams(vmem_limit_bytes=1024 * 1024),
    )(*out)
    flat = lambda a: a.reshape(-1)
    return (
        *(a.reshape(-1, a.shape[-1]) for a in out[0:6]), flat(out[6]), flat(out[7]),
        *out[8:14], flat(out[14]), flat(out[15]),
        *out[16:22], flat(out[22]), flat(out[23]),
    )


def plain(
    slope_up,
    slope_down,
    slope_query,
    slope_key,
    slope_value,
    slope_mixed,
    slope_norm,
    slope_bias,
    param_up,
    param_down,
    param_query,
    param_key,
    param_value,
    param_mixed,
    param_norm,
    param_bias,
    state_up,
    state_down,
    state_query,
    state_key,
    state_value,
    state_mixed,
    state_norm,
    state_bias,
):
    mean_up, mean_down, mean_query, mean_key, mean_value, mean_mixed = (
        lax.psum_scatter(slope_up[0], "replica", scatter_dimension=0, tiled=True),
        lax.psum_scatter(slope_down[0], "replica", scatter_dimension=1, tiled=True),
        lax.psum_scatter(slope_query[0], "replica", scatter_dimension=0, tiled=True),
        lax.psum_scatter(slope_key[0], "replica", scatter_dimension=0, tiled=True),
        lax.psum_scatter(slope_value[0], "replica", scatter_dimension=0, tiled=True),
        lax.psum_scatter(slope_mixed[0], "replica", scatter_dimension=1, tiled=True),
    )
    whole_norm, whole_bias = lax.psum((slope_norm[0], slope_bias[0]), "replica")
    place = lax.axis_index("replica")
    mean_norm = lax.dynamic_slice_in_dim(
        whole_norm, place * param_norm.shape[0], param_norm.shape[0]
    )
    mean_bias = lax.dynamic_slice_in_dim(
        whole_bias, place * param_bias.shape[0], param_bias.shape[0]
    )
    mean_rate = lax.axis_size("replica") ** (-0.5)
    mean_up = mean_up * mean_rate
    mean_down = mean_down * mean_rate
    mean_query = mean_query * mean_rate
    mean_key = mean_key * mean_rate
    mean_value = mean_value * mean_rate
    mean_mixed = mean_mixed * mean_rate
    mean_norm = mean_norm * mean_rate
    mean_bias = mean_bias * mean_rate
    (
        own_up,
        own_down,
        own_query,
        own_key,
        own_value,
        own_mixed,
        slope_up_norm,
        slope_down_norm,
        slope_query_norm,
        slope_key_norm,
        slope_value_norm,
        slope_mixed_norm,
    ) = lax.psum(
        (
            jnp.sum(param_up * param_up, axis=1, keepdims=True),
            jnp.sum(param_down * param_down, axis=0, keepdims=True),
            jnp.sum(param_query * param_query, axis=1, keepdims=True),
            jnp.sum(param_key * param_key, axis=1, keepdims=True),
            jnp.sum(param_value * param_value, axis=1, keepdims=True),
            jnp.sum(param_mixed * param_mixed, axis=0, keepdims=True),
            jnp.sum(mean_up * mean_up, axis=1, keepdims=True),
            jnp.sum(mean_down * mean_down, axis=0, keepdims=True),
            jnp.sum(mean_query * mean_query, axis=1, keepdims=True),
            jnp.sum(mean_key * mean_key, axis=1, keepdims=True),
            jnp.sum(mean_value * mean_value, axis=1, keepdims=True),
            jnp.sum(mean_mixed * mean_mixed, axis=0, keepdims=True),
        ),
        "model",
    )
    mean_up = mean_up * (jnp.sqrt(own_up) * lax.rsqrt(slope_up_norm + 1e-06))
    mean_down = mean_down * (jnp.sqrt(own_down) * lax.rsqrt(slope_down_norm + 1e-06))
    mean_query = mean_query * (jnp.sqrt(own_query) * lax.rsqrt(slope_query_norm + 1e-06))
    mean_key = mean_key * (jnp.sqrt(own_key) * lax.rsqrt(slope_key_norm + 1e-06))
    mean_value = mean_value * (jnp.sqrt(own_value) * lax.rsqrt(slope_value_norm + 1e-06))
    mean_mixed = mean_mixed * (jnp.sqrt(own_mixed) * lax.rsqrt(slope_mixed_norm + 1e-06))
    state_new_up = hold_rate * state_up + (1.0 - hold_rate) * mean_up * mean_up
    next_up = param_up - learn_rate * mean_up * lax.rsqrt(state_new_up + 1e-06)
    state_new_down = hold_rate * state_down + (1.0 - hold_rate) * mean_down * mean_down
    next_down = param_down - learn_rate * mean_down * lax.rsqrt(state_new_down + 1e-06)
    state_new_query = hold_rate * state_query + (1.0 - hold_rate) * mean_query * mean_query
    next_query = param_query - learn_rate * mean_query * lax.rsqrt(state_new_query + 1e-06)
    state_new_key = hold_rate * state_key + (1.0 - hold_rate) * mean_key * mean_key
    next_key = param_key - learn_rate * mean_key * lax.rsqrt(state_new_key + 1e-06)
    state_new_value = hold_rate * state_value + (1.0 - hold_rate) * mean_value * mean_value
    next_value = param_value - learn_rate * mean_value * lax.rsqrt(state_new_value + 1e-06)
    state_new_mixed = hold_rate * state_mixed + (1.0 - hold_rate) * mean_mixed * mean_mixed
    next_mixed = param_mixed - learn_rate * mean_mixed * lax.rsqrt(state_new_mixed + 1e-06)
    state_new_norm = hold_rate * state_norm + (1.0 - hold_rate) * mean_norm * mean_norm
    next_norm = param_norm - learn_rate * mean_norm * lax.rsqrt(state_new_norm + 1e-06)
    state_new_bias = hold_rate * state_bias + (1.0 - hold_rate) * mean_bias * mean_bias
    next_bias = param_bias - learn_rate * mean_bias * lax.rsqrt(state_new_bias + 1e-06)
    half_up, half_down, half_query, half_key, half_value, half_mixed, half_norm, half_bias = (
        lax.all_gather(next_up.astype(jnp.bfloat16), "replica", axis=0, tiled=True),
        lax.all_gather(next_down.astype(jnp.bfloat16), "replica", axis=1, tiled=True),
        lax.all_gather(next_query.astype(jnp.bfloat16), "replica", axis=0, tiled=True),
        lax.all_gather(next_key.astype(jnp.bfloat16), "replica", axis=0, tiled=True),
        lax.all_gather(next_value.astype(jnp.bfloat16), "replica", axis=0, tiled=True),
        lax.all_gather(next_mixed.astype(jnp.bfloat16), "replica", axis=1, tiled=True),
        lax.all_gather(next_norm.astype(jnp.bfloat16), "replica", axis=0, tiled=True),
        lax.all_gather(next_bias.astype(jnp.bfloat16), "replica", axis=0, tiled=True),
    )
    return (
        half_up,
        half_down,
        half_query,
        half_key,
        half_value,
        half_mixed,
        half_norm,
        half_bias,
        next_up,
        next_down,
        next_query,
        next_key,
        next_value,
        next_mixed,
        next_norm,
        next_bias,
        state_new_up,
        state_new_down,
        state_new_query,
        state_new_key,
        state_new_value,
        state_new_mixed,
        state_new_norm,
        state_new_bias,
    )


def solution(mesh):
    replicas, models = mesh.shape["replica"], mesh.shape["model"]

    def local(*args):
        if replicas != 2**3 or any(a.shape[k] % 128 for a in args[8:14] for k in (0, 1)):
            return plain(*args)
        shapes = []
        for g, sizes in zip(GROUPS, SIZES):
            h, w = args[8 + g.members[0]].shape
            shapes.append((h, w * len(g.members)))
            if h % (16 * sum(sizes)) or (w != 128 and not g.rows):
                return plain(*args)
        if args[14].shape[0] % 128:
            return plain(*args)
        return fused(replicas, models, shapes, *args)

    placed = (
        P("replica", None, "model"),
        P("replica", "model", None),
        P("replica", None, "model"),
        P("replica", None, "model"),
        P("replica", None, "model"),
        P("replica", "model", None),
        P("replica", None),
        P("replica", None),
        P("replica", "model"),
        P("model", "replica"),
        P("replica", "model"),
        P("replica", "model"),
        P("replica", "model"),
        P("model", "replica"),
        P("replica"),
        P("replica"),
        P("replica", "model"),
        P("model", "replica"),
        P("replica", "model"),
        P("replica", "model"),
        P("replica", "model"),
        P("model", "replica"),
        P("replica"),
        P("replica"),
    )
    return jax.shard_map(
        local,
        mesh=mesh,
        in_specs=placed,
        out_specs=(
            P(None, "model"),
            P("model", None),
            P(None, "model"),
            P(None, "model"),
            P(None, "model"),
            P("model", None),
            P(),
            P(),
            P("replica", "model"),
            P("model", "replica"),
            P("replica", "model"),
            P("replica", "model"),
            P("replica", "model"),
            P("model", "replica"),
            P("replica"),
            P("replica"),
            P("replica", "model"),
            P("model", "replica"),
            P("replica", "model"),
            P("replica", "model"),
            P("replica", "model"),
            P("model", "replica"),
            P("replica"),
            P("replica"),
        ),
        check_vma=False,
    )
```
